32 devices in a mesh: ctx: 8 (over z, x), fsdp: 4 (over y, core).
Axes of the slice: x: 2, y: 2, z: 4, core: 2. Of those that a mesh axis runs over, the one named last changes fastest.
Arguments:
- tokens: bfloat16 [8, 2, 256, 1536], P('ctx', None, 'fsdp'), may hold values from -6 to 6
- pairing: int32 [8], replicated, may hold values from 0 to 7, each once
- gain_attn: bfloat16 [1536], P('fsdp'), may hold values from 0.099609375 to 1.8984375
- w_qkv: bfloat16 [1536, 2048], P('fsdp'), may hold values from -0.15625 to 0.15625
- b_qkv: bfloat16 [2048], P('fsdp'), may hold values from -10 to 10
- w_out: bfloat16 [1536, 1536], P('fsdp'), may hold values from -0.625 to 0.625
- gain_mlp: bfloat16 [1536], P('fsdp'), may hold values from 0.099609375 to 1.8984375
- w_gate_up: bfloat16 [1536, 2, 4480], P('fsdp'), may hold values from -0.15625 to 0.15625
- w_down: bfloat16 [4480, 1536], P('fsdp'), may hold values from -0.09375 to 0.09375
- cotangent: bfloat16 [8, 2, 256, 1536], P('ctx', None, 'fsdp'), may hold values from -6 to 6
Outputs:
- block_output: bfloat16 [8, 2, 256, 1536], P('ctx', None, 'fsdp')
- d_tokens: float32 [8, 2, 256, 1536], P('ctx', None, 'fsdp')
- d_gain_attn: float32 [1536], P('fsdp')
- d_w_qkv: float32 [1536, 2048], P('fsdp')
- d_b_qkv: float32 [2048], P('fsdp')
- d_w_out: float32 [1536, 1536], P('fsdp')
- d_gain_mlp: float32 [1536], P('fsdp')
- d_w_gate_up: float32 [1536, 2, 4480], P('fsdp')
- d_w_down: float32 [4480, 1536], P('fsdp')
The draws below stay inside these ranges and needn't reach their ends.
Inputs may be any that keep to these rules, and one draw needn't show every extreme that they name: Each index of ctx holds stretches pairing[c] and 2 * 8 - 1 - pairing[c] of the sequence.
All inputs are finite; a program needn't handle non-finite values.
Results may differ from the reference program's by a relative error of at most 0.02.
The reference program's roundings to bfloat16 on the way (of `normed1`, `attended`, `normed2`, `act`, `d_gu` and `d_scores`) count: a program that leaves them out, or rounds other values in their place, can miss the bound.
Values may be sent and summed in bfloat16 or wider, within the bound.
A program may use at most 384 MiB of HBM per device.

```python
import math
import jax
import jax.numpy as jnp
from jax import lax

D = 1536
HEADS = 12
KV_HEADS = 2
HEAD_DIM = 128
FF = 4480
STRETCH = 256
SEQ = 4096
N_CTX = 8


def draw_b_qkv(key, part):
    q_width = HEADS * HEAD_DIM
    kv_width = KV_HEADS * HEAD_DIM
    total_len = q_width + 2 * kv_width
    first_key = jax.random.fold_in(key, 0)
    base = jnp.clip(jax.random.normal(first_key, (total_len,), jnp.float32) * 0.5, -3.0, 3.0)
    return base.astype(jnp.bfloat16)


def steps_of(stream_key, extent, cuts, smallest, top_value):
    level = 1.0
    for dim, shards_of in cuts:
        steps = jax.random.uniform(jax.random.fold_in(jax.random.fold_in(stream_key, 6), dim), (shards_of,), jnp.float32, smallest / len(cuts), top_value / len(cuts))
        level = level * jnp.repeat(jnp.exp(steps), extent[dim] // shards_of).reshape((-1,) + (1,) * (len(extent) - 1 - dim))
    return level


def bell_draw(own_key, shape, spread, most, cuts=(), held_as=jnp.bfloat16):
    entries = spread * jax.random.normal(own_key, shape, jnp.float32)
    if cuts:
        entries = entries * steps_of(own_key, shape, cuts, -0.22, 0.18)
    return jnp.clip(entries, -most, most).astype(held_as)


def setup_inputs(seed: int = 0) -> dict:
    arg_keys = jax.random.split(jax.random.key(seed), 11)
    tokens = bell_draw(arg_keys[0], (N_CTX, 2, STRETCH, D), 1.0, 6.0, ((0, 8), (2, 4)))
    pairing = jax.random.permutation(arg_keys[1], N_CTX).astype(jnp.int32)
    gain_attn = jnp.clip(1.0 + 0.18 * jax.random.normal(arg_keys[2], (D,), jnp.float32), 0.099609375, 1.8984375).astype(jnp.bfloat16)
    w_qkv = bell_draw(arg_keys[3], (D, (HEADS + 2 * KV_HEADS) * HEAD_DIM), D ** -0.5, 0.15625, ((0, 4),))
    b_qkv = draw_b_qkv(jax.random.fold_in(arg_keys[10], 71), 0)
    w_out = bell_draw(arg_keys[5], (HEADS * HEAD_DIM, D), (D // 16) ** -0.5, 0.625, ((0, 4),))
    gain_mlp = jnp.clip(1.0 + 0.18 * jax.random.normal(arg_keys[6], (D,), jnp.float32), 0.099609375, 1.8984375).astype(jnp.bfloat16)
    w_gate_up = bell_draw(arg_keys[7], (D, 2, FF), D ** -0.5, 0.15625, ((0, 4),))
    w_down = bell_draw(arg_keys[8], (FF, D), FF ** -0.5, 0.09375, ((0, 4),))
    cotangent = bell_draw(arg_keys[9], (N_CTX, 2, STRETCH, D), 1.0, 6.0, ((0, 8), (2, 4)))
    return {"tokens": tokens, "pairing": pairing, "gain_attn": gain_attn, "w_qkv": w_qkv, "b_qkv": b_qkv, "w_out": w_out, "gain_mlp": gain_mlp, "w_gate_up": w_gate_up, "w_down": w_down, "cotangent": cotangent}


eps = 1e-06
rope_base = 1000000.0

def rope_tables(position):
    half = HEAD_DIM // 2
    inverse = rope_base ** (-(jnp.arange(half, dtype=jnp.float32) * 2.0 / HEAD_DIM))
    angle = position.astype(jnp.float32)[:, None] * inverse[None, :]
    return (jnp.cos(angle)[:, None, :], jnp.sin(angle)[:, None, :])

def rotate(vectors, cosines, sines):
    half = HEAD_DIM // 2
    first, second = (vectors[..., :half], vectors[..., half:])
    return jnp.concatenate([first * cosines - second * sines, second * cosines + first * sines], -1)

def unrotate(grads, cosines, sines):
    half = HEAD_DIM // 2
    first, second = (grads[..., :half], grads[..., half:])
    return jnp.concatenate([first * cosines + second * sines, second * cosines - first * sines], -1)

def rms_scale(values):
    return lax.rsqrt(lax.optimization_barrier(jnp.mean(values * values, -1, keepdims=True)) + eps)

def rms_backward(values, scale_rows, gain, d_normed):
    d_gain = lax.optimization_barrier(jnp.sum(d_normed * values * scale_rows, 0))
    d_inner = d_normed * gain
    d_values = scale_rows * d_inner - values * scale_rows ** 3 * lax.optimization_barrier(jnp.mean(d_inner * values, -1, keepdims=True))
    return (d_values, d_gain)

def reference(tokens, pairing, gain_attn, w_qkv, b_qkv, w_out, gain_mlp, w_gate_up, w_down, cotangent):
    f32 = jnp.float32
    bf16 = jnp.bfloat16
    q_width = HEADS * HEAD_DIM
    kv_width = KV_HEADS * HEAD_DIM
    per_group = HEADS // KV_HEADS
    softmax_scale = HEAD_DIM ** (-0.5)
    stretches = jnp.stack([pairing, 2 * N_CTX - 1 - pairing], 1).astype(jnp.int32)
    position = (stretches[:, :, None] * STRETCH + jnp.arange(STRETCH, dtype=jnp.int32)[None, None, :]).reshape(SEQ)
    inputs = tokens.reshape(SEQ, D).astype(f32)
    gain_one = gain_attn.astype(f32)
    gain_two = gain_mlp.astype(f32)
    scale_one = rms_scale(inputs)
    normed1 = (inputs * scale_one * gain_one).astype(bf16)
    qkv = jnp.dot(normed1, w_qkv, preferred_element_type=f32) + b_qkv.astype(f32)
    cosines, sines = rope_tables(position)
    query = rotate(qkv[:, :q_width].reshape(SEQ, HEADS, HEAD_DIM), cosines, sines).astype(bf16)
    keys = rotate(qkv[:, q_width:q_width + kv_width].reshape(SEQ, KV_HEADS, HEAD_DIM), cosines, sines).astype(bf16)
    values = qkv[:, q_width + kv_width:].reshape(SEQ, KV_HEADS, HEAD_DIM).astype(bf16)
    keys32 = keys.astype(f32)
    values32 = values.astype(f32)
    qblock = math.gcd(SEQ, 256)
    nblock = SEQ // qblock
    query_blocks = query.reshape(nblock, qblock, KV_HEADS, per_group, HEAD_DIM)
    pos_blocks = position.reshape(nblock, qblock)

    def scores_of(query_block, query_pos):
        scores = jnp.einsum('tkgd,skd->kgts', query_block.astype(f32), keys32) * softmax_scale
        visible = position[None, None, None, :] <= query_pos[None, None, :, None]
        return (jnp.where(visible, scores, -1e+30), visible)

    def forward_step(carry, blocked):
        query_block, query_pos = blocked
        scores, visible = scores_of(query_block, query_pos)
        highest = lax.optimization_barrier(jnp.max(scores, -1, keepdims=True))
        totals = lax.optimization_barrier(jnp.sum(jnp.where(visible, jnp.exp(scores - highest), 0.0), -1, keepdims=True))
        lse = highest + jnp.log(totals)
        probs = jnp.where(visible, jnp.exp(scores - lse), 0.0).astype(bf16)
        attended = jnp.einsum('kgts,skd->tkgd', probs.astype(f32), values32)
        return (carry, (attended, lse[..., 0]))
    _, (attended, lse_all) = lax.scan(forward_step, jnp.zeros((), f32), (query_blocks, pos_blocks))
    attended16 = attended.reshape(SEQ, q_width).astype(bf16)
    hidden = inputs + jnp.dot(attended16, w_out, preferred_element_type=f32)
    scale_two = rms_scale(hidden)
    normed2 = (hidden * scale_two * gain_two).astype(bf16)
    gate_up = jnp.einsum('td,def->tef', normed2.astype(f32), w_gate_up.astype(f32))
    gate_val = gate_up[:, 0]
    up_val = gate_up[:, 1]
    act = (jax.nn.silu(gate_val) * up_val).astype(bf16)
    result = hidden + jnp.dot(act, w_down, preferred_element_type=f32)
    block_output = result.astype(bf16).reshape(tokens.shape)
    cot = cotangent.reshape(SEQ, D)
    d_act = jnp.dot(cot, w_down.T, preferred_element_type=f32)
    d_w_down = jnp.dot(act.T, cot, preferred_element_type=f32)
    sigmoid_gate = jax.nn.sigmoid(gate_val)
    d_gate = d_act * up_val * sigmoid_gate * (1.0 + gate_val * (1.0 - sigmoid_gate))
    d_up = d_act * gate_val * sigmoid_gate
    d_gu = jnp.stack([d_gate, d_up], 1).astype(bf16)
    d_w_gate_up = jnp.einsum('td,tef->def', normed2.astype(f32), d_gu.astype(f32))
    d_normed2 = jnp.einsum('tef,def->td', d_gu.astype(f32), w_gate_up.astype(f32))
    d_hidden_norm, d_gain_mlp = rms_backward(hidden, scale_two, gain_two, d_normed2)
    d_hidden = cot.astype(f32) + d_hidden_norm
    d_hidden16 = d_hidden.astype(bf16)
    d_w_out = jnp.dot(attended16.T, d_hidden16, preferred_element_type=f32)
    d_attended = jnp.dot(d_hidden16, w_out.T, preferred_element_type=f32).astype(bf16)
    delta = lax.optimization_barrier(jnp.sum(d_attended.astype(f32).reshape(SEQ, HEADS, HEAD_DIM) * attended16.astype(f32).reshape(SEQ, HEADS, HEAD_DIM), -1))
    delta_blocks = delta.reshape(nblock, qblock, KV_HEADS, per_group).transpose(0, 2, 3, 1)
    d_att_blocks = d_attended.reshape(nblock, qblock, KV_HEADS, per_group, HEAD_DIM)

    def backward_step(carry, blocked):
        d_keys, d_values = carry
        query_block, query_pos, d_att_block, lse_block, delta_block = blocked
        scores, visible = scores_of(query_block, query_pos)
        probs = jnp.where(visible, jnp.exp(scores - lse_block[..., None]), 0.0)
        probs16 = probs.astype(bf16)
        d_probs = jnp.einsum('tkgd,skd->kgts', d_att_block.astype(f32), values32)
        d_scores = (probs * (d_probs - delta_block[..., None])).astype(bf16).astype(f32)
        d_query = softmax_scale * jnp.einsum('kgts,skd->tkgd', d_scores, keys32)
        d_keys = d_keys + softmax_scale * jnp.einsum('kgts,tkgd->skd', d_scores, query_block.astype(f32))
        d_values = d_values + jnp.einsum('kgts,tkgd->skd', probs16.astype(f32), d_att_block.astype(f32))
        return ((d_keys, d_values), d_query)
    zero_kv = jnp.zeros((SEQ, KV_HEADS, HEAD_DIM), f32)
    (d_keys, d_values), d_query = lax.scan(backward_step, (zero_kv, zero_kv), (query_blocks, pos_blocks, d_att_blocks, lse_all, delta_blocks))
    d_query = unrotate(d_query.reshape(SEQ, HEADS, HEAD_DIM), cosines, sines).reshape(SEQ, q_width)
    d_keys = unrotate(d_keys, cosines, sines).reshape(SEQ, kv_width)
    d_qkv = jnp.concatenate([d_query, d_keys, d_values.reshape(SEQ, kv_width)], 1)
    d_b_qkv = lax.optimization_barrier(jnp.sum(d_qkv, 0))
    d_qkv16 = d_qkv.astype(bf16)
    d_w_qkv = jnp.dot(normed1.T, d_qkv16, preferred_element_type=f32)
    d_normed1 = jnp.dot(d_qkv16, w_qkv.T, preferred_element_type=f32)
    d_input_norm, d_gain_attn = rms_backward(inputs, scale_one, gain_one, d_normed1)
    d_tokens = (d_hidden + d_input_norm).reshape(tokens.shape)
    return (block_output, d_tokens, d_gain_attn, d_w_qkv, d_b_qkv, d_w_out, d_gain_mlp, d_w_gate_up, d_w_down)
```

```python
import functools

import jax
import jax.numpy as jnp
from jax import lax
from jax.experimental import pallas as pl
from jax.experimental.pallas import tpu as pltpu
from jax.sharding import PartitionSpec as P

D = 1536
HEADS = 12
KV_HEADS = 2
HEAD_DIM = 128

eps = 1e-06
rope_base = 1000000.0
F32 = jnp.float32
BF16 = jnp.bfloat16
VMEM_LIMIT = 60 * 1024 * 1024


def rope_tables(position):
    half = HEAD_DIM // 2
    inverse = rope_base ** (-(jnp.arange(half, dtype=F32) * 2.0 / HEAD_DIM))
    angle = position.astype(F32)[:, None] * inverse[None, :]
    return (jnp.cos(angle)[:, None, :], jnp.sin(angle)[:, None, :])


def rotate(vectors, cosines, sines):
    half = HEAD_DIM // 2
    first, second = (vectors[..., :half], vectors[..., half:])
    return jnp.concatenate([first * cosines - second * sines, second * cosines + first * sines], -1)


def unrotate(grads, cosines, sines):
    half = HEAD_DIM // 2
    first, second = (grads[..., :half], grads[..., half:])
    return jnp.concatenate([first * cosines + second * sines, second * cosines - first * sines], -1)


def rms_scale(values):
    return lax.rsqrt(jnp.mean(values * values, -1, keepdims=True) + eps)


def rms_backward(values, scale_rows, gain, d_normed):
    d_gain = jnp.sum(d_normed * values * scale_rows, 0)
    d_inner = d_normed * gain
    d_values = scale_rows * d_inner - values * scale_rows**3 * jnp.mean(
        d_inner * values, -1, keepdims=True
    )
    return (d_values, d_gain)


def dot(left, right, contract):
    return lax.dot_general(left, right, (contract, ((), ())), preferred_element_type=F32)


def contract_rows(left, right):
    return dot(left, right, ((0,), (0,)))


def contract_cols(left, right):
    return dot(left, right, ((1,), (1,)))


def stacked_heads(ref, which, heads):
    return jnp.concatenate(
        [ref[which, :, h * HEAD_DIM : (h + 1) * HEAD_DIM] for h in range(heads)], 0
    )


def causal(block_len, heads):
    keys = lax.broadcasted_iota(jnp.int32, (block_len, block_len), 0)
    queries = lax.broadcasted_iota(jnp.int32, (block_len, block_len), 1)
    return jnp.concatenate([keys <= queries] * heads, 1)


def attend_kernel(heads, table, ids, q_ref, kv_ref, o_ref, lse_ref):
    block_len = q_ref.shape[1]
    cols = heads * block_len
    scale = HEAD_DIM ** (-0.5)
    for which in range(2):
        last = ids[which]
        query = stacked_heads(q_ref, which, heads)

        def step(block, carry, masked=False):
            highest, total, acc = carry
            start = pl.multiple_of(table[block] * block_len, block_len)
            key = kv_ref[pl.ds(start, block_len), :HEAD_DIM]
            value = kv_ref[pl.ds(start, block_len), HEAD_DIM:]
            scores = contract_cols(key, query) * scale
            if masked:
                scores = jnp.where(causal(block_len, heads), scores, -1e30)
            new_high = jnp.maximum(highest, jnp.max(scores, 0, keepdims=True))
            probs = jnp.exp(scores - new_high)
            fade = jnp.exp(highest - new_high)
            total = total * fade + jnp.sum(probs, 0, keepdims=True)
            acc = acc * fade + contract_rows(value, probs.astype(BF16))
            return (new_high, total, acc)

        begin = (
            jnp.full((1, cols), -1e30, F32),
            jnp.zeros((1, cols), F32),
            jnp.zeros((HEAD_DIM, cols), F32),
        )
        carry = lax.fori_loop(0, last, step, begin)
        highest, total, acc = step(last, carry, True)
        lse_ref[which] = highest + jnp.log(total)
        out = (acc / total).T
        for h in range(heads):
            o_ref[which, :, h * HEAD_DIM : (h + 1) * HEAD_DIM] = out[
                h * block_len : (h + 1) * block_len
            ].astype(BF16)


def attend_back_kernel(
    heads, table, ids, q_ref, kv_ref, o_ref, do_ref, lse_ref, dq_ref, dkv_ref, sums
):
    block_len = q_ref.shape[1]
    cols = heads * block_len
    scale = HEAD_DIM ** (-0.5)
    sums[...] = jnp.zeros_like(sums)
    for which in range(2):
        last = ids[which]
        query = stacked_heads(q_ref, which, heads)
        d_out = stacked_heads(do_ref, which, heads)
        out = stacked_heads(o_ref, which, heads)
        delta = jnp.sum((d_out.astype(F32) * out.astype(F32)).T, 0, keepdims=True)
        lse = lse_ref[which]

        def step(block, d_query, masked=False):
            start = pl.multiple_of(table[block] * block_len, block_len)
            key = kv_ref[pl.ds(start, block_len), :HEAD_DIM]
            value = kv_ref[pl.ds(start, block_len), HEAD_DIM:]
            scores = contract_cols(key, query) * scale
            probs = jnp.exp(scores - lse)
            if masked:
                probs = jnp.where(causal(block_len, heads), probs, 0.0)
            d_probs = contract_cols(value, d_out)
            d_scores = (probs * (d_probs - delta)).astype(BF16)
            sums[pl.ds(start, block_len), :HEAD_DIM] += dot(d_scores, query, ((1,), (0,)))
            sums[pl.ds(start, block_len), HEAD_DIM:] += dot(
                probs.astype(BF16), d_out, ((1,), (0,))
            )
            return d_query + contract_rows(key, d_scores)

        d_query = lax.fori_loop(0, last, step, jnp.zeros((HEAD_DIM, cols), F32))
        d_query = step(last, d_query, True)
        d_query = (d_query * scale).T
        for h in range(heads):
            dq_ref[which, :, h * HEAD_DIM : (h + 1) * HEAD_DIM] = d_query[
                h * block_len : (h + 1) * block_len
            ]
    dkv_ref[:, :HEAD_DIM] = (sums[:, :HEAD_DIM] * scale).astype(BF16)
    dkv_ref[:, HEAD_DIM:] = sums[:, HEAD_DIM:].astype(BF16)


def in_vmem(count):
    return [pl.BlockSpec(memory_space=pltpu.VMEM)] * count


def in_smem(count):
    return [pl.BlockSpec(memory_space=pltpu.SMEM)] * count


def attend(table, ids, query, keys_values, heads):
    _, block_len, width = query.shape
    tall = keys_values.shape[0]
    return pl.pallas_call(
        functools.partial(attend_kernel, heads),
        out_shape=(
            jax.ShapeDtypeStruct(query.shape, BF16),
            jax.ShapeDtypeStruct((2, 1, heads * block_len), F32),
        ),
        in_specs=in_smem(2) + in_vmem(2),
        out_specs=tuple(in_vmem(2)),
        compiler_params=pltpu.CompilerParams(vmem_limit_bytes=VMEM_LIMIT),
        cost_estimate=pl.CostEstimate(
            flops=2 * tall * block_len * width * 2,
            bytes_accessed=tall * 512,
            transcendentals=tall * heads * block_len,
        ),
        name="attend",
    )(table, ids, query, keys_values)


def attend_back(table, ids, query, keys_values, out, d_out, lse, heads):
    _, block_len, width = query.shape
    tall = keys_values.shape[0]
    return pl.pallas_call(
        functools.partial(attend_back_kernel, heads),
        out_shape=(
            jax.ShapeDtypeStruct(query.shape, F32),
            jax.ShapeDtypeStruct(keys_values.shape, BF16),
        ),
        in_specs=in_smem(2) + in_vmem(5),
        out_specs=tuple(in_vmem(2)),
        scratch_shapes=[pltpu.VMEM(keys_values.shape, F32)],
        compiler_params=pltpu.CompilerParams(vmem_limit_bytes=VMEM_LIMIT),
        cost_estimate=pl.CostEstimate(
            flops=5 * tall * block_len * width * 2,
            bytes_accessed=tall * 1024,
            transcendentals=tall * heads * block_len,
        ),
        name="attend_back",
    )(table, ids, query, keys_values, out, d_out, lse)


def exchange(pieces, axis):
    return lax.all_to_all(pieces, axis, split_axis=0, concat_axis=0, tiled=True)


def exchange_async(pieces, axis):
    n = pieces.shape[0]
    me = lax.axis_index(axis)
    own = lax.dynamic_index_in_dim(pieces, me, 0, keepdims=True)
    arrived = lax.dynamic_update_slice_in_dim(jnp.zeros_like(pieces), own, me, 0)
    for shift in range(1, n):
        piece = lax.dynamic_index_in_dim(pieces, (me + shift) % n, 0, keepdims=True)
        piece = lax.ppermute(piece, axis, [(i, (i + shift) % n) for i in range(n)])
        arrived = lax.dynamic_update_slice_in_dim(arrived, piece, (me + n - shift) % n, 0)
    return arrived


def body(tokens, pairing, gain_attn, w_qkv, b_qkv, w_out, gain_mlp, w_gate_up, w_down, cotangent):
    half_rows = tokens.shape[2]
    n_ctx = lax.axis_size("ctx")
    n_fsdp = lax.axis_size("fsdp")
    ctx_index = lax.axis_index("ctx")
    fsdp_index = lax.axis_index("fsdp")
    stretch_len = half_rows * n_fsdp
    rows = 2 * stretch_len
    local_count = 2 * half_rows
    q_width = HEADS * HEAD_DIM
    kv_width = KV_HEADS * HEAD_DIM
    heads = HEADS // n_fsdp
    q_cols = heads * HEAD_DIM
    d_shard = w_qkv.shape[0]
    ff_shard = w_down.shape[0]

    owner_range = jnp.arange(n_ctx, dtype=jnp.int32)
    own_first = jnp.sum(jnp.where(owner_range == ctx_index, pairing, 0))
    ids = jnp.stack([own_first, 2 * n_ctx - 1 - own_first])
    inverse_pair = jnp.sum(
        owner_range[:, None] * (pairing[:, None] == owner_range[None, :]).astype(jnp.int32), 0
    )
    table = jnp.concatenate([2 * inverse_pair, 2 * inverse_pair[::-1] + 1])
    position = (
        ids[:, None] * stretch_len + jnp.arange(stretch_len, dtype=jnp.int32)[None, :]
    ).reshape(rows)
    kv_of = [f * KV_HEADS // n_fsdp for f in range(n_fsdp)]
    my_kv = fsdp_index * KV_HEADS // n_fsdp

    small = lax.all_gather(jnp.concatenate([gain_attn, gain_mlp, b_qkv]), "fsdp", axis=0)
    gain_one = small[:, :d_shard].reshape(D).astype(F32)
    gain_two = small[:, d_shard : 2 * d_shard].reshape(D).astype(F32)
    bias = small[:, 2 * d_shard :].reshape(-1).astype(F32)
    x_all = lax.all_gather(tokens[0], "fsdp", axis=1, tiled=True).reshape(rows, D)
    qkv_pieces = jnp.stack(
        [
            jnp.concatenate(
                [
                    w_qkv[:, f * q_cols : (f + 1) * q_cols],
                    w_qkv[:, q_width + kv_of[f] * HEAD_DIM : q_width + (kv_of[f] + 1) * HEAD_DIM],
                    w_qkv[
                        :,
                        q_width + kv_width + kv_of[f] * HEAD_DIM : q_width
                        + kv_width
                        + (kv_of[f] + 1) * HEAD_DIM,
                    ],
                ],
                1,
            )
            for f in range(n_fsdp)
        ]
    )
    w_qkv_cols = exchange(qkv_pieces, "fsdp").reshape(D, -1)
    bias_cols = jnp.concatenate(
        [
            lax.dynamic_slice_in_dim(bias, fsdp_index * q_cols, q_cols),
            lax.dynamic_slice_in_dim(bias, q_width + my_kv * HEAD_DIM, HEAD_DIM),
            lax.dynamic_slice_in_dim(bias, q_width + kv_width + my_kv * HEAD_DIM, HEAD_DIM),
        ]
    )
    w_gate_cols, w_up_cols = (
        exchange_async(
            w_gate_up[:, e].reshape(d_shard, n_fsdp, ff_shard).transpose(1, 0, 2), "fsdp"
        ).reshape(D, ff_shard)
        for e in range(2)
    )
    cot_all = lax.all_gather(cotangent[0], "fsdp", axis=1, tiled=True).reshape(rows, D)

    x32 = x_all.astype(F32)
    normed1 = (x32 * rms_scale(x32) * gain_one).astype(BF16)
    qkv = jnp.dot(normed1, w_qkv_cols, preferred_element_type=F32) + bias_cols
    cosines, sines = rope_tables(position)
    rotated = rotate(
        qkv[:, : q_cols + HEAD_DIM].reshape(rows, heads + 1, HEAD_DIM), cosines, sines
    ).astype(BF16)
    query = rotated[:, :heads].reshape(2, stretch_len, q_cols)
    own_kv = jnp.concatenate([rotated[:, heads], qkv[:, q_cols + HEAD_DIM :].astype(BF16)], 1)
    keys_values = lax.all_gather(own_kv, "ctx", axis=0, tiled=True)
    attended, lse = attend(table, ids, query, keys_values, heads)
    attended16 = attended.reshape(rows, q_cols)

    def scatter(partial):
        return lax.psum_scatter(
            partial.astype(BF16).reshape(2, stretch_len, D), "fsdp", scatter_dimension=1, tiled=True
        ).astype(F32).reshape(local_count, D)

    def gather(own):
        return lax.all_gather(
            own.reshape(2, half_rows, D), "fsdp", axis=1, tiled=True
        ).reshape(rows, D)

    inputs = tokens.reshape(local_count, D).astype(F32)
    scale_one = rms_scale(inputs)
    hidden = inputs + scatter(jnp.dot(attended16, w_out, preferred_element_type=F32))
    scale_two = rms_scale(hidden)
    normed2 = gather((hidden * scale_two * gain_two).astype(BF16))
    gate_val = jnp.dot(normed2, w_gate_cols, preferred_element_type=F32)
    up_val = jnp.dot(normed2, w_up_cols, preferred_element_type=F32)
    sigmoid_gate = jax.nn.sigmoid(gate_val)
    act16 = (jax.nn.silu(gate_val) * up_val).astype(BF16)
    result = hidden + scatter(jnp.dot(act16, w_down, preferred_element_type=F32))
    block_output = result.astype(BF16).reshape(tokens.shape)

    d_act = contract_cols(cot_all, w_down)
    d_gate16 = (d_act * up_val * sigmoid_gate * (1.0 + gate_val * (1.0 - sigmoid_gate))).astype(BF16)
    d_up16 = (d_act * gate_val * sigmoid_gate).astype(BF16)
    d_normed2 = scatter(contract_cols(d_gate16, w_gate_cols) + contract_cols(d_up16, w_up_cols))
    cot = cotangent.reshape(local_count, D).astype(F32)
    d_hidden_norm, d_gain_two = rms_backward(hidden, scale_two, gain_two, d_normed2)
    d_hidden = cot + d_hidden_norm
    dh_all = gather(d_hidden.astype(BF16))
    d_attended16 = contract_cols(dh_all, w_out).astype(BF16).reshape(2, stretch_len, q_cols)
    d_query, d_kv = attend_back(
        table, ids, query, keys_values, attended, d_attended16, lse, heads
    )
    d_kv_own = lax.psum_scatter(d_kv, "ctx", scatter_dimension=0, tiled=True).astype(F32)

    d_w_down = contract_rows(act16, cot_all).astype(BF16)
    d_w_gate, d_w_up = (
        exchange(contract_rows(normed2, piece).astype(BF16).reshape(n_fsdp, d_shard, ff_shard), "fsdp")
        for piece in (d_gate16, d_up16)
    )
    d_w_gate_up = jnp.stack(
        [piece.transpose(1, 0, 2).reshape(d_shard, n_fsdp * ff_shard) for piece in (d_w_gate, d_w_up)], 1
    )
    d_w_out = contract_rows(attended16, dh_all).astype(BF16)

    d_rotated = jnp.concatenate([d_query.reshape(rows, q_cols), d_kv_own[:, :HEAD_DIM]], 1)
    d_rotated = unrotate(
        d_rotated.reshape(rows, heads + 1, HEAD_DIM), cosines, sines
    ).reshape(rows, q_cols + HEAD_DIM)
    d_qkv = jnp.concatenate([d_rotated, d_kv_own[:, HEAD_DIM:]], 1)
    d_bias = jnp.sum(d_qkv, 0)
    d_qkv16 = d_qkv.astype(BF16)
    d_normed1 = scatter(contract_cols(d_qkv16, w_qkv_cols))
    d_input_norm, d_gain_one = rms_backward(inputs, scale_one, gain_one, d_normed1)
    d_tokens = (d_hidden + d_input_norm).reshape(tokens.shape)

    d_w_pieces = exchange(
        contract_rows(normed1, d_qkv16).astype(BF16).reshape(n_fsdp, d_shard, -1), "fsdp"
    )

    def by_columns(pieces):
        queries = [pieces[f][..., :q_cols] for f in range(n_fsdp)]
        rest = []
        for part in range(2):
            lo = q_cols + part * HEAD_DIM
            for g in range(KV_HEADS):
                rest.append(
                    sum(
                        pieces[f][..., lo : lo + HEAD_DIM].astype(F32)
                        for f in range(n_fsdp)
                        if kv_of[f] == g
                    ).astype(pieces[0].dtype)
                )
        return jnp.concatenate(queries + rest, -1)

    d_w_qkv = by_columns([d_w_pieces[f] for f in range(n_fsdp)])

    zeros = jnp.zeros_like(d_bias)
    d_bias_full = by_columns([jnp.where(fsdp_index == f, d_bias, zeros) for f in range(n_fsdp)])
    vector = lax.psum(
        jnp.concatenate([d_gain_one, d_gain_two, d_bias_full]), ("ctx", "fsdp")
    )
    d_gain_attn = lax.dynamic_slice_in_dim(vector[:D], fsdp_index * d_shard, d_shard)
    d_gain_mlp = lax.dynamic_slice_in_dim(vector[D : 2 * D], fsdp_index * d_shard, d_shard)
    b_shard = b_qkv.shape[0]
    d_b_qkv = lax.dynamic_slice_in_dim(vector[2 * D :], fsdp_index * b_shard, b_shard)

    def total(partial):
        return lax.psum(partial, "ctx").astype(F32)

    return (
        block_output,
        d_tokens,
        d_gain_attn,
        total(d_w_qkv),
        d_b_qkv,
        total(d_w_out),
        d_gain_mlp,
        total(d_w_gate_up),
        total(d_w_down),
    )


def solution(mesh):
    placed = (
        P("ctx", None, "fsdp", None),
        P(),
        P("fsdp"),
        P("fsdp", None),
        P("fsdp"),
        P("fsdp", None),
        P("fsdp"),
        P("fsdp", None, None),
        P("fsdp", None),
        P("ctx", None, "fsdp", None),
    )
    return jax.shard_map(
        body,
        mesh=mesh,
        in_specs=placed,
        out_specs=(
            P("ctx", None, "fsdp", None),
            P("ctx", None, "fsdp", None),
            P("fsdp"),
            P("fsdp", None),
            P("fsdp"),
            P("fsdp", None),
            P("fsdp"),
            P("fsdp", None, None),
            P("fsdp", None),
        ),
        check_vma=False,
    )
```

```python
import functools

import jax
import jax.numpy as jnp
from jax import lax
from jax.experimental import pallas as pl
from jax.experimental.pallas import tpu as pltpu
from jax.sharding import PartitionSpec as P

D = 1536
HEADS = 12
KV_HEADS = 2
HEAD_DIM = 128

eps = 1e-06
rope_base = 1000000.0
F32 = jnp.float32
BF16 = jnp.bfloat16
VMEM_LIMIT = 60 * 1024 * 1024


def rope_tables(position):
    half = HEAD_DIM // 2
    inverse = rope_base ** (-(jnp.arange(half, dtype=F32) * 2.0 / HEAD_DIM))
    angle = position.astype(F32)[:, None] * inverse[None, :]
    return (jnp.cos(angle)[:, None, :], jnp.sin(angle)[:, None, :])


def rotate(vectors, cosines, sines):
    half = HEAD_DIM // 2
    first, second = (vectors[..., :half], vectors[..., half:])
    return jnp.concatenate([first * cosines - second * sines, second * cosines + first * sines], -1)


def unrotate(grads, cosines, sines):
    half = HEAD_DIM // 2
    first, second = (grads[..., :half], grads[..., half:])
    return jnp.concatenate([first * cosines + second * sines, second * cosines - first * sines], -1)


def rms_scale(values):
    return lax.rsqrt(jnp.mean(values * values, -1, keepdims=True) + eps)


def rms_backward(values, scale_rows, gain, d_normed):
    d_gain = jnp.sum(d_normed * values * scale_rows, 0)
    d_inner = d_normed * gain
    d_values = scale_rows * d_inner - values * scale_rows**3 * jnp.mean(
        d_inner * values, -1, keepdims=True
    )
    return (d_values, d_gain)


def dot(left, right, contract):
    return lax.dot_general(left, right, (contract, ((), ())), preferred_element_type=F32)


def contract_rows(left, right):
    return dot(left, right, ((0,), (0,)))


def contract_cols(left, right):
    return dot(left, right, ((1,), (1,)))


def stacked_heads(ref, which, heads):
    return jnp.concatenate(
        [ref[which, :, h * HEAD_DIM : (h + 1) * HEAD_DIM] for h in range(heads)], 0
    )


def causal(block_len, heads):
    keys = lax.broadcasted_iota(jnp.int32, (block_len, block_len), 0)
    queries = lax.broadcasted_iota(jnp.int32, (block_len, block_len), 1)
    return jnp.concatenate([keys <= queries] * heads, 1)


def attend_kernel(heads, table, ids, q_ref, kv_ref, o_ref, lse_ref):
    block_len = q_ref.shape[1]
    cols = heads * block_len
    scale = HEAD_DIM ** (-0.5)
    for which in range(2):
        last = ids[which]
        query = stacked_heads(q_ref, which, heads)

        def step(block, carry, masked=False):
            highest, total, acc = carry
            start = pl.multiple_of(table[block] * block_len, block_len)
            key = kv_ref[pl.ds(start, block_len), :HEAD_DIM]
            value = kv_ref[pl.ds(start, block_len), HEAD_DIM:]
            scores = contract_cols(key, query) * scale
            if masked:
                scores = jnp.where(causal(block_len, heads), scores, -1e30)
            new_high = jnp.maximum(highest, jnp.max(scores, 0, keepdims=True))
            probs = jnp.exp(scores - new_high)
            fade = jnp.exp(highest - new_high)
            total = total * fade + jnp.sum(probs, 0, keepdims=True)
            acc = acc * fade + contract_rows(value, probs.astype(BF16))
            return (new_high, total, acc)

        begin = (
            jnp.full((1, cols), -1e30, F32),
            jnp.zeros((1, cols), F32),
            jnp.zeros((HEAD_DIM, cols), F32),
        )
        carry = lax.fori_loop(0, last, step, begin)
        highest, total, acc = step(last, carry, True)
        lse_ref[which] = highest + jnp.log(total)
        out = (acc / total).T
        for h in range(heads):
            o_ref[which, :, h * HEAD_DIM : (h + 1) * HEAD_DIM] = out[
                h * block_len : (h + 1) * block_len
            ].astype(BF16)


def attend_back_kernel(
    heads, table, ids, q_ref, kv_ref, o_ref, do_ref, lse_ref, dq_ref, dkv_ref, sums
):
    block_len = q_ref.shape[1]
    cols = heads * block_len
    scale = HEAD_DIM ** (-0.5)
    sums[...] = jnp.zeros_like(sums)
    for which in range(2):
        last = ids[which]
        query = stacked_heads(q_ref, which, heads)
        d_out = stacked_heads(do_ref, which, heads)
        out = stacked_heads(o_ref, which, heads)
        delta = jnp.sum((d_out.astype(F32) * out.astype(F32)).T, 0, keepdims=True)
        lse = lse_ref[which]

        def step(block, d_query, masked=False):
            start = pl.multiple_of(table[block] * block_len, block_len)
            key = kv_ref[pl.ds(start, block_len), :HEAD_DIM]
            value = kv_ref[pl.ds(start, block_len), HEAD_DIM:]
            scores = contract_cols(key, query) * scale
            probs = jnp.exp(scores - lse)
            if masked:
                probs = jnp.where(causal(block_len, heads), probs, 0.0)
            d_probs = contract_cols(value, d_out)
            d_scores = (probs * (d_probs - delta)).astype(BF16)
            sums[pl.ds(start, block_len), :HEAD_DIM] += dot(d_scores, query, ((1,), (0,)))
            sums[pl.ds(start, block_len), HEAD_DIM:] += dot(
                probs.astype(BF16), d_out, ((1,), (0,))
            )
            return d_query + contract_rows(key, d_scores)

        d_query = lax.fori_loop(0, last, step, jnp.zeros((HEAD_DIM, cols), F32))
        d_query = step(last, d_query, True)
        d_query = (d_query * scale).T
        for h in range(heads):
            dq_ref[which, :, h * HEAD_DIM : (h + 1) * HEAD_DIM] = d_query[
                h * block_len : (h + 1) * block_len
            ]
    dkv_ref[:, :HEAD_DIM] = (sums[:, :HEAD_DIM] * scale).astype(BF16)
    dkv_ref[:, HEAD_DIM:] = sums[:, HEAD_DIM:].astype(BF16)


def in_vmem(count):
    return [pl.BlockSpec(memory_space=pltpu.VMEM)] * count


def in_smem(count):
    return [pl.BlockSpec(memory_space=pltpu.SMEM)] * count


def attend(table, ids, query, keys_values, heads):
    _, block_len, width = query.shape
    tall = keys_values.shape[0]
    return pl.pallas_call(
        functools.partial(attend_kernel, heads),
        out_shape=(
            jax.ShapeDtypeStruct(query.shape, BF16),
            jax.ShapeDtypeStruct((2, 1, heads * block_len), F32),
        ),
        in_specs=in_smem(2) + in_vmem(2),
        out_specs=tuple(in_vmem(2)),
        compiler_params=pltpu.CompilerParams(vmem_limit_bytes=VMEM_LIMIT),
        cost_estimate=pl.CostEstimate(
            flops=2 * tall * block_len * width * 2,
            bytes_accessed=tall * 512,
            transcendentals=tall * heads * block_len,
        ),
        name="attend",
    )(table, ids, query, keys_values)


def attend_back(table, ids, query, keys_values, out, d_out, lse, heads):
    _, block_len, width = query.shape
    tall = keys_values.shape[0]
    return pl.pallas_call(
        functools.partial(attend_back_kernel, heads),
        out_shape=(
            jax.ShapeDtypeStruct(query.shape, F32),
            jax.ShapeDtypeStruct(keys_values.shape, BF16),
        ),
        in_specs=in_smem(2) + in_vmem(5),
        out_specs=tuple(in_vmem(2)),
        scratch_shapes=[pltpu.VMEM(keys_values.shape, F32)],
        compiler_params=pltpu.CompilerParams(vmem_limit_bytes=VMEM_LIMIT),
        cost_estimate=pl.CostEstimate(
            flops=5 * tall * block_len * width * 2,
            bytes_accessed=tall * 1024,
            transcendentals=tall * heads * block_len,
        ),
        name="attend_back",
    )(table, ids, query, keys_values, out, d_out, lse)


MESH = pl.DeviceIdType.MESH


def greet(devices):
    barrier = pltpu.get_barrier_semaphore()
    for device in devices:
        pl.semaphore_signal(barrier, inc=1, device_id=device, device_id_type=MESH)
    pl.semaphore_wait(barrier, len(devices))


def remote(src, dst, send, recv, device):
    return pltpu.make_async_remote_copy(
        src_ref=src, dst_ref=dst, send_sem=send, recv_sem=recv, device_id=device, device_id_type=MESH
    )


def group_places(n):
    ctx = lax.axis_index("ctx")
    me = lax.axis_index("fsdp")
    partner = me + 1 - 2 * (me % 2)
    others = [(me + 2 * k) % n for k in range(1, n // 2)]
    senders = [(me + n - 2 * k) % n for k in range(1, n // 2)]
    return ctx, me, partner, others, senders


def sum_kernel(mode, n, cuts, *refs):
    gathers = mode != "input"
    if mode == "attention":
        partial, tokens, gain, hidden_out, all_out = refs[:5]
    elif mode == "mlp":
        partial, hidden_in, cot, gain, d_out, all_out, d_gain = refs[:7]
    else:
        partial, tokens, d_hidden_in, gain, d_out, d_gain = refs[:6]
    near, summed, far, stage, near_s, near_r, far_s, far_r, own_s, own_r, out_s, out_r, fwd_s, fwd_r = refs[-14:]
    ctx, me, partner, others, senders = group_places(n)
    chips = n // 2
    rows = partial.shape[2]
    piece = rows // cuts
    chunks = [(w, i * piece) for w in range(2) for i in range(cuts)]
    greet([(ctx, partner)] + [(ctx, o) for o in others])

    def part(ref, w, lead, start):
        return ref.at[w, lead, pl.ds(start, piece)]

    first = []
    for c, (w, start) in enumerate(chunks):
        for j in range(chips):
            target = (partner + 2 * (j + 1)) % n
            copy = remote(
                part(partial, w, target, start),
                part(near, w, j, start),
                near_s.at[c, j],
                near_r.at[c, j],
                (ctx, partner),
            )
            copy.start()
            first.append(copy)

    second = []

    def post(c):
        w, start = chunks[c]
        for j in range(chips - 1):
            copy = remote(
                part(summed, w, j, start),
                part(far, w, j, start),
                far_s.at[c, j],
                far_r.at[c, j],
                (ctx, others[j]),
            )
            copy.start()
            second.append(copy)

    for c, (w, start) in enumerate(chunks):
        span = pl.ds(start, piece)
        for j in range(chips - 1):
            first[c * chips + j].wait()
            target = (me + 2 * (j + 1)) % n
            summed[w, j, span] = (
                partial[w, target, span].astype(F32) + near[w, j, span].astype(F32)
            ).astype(BF16)
        if c:
            post(c - 1)
    post(len(chunks) - 1)

    if mode != "attention":
        d_gain[...] = jnp.zeros_like(d_gain)
    third = []

    def spread(c):
        w, start = chunks[c]
        src = stage.at[w, pl.ds(start, piece)]
        for k in range(chips - 1):
            copy = remote(src, part(all_out, w, me, start), out_s.at[c, k], out_r.at[c, k], (ctx, others[k]))
            copy.start()
            third.append(copy)
        copy = remote(src, part(all_out, w, me, start), own_s.at[c], own_r.at[c], (ctx, partner))
        copy.start()
        return copy

    near_copies = []
    for c, (w, start) in enumerate(chunks):
        span = pl.ds(start, piece)
        first[c * chips + chips - 1].wait()
        total = partial[w, me, span].astype(F32) + near[w, chips - 1, span].astype(F32)
        for j in range(chips - 1):
            second[c * (chips - 1) + j].wait()
            total += far[w, j, span].astype(F32)
        if mode == "attention":
            hidden = tokens[w, span].astype(F32) + total
            hidden_out[w, span] = hidden
            rounded = (hidden * rms_scale(hidden) * gain[...]).astype(BF16)
        elif mode == "mlp":
            hidden = hidden_in[w, span]
            d_norm, gain_part = rms_backward(hidden, rms_scale(hidden), gain[...], total)
            d_gain[...] += gain_part[None]
            d_hidden = cot[w, span].astype(F32) + d_norm
            d_out[w, span] = d_hidden
            rounded = d_hidden.astype(BF16)
        else:
            values = tokens[w, span].astype(F32)
            d_norm, gain_part = rms_backward(values, rms_scale(values), gain[...], total)
            d_gain[...] += gain_part[None]
            d_out[w, span] = d_hidden_in[w, span] + d_norm
        if gathers:
            stage[w, span] = rounded
            all_out[w, me, span] = rounded
            if c:
                near_copies.append(spread(c - 1))
    if not gathers:
        return
    near_copies.append(spread(len(chunks) - 1))

    forwards = []
    for c, (w, start) in enumerate(chunks):
        for k in range(chips - 1):
            third[c * (chips - 1) + k].wait_recv()
            block = part(all_out, w, senders[k], start)
            copy = remote(block, block, fwd_s.at[c, k], fwd_r.at[c, k], (ctx, partner))
            copy.start()
            forwards.append(copy)
    for copy in third:
        copy.wait_send()
    for copy in near_copies + forwards:
        copy.wait()


def group_sum(mode, partial, *operands, collective):
    _, n, rows, width = partial.shape
    cuts = 2
    chunks = 2 * cuts
    chips = n // 2
    row_shape = (2, rows, width)
    full = jax.ShapeDtypeStruct(row_shape, F32)
    gathered = jax.ShapeDtypeStruct(partial.shape, BF16)
    gain_sum = jax.ShapeDtypeStruct((1, width), F32)
    out_shape = {
        "attention": (full, gathered),
        "mlp": (full, gathered, gain_sum),
        "input": (full, gain_sum),
    }[mode]
    dma = pltpu.SemaphoreType.DMA
    return pl.pallas_call(
        functools.partial(sum_kernel, mode, n, cuts),
        out_shape=out_shape,
        in_specs=in_vmem(1 + len(operands)),
        out_specs=tuple(in_vmem(len(out_shape))),
        scratch_shapes=[
            pltpu.VMEM((2, chips, rows, width), BF16),
            pltpu.VMEM((2, chips - 1, rows, width), BF16),
            pltpu.VMEM((2, chips - 1, rows, width), BF16),
            pltpu.VMEM(row_shape, BF16),
            dma((chunks, chips)),
            dma((chunks, chips)),
            dma((chunks, chips - 1)),
            dma((chunks, chips - 1)),
            dma((chunks,)),
            dma((chunks,)),
            dma((chunks, chips - 1)),
            dma((chunks, chips - 1)),
            dma((chunks, chips - 1)),
            dma((chunks, chips - 1)),
        ],
        compiler_params=pltpu.CompilerParams(
            vmem_limit_bytes=VMEM_LIMIT, collective_id=collective, has_side_effects=True
        ),
        cost_estimate=pl.CostEstimate(
            flops=20 * rows * width, bytes_accessed=60_000_000, transcendentals=0
        ),
        name="group_sum_" + mode,
    )(partial, *operands)


def ring_index(place, n):
    late = place // (n // 2)
    return (1 - late) * 2 * place + late * (2 * n - 1 - 2 * place)


def ring_place(index, n):
    odd = index % 2
    return (1 - odd) * (index // 2) + odd * (n - 1 - index // 2)


def share_kernel(n, own, out, right_s, right_r, left_s, left_r, near_s, near_r):
    ctx = lax.axis_index("ctx")
    me = lax.axis_index("fsdp")
    which = me % 2
    partner = me + 1 - 2 * which
    place = ring_place(ctx, n)
    right = (ring_index((place + 1) % n, n), me)
    left = (ring_index((place + n - 1) % n, n), me)
    greet([right, left, (ctx, partner)])

    def block(offset):
        return out.at[ring_index((place + n + offset) % n, n), which]

    def to_right(step):
        src = own.at[which] if step == 0 else block(-step)
        return remote(src, block(-step), right_s.at[step], right_r.at[step], right)

    def to_left(step):
        src = own.at[which] if step == 0 else block(step)
        return remote(src, block(step), left_s.at[step], left_r.at[step], left)

    rights, lefts = n // 2, n - 1 - n // 2
    sent = [to_right(0), to_left(0)]
    for copy in sent:
        copy.start()
    out[ctx] = own[...]
    going = [sent[0], sent[1]]
    for step in range(1, rights + 1):
        going[0].wait_recv()
        if step < rights:
            going[0] = to_right(step)
            going[0].start()
            sent.append(going[0])
        hand = remote(block(-step), block(-step), near_s.at[step - 1], near_r.at[step - 1], (ctx, partner))
        hand.start()
        sent.append(hand)
        if step <= lefts:
            going[1].wait_recv()
            if step < lefts:
                going[1] = to_left(step)
                going[1].start()
                sent.append(going[1])
            slot = rights + step - 1
            hand = remote(block(step), block(step), near_s.at[slot], near_r.at[slot], (ctx, partner))
            hand.start()
            sent.append(hand)
    for copy in sent:
        copy.wait_send()
    for step in range(1, rights + 1):
        remote(block(-step), block(-step), near_s.at[step - 1], near_r.at[step - 1], (ctx, partner)).wait_recv()
    for step in range(1, lefts + 1):
        slot = rights + step - 1
        remote(block(step), block(step), near_s.at[slot], near_r.at[slot], (ctx, partner)).wait_recv()


def share_keys(own, n, collective):
    dma = pltpu.SemaphoreType.DMA
    return pl.pallas_call(
        functools.partial(share_kernel, n),
        out_shape=jax.ShapeDtypeStruct((n,) + own.shape, BF16),
        in_specs=in_vmem(1),
        out_specs=in_vmem(1)[0],
        scratch_shapes=[dma((n // 2,))] * 4 + [dma((n - 1,))] * 2,
        compiler_params=pltpu.CompilerParams(
            vmem_limit_bytes=VMEM_LIMIT, collective_id=collective, has_side_effects=True
        ),
        cost_estimate=pl.CostEstimate(flops=0, bytes_accessed=60_000_000, transcendentals=0),
        name="share_keys",
    )(own)


def return_kernel(n, partial, out, near, summed, far, near_s, near_r, far_s, far_r):
    ctx = lax.axis_index("ctx")
    me = lax.axis_index("fsdp")
    which = me % 2
    partner = me + 1 - 2 * which
    others = [(ctx + k) % n for k in range(1, n)]
    greet([(ctx, partner)] + [(o, me) for o in others])
    order = others + [ctx]
    first = []
    for k, target in enumerate(order):
        copy = remote(partial.at[target, 1 - which], near.at[k], near_s.at[k], near_r.at[k], (ctx, partner))
        copy.start()
        first.append(copy)
    second = []

    def post(k):
        copy = remote(summed.at[k], far.at[k], far_s.at[k], far_r.at[k], (others[k], me))
        copy.start()
        second.append(copy)

    for k in range(n - 1):
        first[k].wait()
        summed[k] = (partial[others[k], which].astype(F32) + near[k].astype(F32)).astype(BF16)
        if k:
            post(k - 1)
    post(n - 2)
    out[1 - which] = jnp.zeros(out.shape[1:], F32)
    first[n - 1].wait()
    out[which] = partial[ctx, which].astype(F32) + near[n - 1].astype(F32)
    for k in range(n - 1):
        second[k].wait()
        out[which] += far[k].astype(F32)


def return_grads(partial, collective):
    n = partial.shape[0]
    block = partial.shape[2:]
    dma = pltpu.SemaphoreType.DMA
    return pl.pallas_call(
        functools.partial(return_kernel, n),
        out_shape=jax.ShapeDtypeStruct(partial.shape[1:], F32),
        in_specs=in_vmem(1),
        out_specs=in_vmem(1)[0],
        scratch_shapes=[
            pltpu.VMEM((n,) + block, BF16),
            pltpu.VMEM((n - 1,) + block, BF16),
            pltpu.VMEM((n - 1,) + block, BF16),
            dma((n,)),
            dma((n,)),
            dma((n - 1,)),
            dma((n - 1,)),
        ],
        compiler_params=pltpu.CompilerParams(
            vmem_limit_bytes=VMEM_LIMIT, collective_id=collective, has_side_effects=True
        ),
        cost_estimate=pl.CostEstimate(flops=0, bytes_accessed=80_000_000, transcendentals=0),
        name="return_grads",
    )(partial)


def vector_kernel(n_ctx, n, parts, out, near, summed, far, near_s, near_r, far_s, far_r):
    ctx = lax.axis_index("ctx")
    me = lax.axis_index("fsdp")
    members = [(me + k) % n for k in range(1, n)]
    others = [(ctx + k) % n_ctx for k in range(1, n_ctx)]
    greet([(ctx, m) for m in members] + [(o, me) for o in others])
    first = []
    for k in range(n - 1):
        copy = remote(parts.at[members[k]], near.at[k], near_s.at[k], near_r.at[k], (ctx, members[k]))
        copy.start()
        first.append(copy)
    total = parts[me]
    for k in range(n - 1):
        first[k].wait()
        total += near[k]
    summed[...] = total
    second = []
    for k in range(n_ctx - 1):
        copy = remote(summed, far.at[k], far_s.at[k], far_r.at[k], (others[k], me))
        copy.start()
        second.append(copy)
    for k in range(n_ctx - 1):
        second[k].wait()
        total += far[k]
    out[...] = total


def vector_sum(parts, n_ctx, collective):
    n = parts.shape[0]
    block = parts.shape[1:]
    dma = pltpu.SemaphoreType.DMA
    return pl.pallas_call(
        functools.partial(vector_kernel, n_ctx, n),
        out_shape=jax.ShapeDtypeStruct(block, F32),
        in_specs=in_vmem(1),
        out_specs=in_vmem(1)[0],
        scratch_shapes=[
            pltpu.VMEM((n - 1,) + block, F32),
            pltpu.VMEM(block, F32),
            pltpu.VMEM((n_ctx - 1,) + block, F32),
            dma((n - 1,)),
            dma((n - 1,)),
            dma((n_ctx - 1,)),
            dma((n_ctx - 1,)),
        ],
        compiler_params=pltpu.CompilerParams(
            vmem_limit_bytes=VMEM_LIMIT, collective_id=collective, has_side_effects=True
        ),
        cost_estimate=pl.CostEstimate(flops=0, bytes_accessed=30_000_000, transcendentals=0),
        name="vector_sum",
    )(parts)


def ring_pairs(n, step):
    return [(ring_index(p, n), ring_index((p + step) % n, n)) for p in range(n)]


def ring_begin(chunks, take, step):
    n = lax.axis_size("ctx")
    place = ring_place(lax.axis_index("ctx"), n)
    return take(chunks, (place + n - step) % n)


def ring_send(held, step):
    pairs = ring_pairs(lax.axis_size("ctx"), step)
    return jax.tree.map(lambda a: lax.ppermute(a, "ctx", pairs), held)


def ring_add(arrived, chunks, take, step, hop):
    n = lax.axis_size("ctx")
    place = ring_place(lax.axis_index("ctx"), n)
    mine = take(chunks, (place + n * n - step * (hop + 1)) % n)
    return jax.tree.map(lambda a, b: (a.astype(F32) + b.astype(F32)).astype(BF16), arrived, mine)


class RingSum:
    def __init__(self, right, left, take):
        self.sides = [(right, 1), (left, -1)]
        self.take = take
        self.held = [ring_begin(chunks, take, step) for chunks, step in self.sides]
        self.hop = 0
        self.hops = lax.axis_size("ctx") - 1

    def beside(self, *values):
        if self.hop == self.hops:
            return values
        self.hop += 1
        arrived = [ring_send(h, step) for h, (_, step) in zip(self.held, self.sides)]
        if values:
            arrived, *values = together(arrived, *values)
        self.held = [
            ring_add(a, chunks, self.take, step, self.hop)
            for a, (chunks, step) in zip(arrived, self.sides)
        ]
        return values

    def finish(self):
        while self.hop < self.hops:
            self.beside()
        return self.held


def ring_gather(own, halves, joined):
    n = lax.axis_size("ctx")
    place = ring_place(lax.axis_index("ctx"), n)
    out = jnp.zeros((n,) + own.shape, F32)

    def put(out, block, q):
        return lax.dynamic_update_index_in_dim(out, block.astype(F32), q % n, 0)

    out = put(out, own, place)
    right = left = own
    for hop in range(1, n // 2):
        right = lax.ppermute(right, "ctx", ring_pairs(n, 1))
        out = put(out, right, place + n - hop)
        left = lax.ppermute(left, "ctx", ring_pairs(n, -1))
        out = put(out, left, place + hop)
    right = lax.ppermute(halves(right)[0], "ctx", ring_pairs(n, 1))
    left = lax.ppermute(halves(left)[1], "ctx", ring_pairs(n, -1))
    return put(out, joined(right, left), place + n // 2)


def exchange(pieces, axis):
    return lax.all_to_all(pieces, axis, split_axis=0, concat_axis=0, tiled=True)


def together(*values):
    return lax.optimization_barrier(values)


def body(tokens, pairing, gain_attn, w_qkv, b_qkv, w_out, gain_mlp, w_gate_up, w_down, cotangent):
    half_rows = tokens.shape[2]
    n_ctx = lax.axis_size("ctx")
    n_fsdp = lax.axis_size("fsdp")
    ctx_index = lax.axis_index("ctx")
    fsdp_index = lax.axis_index("fsdp")
    stretch_len = half_rows * n_fsdp
    rows = 2 * stretch_len
    local_count = 2 * half_rows
    q_width = HEADS * HEAD_DIM
    kv_width = KV_HEADS * HEAD_DIM
    heads = HEADS // n_fsdp
    q_cols = heads * HEAD_DIM
    d_shard = w_qkv.shape[0]
    ff_shard = w_down.shape[0]

    owner_range = jnp.arange(n_ctx, dtype=jnp.int32)
    own_first = jnp.sum(jnp.where(owner_range == ctx_index, pairing, 0))
    ids = jnp.stack([own_first, 2 * n_ctx - 1 - own_first])
    inverse_pair = jnp.sum(
        owner_range[:, None] * (pairing[:, None] == owner_range[None, :]).astype(jnp.int32), 0
    )
    table = jnp.concatenate([2 * inverse_pair, 2 * inverse_pair[::-1] + 1])
    position = (
        ids[:, None] * stretch_len + jnp.arange(stretch_len, dtype=jnp.int32)[None, :]
    ).reshape(rows)
    kv_of = [f * KV_HEADS // n_fsdp for f in range(n_fsdp)]
    my_kv = fsdp_index * KV_HEADS // n_fsdp

    small = lax.all_gather(jnp.concatenate([gain_attn, gain_mlp, b_qkv]), "fsdp", axis=0)
    small, w_qkv, w_gate_up = together(small, w_qkv, w_gate_up)
    gain_one = small[:, :d_shard].reshape(D).astype(F32)
    gain_two = small[:, d_shard : 2 * d_shard].reshape(D).astype(F32)
    bias = small[:, 2 * d_shard :].reshape(-1).astype(F32)
    x_all = lax.all_gather(tokens[0], "fsdp", axis=1, tiled=True).reshape(rows, D)
    qkv_pieces = jnp.stack(
        [
            jnp.concatenate(
                [
                    w_qkv[:, f * q_cols : (f + 1) * q_cols],
                    w_qkv[:, q_width + kv_of[f] * HEAD_DIM : q_width + (kv_of[f] + 1) * HEAD_DIM],
                    w_qkv[
                        :,
                        q_width + kv_width + kv_of[f] * HEAD_DIM : q_width
                        + kv_width
                        + (kv_of[f] + 1) * HEAD_DIM,
                    ],
                ],
                1,
            )
            for f in range(n_fsdp)
        ]
    )
    w_qkv_cols = exchange(qkv_pieces, "fsdp").reshape(D, -1)
    bias_cols = jnp.concatenate(
        [
            lax.dynamic_slice_in_dim(bias, fsdp_index * q_cols, q_cols),
            lax.dynamic_slice_in_dim(bias, q_width + my_kv * HEAD_DIM, HEAD_DIM),
            lax.dynamic_slice_in_dim(bias, q_width + kv_width + my_kv * HEAD_DIM, HEAD_DIM),
        ]
    )
    gate_up_pieces = [
        w_gate_up[:, e].reshape(d_shard, n_fsdp, ff_shard).transpose(1, 0, 2) for e in range(2)
    ]
    x_all, w_qkv_cols, gate_up_pieces = together(x_all, w_qkv_cols, gate_up_pieces)
    w_gate_cols, w_up_cols = (
        exchange(pieces, "fsdp").reshape(D, ff_shard) for pieces in gate_up_pieces
    )
    cot_all = lax.all_gather(cotangent[0], "fsdp", axis=1, tiled=True).reshape(rows, D)

    x32 = x_all.astype(F32)
    normed1 = (x32 * rms_scale(x32) * gain_one).astype(BF16)
    qkv = jnp.dot(normed1, w_qkv_cols, preferred_element_type=F32) + bias_cols
    cosines, sines = rope_tables(position)
    rotated = rotate(
        qkv[:, : q_cols + HEAD_DIM].reshape(rows, heads + 1, HEAD_DIM), cosines, sines
    ).astype(BF16)
    query = rotated[:, :heads].reshape(2, stretch_len, q_cols)
    own_kv = jnp.concatenate([rotated[:, heads], qkv[:, q_cols + HEAD_DIM :].astype(BF16)], 1)
    keys_values = share_keys(own_kv.reshape(2, stretch_len, 2 * HEAD_DIM), n_ctx, 4)
    keys_values = keys_values.reshape(n_ctx * rows, 2 * HEAD_DIM)
    attended, lse = attend(table, ids, query, keys_values, heads)
    attended16 = attended.reshape(rows, q_cols)

    def scatter(partial):
        return lax.psum_scatter(
            partial.astype(BF16).reshape(2, stretch_len, D), "fsdp", scatter_dimension=1, tiled=True
        ).astype(F32).reshape(local_count, D)

    def by_member(partial):
        return partial.astype(BF16).reshape(2, n_fsdp, half_rows, D)

    tokens_own = tokens[0]
    hidden, normed2 = group_sum(
        "attention",
        by_member(jnp.dot(attended16, w_out, preferred_element_type=F32)),
        tokens_own,
        gain_two[None],
        collective=1,
    )
    normed2 = normed2.reshape(rows, D)
    gate_val = jnp.dot(normed2, w_gate_cols, preferred_element_type=F32)
    up_val = jnp.dot(normed2, w_up_cols, preferred_element_type=F32)
    sigmoid_gate = jax.nn.sigmoid(gate_val)
    act16 = (jax.nn.silu(gate_val) * up_val).astype(BF16)
    result = hidden.reshape(local_count, D) + scatter(jnp.dot(act16, w_down, preferred_element_type=F32))
    block_output = result.astype(BF16).reshape(tokens.shape)

    d_act = contract_cols(cot_all, w_down)
    d_gate16 = (d_act * up_val * sigmoid_gate * (1.0 + gate_val * (1.0 - sigmoid_gate))).astype(BF16)
    d_up16 = (d_act * gate_val * sigmoid_gate).astype(BF16)
    d_normed2 = contract_cols(d_gate16, w_gate_cols) + contract_cols(d_up16, w_up_cols)
    def by_columns(pieces):
        queries = [pieces[f][..., :q_cols] for f in range(n_fsdp)]
        rest = []
        for part in range(2):
            lo = q_cols + part * HEAD_DIM
            for g in range(KV_HEADS):
                rest.append(
                    sum(
                        pieces[f][..., lo : lo + HEAD_DIM].astype(F32)
                        for f in range(n_fsdp)
                        if kv_of[f] == g
                    ).astype(pieces[0].dtype)
                )
        return jnp.concatenate(queries + rest, -1)

    chunk_rows = d_shard // n_ctx
    down_rows = -(-ff_shard // (16 * n_ctx)) * 16
    side = D // 2

    def padded(grad):
        extra = n_ctx * down_rows - grad.shape[0]
        return jnp.pad(grad, ((0, extra), (0, 0))).astype(BF16).reshape(n_ctx, down_rows, D)

    d_w_down = padded(contract_rows(act16, cot_all))
    d_w_gate, d_w_up = (
        contract_rows(normed2, piece).astype(BF16).reshape(n_fsdp, n_ctx, chunk_rows, ff_shard)
        for piece in (d_gate16, d_up16)
    )

    def take(arrays, q):
        return (
            lax.dynamic_index_in_dim(arrays[0], q, 1, keepdims=False),
            lax.dynamic_index_in_dim(arrays[1], q, 0, keepdims=False),
        )

    mlp_ring = RingSum((d_w_gate, d_w_down[..., :side]), (d_w_up, d_w_down[..., side:]), take)
    d_hidden, dh_all, d_gain_two = group_sum(
        "mlp", by_member(d_normed2), hidden, cotangent[0], gain_two[None], collective=2
    )
    d_hidden, dh_all, d_gain_two = mlp_ring.beside(d_hidden, dh_all, d_gain_two)
    dh_all = dh_all.reshape(rows, D)
    d_attended16 = contract_cols(dh_all, w_out).astype(BF16).reshape(2, stretch_len, q_cols)
    d_query, d_kv = attend_back(
        table, ids, query, keys_values, attended, d_attended16, lse, heads
    )
    d_query, d_kv = mlp_ring.beside(d_query, d_kv)
    d_kv_own = return_grads(d_kv.reshape(n_ctx, 2, stretch_len, 2 * HEAD_DIM), 5).reshape(rows, -1)
    d_kv_own, d_query = mlp_ring.beside(d_kv_own, d_query)

    d_w_out = contract_rows(attended16, dh_all).astype(BF16).reshape(n_ctx, chunk_rows, D)
    d_rotated = jnp.concatenate([d_query.reshape(rows, q_cols), d_kv_own[:, :HEAD_DIM]], 1)
    d_rotated = unrotate(
        d_rotated.reshape(rows, heads + 1, HEAD_DIM), cosines, sines
    ).reshape(rows, q_cols + HEAD_DIM)
    d_qkv = jnp.concatenate([d_rotated, d_kv_own[:, HEAD_DIM:]], 1)
    d_bias = jnp.sum(d_qkv, 0)
    d_qkv16 = d_qkv.astype(BF16)
    d_normed1 = by_member(contract_cols(d_qkv16, w_qkv_cols))
    d_normed1, d_qkv16, d_bias = mlp_ring.beside(d_normed1, d_qkv16, d_bias)
    d_tokens, d_gain_one = group_sum(
        "input",
        d_normed1,
        tokens_own,
        d_hidden,
        gain_one[None],
        collective=3,
    )
    d_tokens, d_gain_one = mlp_ring.beside(d_tokens, d_gain_one)
    d_tokens = d_tokens.reshape(tokens.shape)

    zeros = jnp.zeros_like(d_bias)
    d_bias_full = by_columns([jnp.where(fsdp_index == f, d_bias, zeros) for f in range(n_fsdp)])
    parts = jnp.concatenate(
        [v.reshape(n_fsdp, -1, HEAD_DIM) for v in (d_gain_one, d_gain_two, d_bias_full)], 1
    )
    parts = jnp.pad(parts, ((0, 0), (0, -parts.shape[1] % 8), (0, 0)))
    vector = vector_sum(parts, n_ctx, 6)
    d_w_qkv = contract_rows(normed1, d_qkv16).astype(BF16).reshape(n_fsdp, n_ctx, chunk_rows, -1)
    vector, d_w_qkv, d_w_out = mlp_ring.beside(vector, d_w_qkv, d_w_out)
    vector = vector.reshape(-1)
    (gate_sum, down_left), (up_sum, down_right) = mlp_ring.finish()
    gate_sum, up_sum, d_w_qkv, d_w_out = together(gate_sum, up_sum, d_w_qkv, d_w_out)
    gate_up_sum = exchange(jnp.stack([gate_sum, up_sum], 1), "fsdp")
    gate_up_sum = gate_up_sum.transpose(2, 1, 0, 3).reshape(chunk_rows, 2, n_fsdp * ff_shard)

    def halves(block):
        middle = block.shape[-1] // 2
        return block[..., :middle], block[..., middle:]

    def joined(first, second):
        return jnp.concatenate([first, second], -1)

    d_w_gate_up = ring_gather(gate_up_sum, halves, joined).reshape(d_shard, 2, n_fsdp * ff_shard)
    d_w_down = ring_gather(joined(down_left, down_right), halves, joined)
    d_w_down = d_w_down.reshape(n_ctx * down_rows, D)[:ff_shard]

    ring = RingSum(
        (d_w_qkv[..., :q_cols], d_w_out[..., :side]), (d_w_qkv[..., q_cols:], d_w_out[..., side:]), take
    )
    (q_sum, out_left), (kv_sum, out_right) = ring.finish()
    d_w_pieces = exchange(joined(q_sum, kv_sum), "fsdp")

    qkv_sum = by_columns([d_w_pieces[f] for f in range(n_fsdp)])
    attention_sum = ring_gather(
        jnp.concatenate([qkv_sum, joined(out_left, out_right)], -1), halves, joined
    ).reshape(d_shard, -1)
    d_w_qkv, d_w_out = attention_sum[:, :-D], attention_sum[:, -D:]

    d_gain_attn = vector[:d_shard]
    d_gain_mlp = vector[d_shard : 2 * d_shard]
    d_b_qkv = vector[2 * d_shard : 2 * d_shard + b_qkv.shape[0]]

    return (
        block_output,
        d_tokens,
        d_gain_attn,
        d_w_qkv,
        d_b_qkv,
        d_w_out,
        d_gain_mlp,
        d_w_gate_up,
        d_w_down,
    )


def solution(mesh):
    placed = (
        P("ctx", None, "fsdp", None),
        P(),
        P("fsdp"),
        P("fsdp", None),
        P("fsdp"),
        P("fsdp", None),
        P("fsdp"),
        P("fsdp", None, None),
        P("fsdp", None),
        P("ctx", None, "fsdp", None),
    )
    return jax.shard_map(
        body,
        mesh=mesh,
        in_specs=placed,
        out_specs=(
            P("ctx", None, "fsdp", None),
            P("ctx", None, "fsdp", None),
            P("fsdp"),
            P("fsdp", None),
            P("fsdp"),
            P("fsdp", None),
            P("fsdp"),
            P("fsdp", None, None),
            P("fsdp", None),
        ),
        check_vma=False,
    )
```

```python
import functools

import jax
import jax.numpy as jnp
from jax import lax
from jax.experimental import pallas as pl
from jax.experimental.pallas import tpu as pltpu
from jax.sharding import PartitionSpec as P

D = 1536
HEADS = 12
KV_HEADS = 2
HEAD_DIM = 128

eps = 1e-06
rope_base = 1000000.0
F32 = jnp.float32
BF16 = jnp.bfloat16
VMEM_LIMIT = 60 * 1024 * 1024


def rope_tables(position):
    half = HEAD_DIM // 2
    inverse = rope_base ** (-(jnp.arange(half, dtype=F32) * 2.0 / HEAD_DIM))
    angle = position.astype(F32)[:, None] * inverse[None, :]
    return (jnp.cos(angle)[:, None, :], jnp.sin(angle)[:, None, :])


def rotate(vectors, cosines, sines):
    half = HEAD_DIM // 2
    first, second = (vectors[..., :half], vectors[..., half:])
    return jnp.concatenate([first * cosines - second * sines, second * cosines + first * sines], -1)


def unrotate(grads, cosines, sines):
    half = HEAD_DIM // 2
    first, second = (grads[..., :half], grads[..., half:])
    return jnp.concatenate([first * cosines + second * sines, second * cosines - first * sines], -1)


def rms_scale(values):
    return lax.rsqrt(jnp.mean(values * values, -1, keepdims=True) + eps)


def rms_backward(values, scale_rows, gain, d_normed):
    d_gain = jnp.sum(d_normed * values * scale_rows, 0)
    d_inner = d_normed * gain
    d_values = scale_rows * d_inner - values * scale_rows**3 * jnp.mean(
        d_inner * values, -1, keepdims=True
    )
    return (d_values, d_gain)


def dot(left, right, contract):
    return lax.dot_general(left, right, (contract, ((), ())), preferred_element_type=F32)


def contract_rows(left, right):
    return dot(left, right, ((0,), (0,)))


def contract_cols(left, right):
    return dot(left, right, ((1,), (1,)))


def stacked_heads(ref, which, heads):
    return jnp.concatenate(
        [ref[which, :, h * HEAD_DIM : (h + 1) * HEAD_DIM] for h in range(heads)], 0
    )


def causal(block_len, heads):
    keys = lax.broadcasted_iota(jnp.int32, (block_len, block_len), 0)
    queries = lax.broadcasted_iota(jnp.int32, (block_len, block_len), 1)
    return jnp.concatenate([keys <= queries] * heads, 1)


def attend_kernel(heads, table, ids, q_ref, kv_ref, o_ref, lse_ref):
    block_len = q_ref.shape[1]
    cols = heads * block_len
    scale = HEAD_DIM ** (-0.5)
    for which in range(2):
        last = ids[which]
        query = stacked_heads(q_ref, which, heads)

        def step(block, carry, masked=False):
            highest, total, acc = carry
            start = pl.multiple_of(table[block] * block_len, block_len)
            key = kv_ref[pl.ds(start, block_len), :HEAD_DIM]
            value = kv_ref[pl.ds(start, block_len), HEAD_DIM:]
            scores = contract_cols(key, query) * scale
            if masked:
                scores = jnp.where(causal(block_len, heads), scores, -1e30)
            new_high = jnp.maximum(highest, jnp.max(scores, 0, keepdims=True))
            probs = jnp.exp(scores - new_high)
            fade = jnp.exp(highest - new_high)
            total = total * fade + jnp.sum(probs, 0, keepdims=True)
            acc = acc * fade + contract_rows(value, probs.astype(BF16))
            return (new_high, total, acc)

        begin = (
            jnp.full((1, cols), -1e30, F32),
            jnp.zeros((1, cols), F32),
            jnp.zeros((HEAD_DIM, cols), F32),
        )
        carry = lax.fori_loop(0, last, step, begin)
        highest, total, acc = step(last, carry, True)
        lse_ref[which] = highest + jnp.log(total)
        out = (acc / total).T
        for h in range(heads):
            o_ref[which, :, h * HEAD_DIM : (h + 1) * HEAD_DIM] = out[
                h * block_len : (h + 1) * block_len
            ].astype(BF16)


def attend_back_kernel(
    heads, table, ids, q_ref, kv_ref, o_ref, do_ref, lse_ref, dq_ref, dkv_ref, sums
):
    block_len = q_ref.shape[1]
    cols = heads * block_len
    scale = HEAD_DIM ** (-0.5)
    sums[...] = jnp.zeros_like(sums)
    for which in range(2):
        last = ids[which]
        query = stacked_heads(q_ref, which, heads)
        d_out = stacked_heads(do_ref, which, heads)
        out = stacked_heads(o_ref, which, heads)
        delta = jnp.sum((d_out.astype(F32) * out.astype(F32)).T, 0, keepdims=True)
        lse = lse_ref[which]

        def step(block, d_query, masked=False):
            start = pl.multiple_of(table[block] * block_len, block_len)
            key = kv_ref[pl.ds(start, block_len), :HEAD_DIM]
            value = kv_ref[pl.ds(start, block_len), HEAD_DIM:]
            scores = contract_cols(key, query) * scale
            probs = jnp.exp(scores - lse)
            if masked:
                probs = jnp.where(causal(block_len, heads), probs, 0.0)
            d_probs = contract_cols(value, d_out)
            d_scores = (probs * (d_probs - delta)).astype(BF16)
            sums[pl.ds(start, block_len), :HEAD_DIM] += dot(d_scores, query, ((1,), (0,)))
            sums[pl.ds(start, block_len), HEAD_DIM:] += dot(
                probs.astype(BF16), d_out, ((1,), (0,))
            )
            return d_query + contract_rows(key, d_scores)

        d_query = lax.fori_loop(0, last, step, jnp.zeros((HEAD_DIM, cols), F32))
        d_query = step(last, d_query, True)
        d_query = (d_query * scale).T
        for h in range(heads):
            dq_ref[which, :, h * HEAD_DIM : (h + 1) * HEAD_DIM] = d_query[
                h * block_len : (h + 1) * block_len
            ]
    dkv_ref[:, :HEAD_DIM] = (sums[:, :HEAD_DIM] * scale).astype(BF16)
    dkv_ref[:, HEAD_DIM:] = sums[:, HEAD_DIM:].astype(BF16)


def in_vmem(count):
    return [pl.BlockSpec(memory_space=pltpu.VMEM)] * count


def in_smem(count):
    return [pl.BlockSpec(memory_space=pltpu.SMEM)] * count


def attend(table, ids, query, keys_values, heads):
    _, block_len, width = query.shape
    tall = keys_values.shape[0]
    return pl.pallas_call(
        functools.partial(attend_kernel, heads),
        out_shape=(
            jax.ShapeDtypeStruct(query.shape, BF16),
            jax.ShapeDtypeStruct((2, 1, heads * block_len), F32),
        ),
        in_specs=in_smem(2) + in_vmem(2),
        out_specs=tuple(in_vmem(2)),
        compiler_params=pltpu.CompilerParams(vmem_limit_bytes=VMEM_LIMIT),
        cost_estimate=pl.CostEstimate(
            flops=2 * tall * block_len * width * 2,
            bytes_accessed=tall * 512,
            transcendentals=tall * heads * block_len,
        ),
        name="attend",
    )(table, ids, query, keys_values)


def attend_back(table, ids, query, keys_values, out, d_out, lse, heads):
    _, block_len, width = query.shape
    tall = keys_values.shape[0]
    return pl.pallas_call(
        functools.partial(attend_back_kernel, heads),
        out_shape=(
            jax.ShapeDtypeStruct(query.shape, F32),
            jax.ShapeDtypeStruct(keys_values.shape, BF16),
        ),
        in_specs=in_smem(2) + in_vmem(5),
        out_specs=tuple(in_vmem(2)),
        scratch_shapes=[pltpu.VMEM(keys_values.shape, F32)],
        compiler_params=pltpu.CompilerParams(vmem_limit_bytes=VMEM_LIMIT),
        cost_estimate=pl.CostEstimate(
            flops=5 * tall * block_len * width * 2,
            bytes_accessed=tall * 1024,
            transcendentals=tall * heads * block_len,
        ),
        name="attend_back",
    )(table, ids, query, keys_values, out, d_out, lse)


MESH = pl.DeviceIdType.MESH


def greet(devices):
    barrier = pltpu.get_barrier_semaphore()
    for device in devices:
        pl.semaphore_signal(barrier, inc=1, device_id=device, device_id_type=MESH)
    pl.semaphore_wait(barrier, len(devices))


def remote(src, dst, send, recv, device):
    return pltpu.make_async_remote_copy(
        src_ref=src, dst_ref=dst, send_sem=send, recv_sem=recv, device_id=device, device_id_type=MESH
    )


def group_places(n):
    ctx = lax.axis_index("ctx")
    me = lax.axis_index("fsdp")
    partner = me + 1 - 2 * (me % 2)
    others = [(me + 2 * k) % n for k in range(1, n // 2)]
    senders = [(me + n - 2 * k) % n for k in range(1, n // 2)]
    return ctx, me, partner, others, senders


def sum_kernel(mode, n, cuts, *refs):
    gathers = mode != "input"
    if mode == "attention":
        partial, tokens, gain, hidden_out, all_out = refs[:5]
    elif mode == "mlp":
        partial, hidden_in, cot, gain, d_out, all_out, d_gain = refs[:7]
    else:
        partial, tokens, d_hidden_in, gain, d_out, d_gain = refs[:6]
    near, summed, far, stage, near_s, near_r, far_s, far_r, own_s, own_r, out_s, out_r, fwd_s, fwd_r = refs[-14:]
    ctx, me, partner, others, senders = group_places(n)
    chips = n // 2
    rows = partial.shape[2]
    piece = rows // cuts
    chunks = [(w, i * piece) for w in range(2) for i in range(cuts)]
    greet([(ctx, partner)] + [(ctx, o) for o in others])

    def part(ref, w, lead, start):
        return ref.at[w, lead, pl.ds(start, piece)]

    first = []
    for c, (w, start) in enumerate(chunks):
        for j in range(chips):
            target = (partner + 2 * (j + 1)) % n
            copy = remote(
                part(partial, w, target, start),
                part(near, w, j, start),
                near_s.at[c, j],
                near_r.at[c, j],
                (ctx, partner),
            )
            copy.start()
            first.append(copy)

    second = []

    def post(c):
        w, start = chunks[c]
        for j in range(chips - 1):
            copy = remote(
                part(summed, w, j, start),
                part(far, w, j, start),
                far_s.at[c, j],
                far_r.at[c, j],
                (ctx, others[j]),
            )
            copy.start()
            second.append(copy)

    for c, (w, start) in enumerate(chunks):
        span = pl.ds(start, piece)
        for j in range(chips - 1):
            first[c * chips + j].wait()
            target = (me + 2 * (j + 1)) % n
            summed[w, j, span] = (
                partial[w, target, span].astype(F32) + near[w, j, span].astype(F32)
            ).astype(BF16)
        if c:
            post(c - 1)
    post(len(chunks) - 1)

    if mode != "attention":
        d_gain[...] = jnp.zeros_like(d_gain)
    third = []

    def spread(c):
        w, start = chunks[c]
        src = stage.at[w, pl.ds(start, piece)]
        for k in range(chips - 1):
            copy = remote(src, part(all_out, w, me, start), out_s.at[c, k], out_r.at[c, k], (ctx, others[k]))
            copy.start()
            third.append(copy)
        copy = remote(src, part(all_out, w, me, start), own_s.at[c], own_r.at[c], (ctx, partner))
        copy.start()
        return copy

    near_copies = []
    for c, (w, start) in enumerate(chunks):
        span = pl.ds(start, piece)
        first[c * chips + chips - 1].wait()
        total = partial[w, me, span].astype(F32) + near[w, chips - 1, span].astype(F32)
        for j in range(chips - 1):
            second[c * (chips - 1) + j].wait()
            total += far[w, j, span].astype(F32)
        if mode == "attention":
            hidden = tokens[w, span].astype(F32) + total
            hidden_out[w, span] = hidden
            rounded = (hidden * rms_scale(hidden) * gain[...]).astype(BF16)
        elif mode == "mlp":
            hidden = hidden_in[w, span]
            d_norm, gain_part = rms_backward(hidden, rms_scale(hidden), gain[...], total)
            d_gain[...] += gain_part[None]
            d_hidden = cot[w, span].astype(F32) + d_norm
            d_out[w, span] = d_hidden
            rounded = d_hidden.astype(BF16)
        else:
            values = tokens[w, span].astype(F32)
            d_norm, gain_part = rms_backward(values, rms_scale(values), gain[...], total)
            d_gain[...] += gain_part[None]
            d_out[w, span] = d_hidden_in[w, span] + d_norm
        if gathers:
            stage[w, span] = rounded
            all_out[w, me, span] = rounded
            if c:
                near_copies.append(spread(c - 1))
    if not gathers:
        return
    near_copies.append(spread(len(chunks) - 1))

    forwards = []
    for c, (w, start) in enumerate(chunks):
        for k in range(chips - 1):
            third[c * (chips - 1) + k].wait_recv()
            block = part(all_out, w, senders[k], start)
            copy = remote(block, block, fwd_s.at[c, k], fwd_r.at[c, k], (ctx, partner))
            copy.start()
            forwards.append(copy)
    for copy in third:
        copy.wait_send()
    for copy in near_copies + forwards:
        copy.wait()


def group_sum(mode, partial, *operands, collective):
    _, n, rows, width = partial.shape
    cuts = 2
    chunks = 2 * cuts
    chips = n // 2
    row_shape = (2, rows, width)
    full = jax.ShapeDtypeStruct(row_shape, F32)
    gathered = jax.ShapeDtypeStruct(partial.shape, BF16)
    gain_sum = jax.ShapeDtypeStruct((1, width), F32)
    out_shape = {
        "attention": (full, gathered),
        "mlp": (full, gathered, gain_sum),
        "input": (full, gain_sum),
    }[mode]
    dma = pltpu.SemaphoreType.DMA
    return pl.pallas_call(
        functools.partial(sum_kernel, mode, n, cuts),
        out_shape=out_shape,
        in_specs=in_vmem(1 + len(operands)),
        out_specs=tuple(in_vmem(len(out_shape))),
        scratch_shapes=[
            pltpu.VMEM((2, chips, rows, width), BF16),
            pltpu.VMEM((2, chips - 1, rows, width), BF16),
            pltpu.VMEM((2, chips - 1, rows, width), BF16),
            pltpu.VMEM(row_shape, BF16),
            dma((chunks, chips)),
            dma((chunks, chips)),
            dma((chunks, chips - 1)),
            dma((chunks, chips - 1)),
            dma((chunks,)),
            dma((chunks,)),
            dma((chunks, chips - 1)),
            dma((chunks, chips - 1)),
            dma((chunks, chips - 1)),
            dma((chunks, chips - 1)),
        ],
        compiler_params=pltpu.CompilerParams(
            vmem_limit_bytes=VMEM_LIMIT, collective_id=collective, has_side_effects=True
        ),
        cost_estimate=pl.CostEstimate(
            flops=20 * rows * width, bytes_accessed=60_000_000, transcendentals=0
        ),
        name="group_sum_" + mode,
    )(partial, *operands)


def ring_index(place, n):
    late = place // (n // 2)
    return (1 - late) * 2 * place + late * (2 * n - 1 - 2 * place)


def ring_place(index, n):
    odd = index % 2
    return (1 - odd) * (index // 2) + odd * (n - 1 - index // 2)


def share_kernel(n, own, out, right_s, right_r, left_s, left_r, near_s, near_r):
    ctx = lax.axis_index("ctx")
    me = lax.axis_index("fsdp")
    which = me % 2
    partner = me + 1 - 2 * which
    place = ring_place(ctx, n)
    right = (ring_index((place + 1) % n, n), me)
    left = (ring_index((place + n - 1) % n, n), me)
    greet([right, left, (ctx, partner)])

    def block(offset):
        return out.at[ring_index((place + n + offset) % n, n), which]

    def to_right(step):
        src = own.at[which] if step == 0 else block(-step)
        return remote(src, block(-step), right_s.at[step], right_r.at[step], right)

    def to_left(step):
        src = own.at[which] if step == 0 else block(step)
        return remote(src, block(step), left_s.at[step], left_r.at[step], left)

    rights, lefts = n // 2, n - 1 - n // 2
    sent = [to_right(0), to_left(0)]
    for copy in sent:
        copy.start()
    out[ctx] = own[...]
    going = [sent[0], sent[1]]
    for step in range(1, rights + 1):
        going[0].wait_recv()
        if step < rights:
            going[0] = to_right(step)
            going[0].start()
            sent.append(going[0])
        hand = remote(block(-step), block(-step), near_s.at[step - 1], near_r.at[step - 1], (ctx, partner))
        hand.start()
        sent.append(hand)
        if step <= lefts:
            going[1].wait_recv()
            if step < lefts:
                going[1] = to_left(step)
                going[1].start()
                sent.append(going[1])
            slot = rights + step - 1
            hand = remote(block(step), block(step), near_s.at[slot], near_r.at[slot], (ctx, partner))
            hand.start()
            sent.append(hand)
    for copy in sent:
        copy.wait_send()
    for step in range(1, rights + 1):
        remote(block(-step), block(-step), near_s.at[step - 1], near_r.at[step - 1], (ctx, partner)).wait_recv()
    for step in range(1, lefts + 1):
        slot = rights + step - 1
        remote(block(step), block(step), near_s.at[slot], near_r.at[slot], (ctx, partner)).wait_recv()


def share_keys(own, n, collective):
    dma = pltpu.SemaphoreType.DMA
    return pl.pallas_call(
        functools.partial(share_kernel, n),
        out_shape=jax.ShapeDtypeStruct((n,) + own.shape, BF16),
        in_specs=in_vmem(1),
        out_specs=in_vmem(1)[0],
        scratch_shapes=[dma((n // 2,))] * 4 + [dma((n - 1,))] * 2,
        compiler_params=pltpu.CompilerParams(
            vmem_limit_bytes=VMEM_LIMIT, collective_id=collective, has_side_effects=True
        ),
        cost_estimate=pl.CostEstimate(flops=0, bytes_accessed=60_000_000, transcendentals=0),
        name="share_keys",
    )(own)


def return_kernel(n, partial, out, near, summed, far, near_s, near_r, far_s, far_r):
    ctx = lax.axis_index("ctx")
    me = lax.axis_index("fsdp")
    which = me % 2
    partner = me + 1 - 2 * which
    others = [(ctx + k) % n for k in range(1, n)]
    greet([(ctx, partner)] + [(o, me) for o in others])
    order = others + [ctx]
    first = []
    for k, target in enumerate(order):
        copy = remote(partial.at[target, 1 - which], near.at[k], near_s.at[k], near_r.at[k], (ctx, partner))
        copy.start()
        first.append(copy)
    second = []

    def post(k):
        copy = remote(summed.at[k], far.at[k], far_s.at[k], far_r.at[k], (others[k], me))
        copy.start()
        second.append(copy)

    for k in range(n - 1):
        first[k].wait()
        summed[k] = (partial[others[k], which].astype(F32) + near[k].astype(F32)).astype(BF16)
        if k:
            post(k - 1)
    post(n - 2)
    out[1 - which] = jnp.zeros(out.shape[1:], F32)
    first[n - 1].wait()
    out[which] = partial[ctx, which].astype(F32) + near[n - 1].astype(F32)
    for k in range(n - 1):
        second[k].wait()
        out[which] += far[k].astype(F32)


def return_grads(partial, collective):
    n = partial.shape[0]
    block = partial.shape[2:]
    dma = pltpu.SemaphoreType.DMA
    return pl.pallas_call(
        functools.partial(return_kernel, n),
        out_shape=jax.ShapeDtypeStruct(partial.shape[1:], F32),
        in_specs=in_vmem(1),
        out_specs=in_vmem(1)[0],
        scratch_shapes=[
            pltpu.VMEM((n,) + block, BF16),
            pltpu.VMEM((n - 1,) + block, BF16),
            pltpu.VMEM((n - 1,) + block, BF16),
            dma((n,)),
            dma((n,)),
            dma((n - 1,)),
            dma((n - 1,)),
        ],
        compiler_params=pltpu.CompilerParams(
            vmem_limit_bytes=VMEM_LIMIT, collective_id=collective, has_side_effects=True
        ),
        cost_estimate=pl.CostEstimate(flops=0, bytes_accessed=80_000_000, transcendentals=0),
        name="return_grads",
    )(partial)


def vector_kernel(n_ctx, n, parts, out, near, summed, far, near_s, near_r, far_s, far_r):
    ctx = lax.axis_index("ctx")
    me = lax.axis_index("fsdp")
    members = [(me + k) % n for k in range(1, n)]
    others = [(ctx + k) % n_ctx for k in range(1, n_ctx)]
    greet([(ctx, m) for m in members] + [(o, me) for o in others])
    first = []
    for k in range(n - 1):
        copy = remote(parts.at[members[k]], near.at[k], near_s.at[k], near_r.at[k], (ctx, members[k]))
        copy.start()
        first.append(copy)
    total = parts[me]
    for k in range(n - 1):
        first[k].wait()
        total += near[k]
    summed[...] = total
    second = []
    for k in range(n_ctx - 1):
        copy = remote(summed, far.at[k], far_s.at[k], far_r.at[k], (others[k], me))
        copy.start()
        second.append(copy)
    for k in range(n_ctx - 1):
        second[k].wait()
        total += far[k]
    out[...] = total


def vector_sum(parts, n_ctx, collective):
    n = parts.shape[0]
    block = parts.shape[1:]
    dma = pltpu.SemaphoreType.DMA
    return pl.pallas_call(
        functools.partial(vector_kernel, n_ctx, n),
        out_shape=jax.ShapeDtypeStruct(block, F32),
        in_specs=in_vmem(1),
        out_specs=in_vmem(1)[0],
        scratch_shapes=[
            pltpu.VMEM((n - 1,) + block, F32),
            pltpu.VMEM(block, F32),
            pltpu.VMEM((n_ctx - 1,) + block, F32),
            dma((n - 1,)),
            dma((n - 1,)),
            dma((n_ctx - 1,)),
            dma((n_ctx - 1,)),
        ],
        compiler_params=pltpu.CompilerParams(
            vmem_limit_bytes=VMEM_LIMIT, collective_id=collective, has_side_effects=True
        ),
        cost_estimate=pl.CostEstimate(flops=0, bytes_accessed=30_000_000, transcendentals=0),
        name="vector_sum",
    )(parts)


def ring_sum_kernel(n, plan, arrays, *refs):
    ins, outs = refs[:arrays], refs[arrays : 2 * arrays]
    refs = refs[2 * arrays :]
    count = len(plan)
    arrived, stages, sends, recvs = (refs[i * count : (i + 1) * count] for i in range(4))
    ctx = lax.axis_index("ctx")
    me = lax.axis_index("fsdp")
    place = ring_place(ctx, n)
    around = {step: (ring_index((place + n + step) % n, n), me) for step in (1, -1)}
    greet([around[1], around[-1]])

    def copy(i, hop, src):
        step = plan[i][3]
        return remote(src, arrived[i].at[hop], sends[i].at[hop], recvs[i].at[hop], around[step])

    def chunk(i, hop):
        step = plan[i][3]
        return ring_index((place + n * n - step * (hop + 1)) % n, n)

    def window(i, group, hop):
        which, low, high, _ = plan[i]
        return ins[which][group, chunk(i, hop), :, low:high].astype(F32)

    for i, (which, low, high, _) in enumerate(plan):
        copy(i, 0, ins[which].at[:, chunk(i, 0), :, pl.ds(low, high - low)]).start()

    def add(i, hop, store):
        copy(i, hop - 1, stages[i].at[0]).wait_recv()

        def group_add(group, carry):
            store(group, (arrived[i][hop - 1, group].astype(F32) + window(i, group, hop)).astype(BF16))
            return carry

        lax.fori_loop(0, ins[plan[i][0]].shape[0], group_add, 0)

    def one_hop(hop, carry):
        slot = hop % 2
        for i in range(count):
            @pl.when(hop > 2)
            def _():
                copy(i, hop - 2, stages[i].at[slot]).wait_send()

            def store(group, value):
                stages[i][slot, group] = value

            add(i, hop, store)
            if i:
                copy(i - 1, hop, stages[i - 1].at[slot]).start()
        copy(count - 1, hop, stages[count - 1].at[slot]).start()
        return carry

    lax.fori_loop(1, n - 1, one_hop, 0)
    for i, (which, low, high, _) in enumerate(plan):
        def store(group, value):
            outs[which][group, :, low:high] = value

        add(i, n - 1, store)
    for i, (which, low, high, _) in enumerate(plan):
        copy(i, 0, ins[which].at[:, chunk(i, 0), :, pl.ds(low, high - low)]).wait_send()
        for hop in (n - 3, n - 2):
            copy(i, hop, stages[i].at[hop % 2]).wait_send()


def ring_sum(arrays, plan, collective):
    n = arrays[0].shape[1]
    dma = pltpu.SemaphoreType.DMA
    blocks = [
        (arrays[which].shape[0], arrays[which].shape[2], high - low) for which, low, high, _ in plan
    ]
    return pl.pallas_call(
        functools.partial(ring_sum_kernel, n, plan, len(arrays)),
        out_shape=tuple(
            jax.ShapeDtypeStruct((a.shape[0],) + a.shape[2:], BF16) for a in arrays
        ),
        in_specs=in_vmem(len(arrays)),
        out_specs=tuple(in_vmem(len(arrays))),
        scratch_shapes=[pltpu.VMEM((n - 1,) + b, BF16) for b in blocks]
        + [pltpu.VMEM((2,) + b, BF16) for b in blocks]
        + [dma((n - 1,)) for _ in blocks] * 2,
        compiler_params=pltpu.CompilerParams(
            vmem_limit_bytes=VMEM_LIMIT, collective_id=collective, has_side_effects=True
        ),
        cost_estimate=pl.CostEstimate(flops=0, bytes_accessed=200_000_000, transcendentals=0),
        name="ring_sum",
    )(*arrays)


def ring_gather_kernel(n, own, out, sends, recvs):
    ctx = lax.axis_index("ctx")
    me = lax.axis_index("fsdp")
    place = ring_place(ctx, n)
    around = {step: (ring_index((place + n + step) % n, n), me) for step in (1, -1)}
    greet([around[1], around[-1]])
    middle = own.shape[-1] // 2
    far = n // 2

    def copy(step, half, hop):
        lanes = pl.ds(half * middle, middle)
        block = out.at[ring_index((place + n - step * hop) % n, n), :, lanes]
        src = block if hop else own.at[:, lanes]
        row = half if step == 1 else 2 + half
        return remote(src, block, sends.at[row, hop], recvs.at[row, hop], around[step])

    def hops(step, half):
        return far if (step == 1) == (half == 0) else far - 1

    lines = [(1, 0), (-1, 1), (1, 1), (-1, 0)]
    for step, half in lines:
        copy(step, half, 0).start()
    out[ctx] = own[...]
    for hop in range(1, far + 1):
        for step, half in lines:
            if hop <= hops(step, half):
                copy(step, half, hop - 1).wait_recv()
                if hop < hops(step, half):
                    copy(step, half, hop).start()
    for step, half in lines:
        for hop in range(hops(step, half)):
            copy(step, half, hop).wait_send()


def ring_gather(own, n, collective):
    dma = pltpu.SemaphoreType.DMA
    return pl.pallas_call(
        functools.partial(ring_gather_kernel, n),
        out_shape=jax.ShapeDtypeStruct((n,) + own.shape, BF16),
        in_specs=in_vmem(1),
        out_specs=in_vmem(1)[0],
        scratch_shapes=[dma((4, n // 2))] * 2,
        compiler_params=pltpu.CompilerParams(
            vmem_limit_bytes=VMEM_LIMIT, collective_id=collective, has_side_effects=True
        ),
        cost_estimate=pl.CostEstimate(flops=0, bytes_accessed=80_000_000, transcendentals=0),
        name="ring_gather",
    )(own)


def exchange(pieces, axis):
    return lax.all_to_all(pieces, axis, split_axis=0, concat_axis=0, tiled=True)


def together(*values):
    return lax.optimization_barrier(values)


def body(tokens, pairing, gain_attn, w_qkv, b_qkv, w_out, gain_mlp, w_gate_up, w_down, cotangent):
    half_rows = tokens.shape[2]
    n_ctx = lax.axis_size("ctx")
    n_fsdp = lax.axis_size("fsdp")
    ctx_index = lax.axis_index("ctx")
    fsdp_index = lax.axis_index("fsdp")
    stretch_len = half_rows * n_fsdp
    rows = 2 * stretch_len
    local_count = 2 * half_rows
    q_width = HEADS * HEAD_DIM
    kv_width = KV_HEADS * HEAD_DIM
    heads = HEADS // n_fsdp
    q_cols = heads * HEAD_DIM
    d_shard = w_qkv.shape[0]
    ff_shard = w_down.shape[0]

    owner_range = jnp.arange(n_ctx, dtype=jnp.int32)
    own_first = jnp.sum(jnp.where(owner_range == ctx_index, pairing, 0))
    ids = jnp.stack([own_first, 2 * n_ctx - 1 - own_first])
    inverse_pair = jnp.sum(
        owner_range[:, None] * (pairing[:, None] == owner_range[None, :]).astype(jnp.int32), 0
    )
    table = jnp.concatenate([2 * inverse_pair, 2 * inverse_pair[::-1] + 1])
    position = (
        ids[:, None] * stretch_len + jnp.arange(stretch_len, dtype=jnp.int32)[None, :]
    ).reshape(rows)
    kv_of = [f * KV_HEADS // n_fsdp for f in range(n_fsdp)]
    my_kv = fsdp_index * KV_HEADS // n_fsdp

    small = lax.all_gather(jnp.concatenate([gain_attn, gain_mlp, b_qkv]), "fsdp", axis=0)
    small, w_qkv, w_gate_up = together(small, w_qkv, w_gate_up)
    gain_one = small[:, :d_shard].reshape(D).astype(F32)
    gain_two = small[:, d_shard : 2 * d_shard].reshape(D).astype(F32)
    bias = small[:, 2 * d_shard :].reshape(-1).astype(F32)
    x_all = lax.all_gather(tokens[0], "fsdp", axis=1, tiled=True).reshape(rows, D)
    qkv_pieces = jnp.stack(
        [
            jnp.concatenate(
                [
                    w_qkv[:, f * q_cols : (f + 1) * q_cols],
                    w_qkv[:, q_width + kv_of[f] * HEAD_DIM : q_width + (kv_of[f] + 1) * HEAD_DIM],
                    w_qkv[
                        :,
                        q_width + kv_width + kv_of[f] * HEAD_DIM : q_width
                        + kv_width
                        + (kv_of[f] + 1) * HEAD_DIM,
                    ],
                ],
                1,
            )
            for f in range(n_fsdp)
        ]
    )
    w_qkv_cols = exchange(qkv_pieces, "fsdp").reshape(D, -1)
    bias_cols = jnp.concatenate(
        [
            lax.dynamic_slice_in_dim(bias, fsdp_index * q_cols, q_cols),
            lax.dynamic_slice_in_dim(bias, q_width + my_kv * HEAD_DIM, HEAD_DIM),
            lax.dynamic_slice_in_dim(bias, q_width + kv_width + my_kv * HEAD_DIM, HEAD_DIM),
        ]
    )
    gate_up_pieces = w_gate_up.reshape(d_shard, 2, n_fsdp, ff_shard).transpose(2, 1, 0, 3)
    x_all, w_qkv_cols, gate_up_pieces = together(x_all, w_qkv_cols, gate_up_pieces)
    gate_up_cols = exchange(gate_up_pieces, "fsdp")
    cot_all = lax.all_gather(cotangent[0], "fsdp", axis=1, tiled=True).reshape(rows, D)

    x32 = x_all.astype(F32)
    normed1 = (x32 * rms_scale(x32) * gain_one).astype(BF16)
    qkv = jnp.dot(normed1, w_qkv_cols, preferred_element_type=F32) + bias_cols
    cosines, sines = rope_tables(position)
    rotated = rotate(
        qkv[:, : q_cols + HEAD_DIM].reshape(rows, heads + 1, HEAD_DIM), cosines, sines
    ).astype(BF16)
    query = rotated[:, :heads].reshape(2, stretch_len, q_cols)
    own_kv = jnp.concatenate([rotated[:, heads], qkv[:, q_cols + HEAD_DIM :].astype(BF16)], 1)
    keys_values = share_keys(own_kv.reshape(2, stretch_len, 2 * HEAD_DIM), n_ctx, 4)
    keys_values = keys_values.reshape(n_ctx * rows, 2 * HEAD_DIM)
    attended, lse = attend(table, ids, query, keys_values, heads)
    attended16 = attended.reshape(rows, q_cols)

    def scatter(partial):
        return lax.psum_scatter(
            partial.astype(BF16).reshape(2, stretch_len, D), "fsdp", scatter_dimension=1, tiled=True
        ).astype(F32).reshape(local_count, D)

    def by_member(partial):
        return partial.astype(BF16).reshape(2, n_fsdp, half_rows, D)

    tokens_own = tokens[0]
    hidden, normed2 = group_sum(
        "attention",
        by_member(jnp.dot(attended16, w_out, preferred_element_type=F32)),
        tokens_own,
        gain_two[None],
        collective=1,
    )
    normed2 = normed2.reshape(rows, D)
    w_gate_cols, w_up_cols = (gate_up_cols[:, e].reshape(D, ff_shard) for e in range(2))
    gate_val = jnp.dot(normed2, w_gate_cols, preferred_element_type=F32)
    up_val = jnp.dot(normed2, w_up_cols, preferred_element_type=F32)
    sigmoid_gate = jax.nn.sigmoid(gate_val)
    act16 = (jax.nn.silu(gate_val) * up_val).astype(BF16)
    result = hidden.reshape(local_count, D) + scatter(jnp.dot(act16, w_down, preferred_element_type=F32))
    block_output = result.astype(BF16).reshape(tokens.shape)

    d_act = contract_cols(cot_all, w_down)
    d_gate16 = (d_act * up_val * sigmoid_gate * (1.0 + gate_val * (1.0 - sigmoid_gate))).astype(BF16)
    d_up16 = (d_act * gate_val * sigmoid_gate).astype(BF16)
    d_normed2 = contract_cols(d_gate16, w_gate_cols) + contract_cols(d_up16, w_up_cols)
    def by_columns(pieces):
        queries = [pieces[f][..., :q_cols] for f in range(n_fsdp)]
        rest = []
        for part in range(2):
            lo = q_cols + part * HEAD_DIM
            for g in range(KV_HEADS):
                rest.append(
                    sum(
                        pieces[f][..., lo : lo + HEAD_DIM].astype(F32)
                        for f in range(n_fsdp)
                        if kv_of[f] == g
                    ).astype(pieces[0].dtype)
                )
        return jnp.concatenate(queries + rest, -1)

    chunk_rows = d_shard // n_ctx
    down_rows = -(-ff_shard // (16 * n_ctx)) * 16
    side = D // 2

    def padded(grad):
        extra = n_ctx * down_rows - grad.shape[0]
        return jnp.pad(grad, ((0, extra), (0, 0))).astype(BF16).reshape(n_ctx, down_rows, D)

    d_w_down = padded(contract_rows(act16, cot_all))
    d_w_gate, d_w_up = (
        contract_rows(normed2, piece).astype(BF16).reshape(n_fsdp, n_ctx, chunk_rows, ff_shard)
        for piece in (d_gate16, d_up16)
    )

    gate_sum, up_sum, down_sum = ring_sum(
        (d_w_gate, d_w_up, d_w_down[None]),
        ((0, 0, ff_shard, 1), (1, 0, ff_shard, -1), (2, 0, side, 1), (2, side, D, -1)),
        7,
    )
    d_normed2, gate_sum, up_sum, down_sum = together(by_member(d_normed2), gate_sum, up_sum, down_sum)
    gate_up_sum = exchange(jnp.stack([gate_sum, up_sum], 1), "fsdp")
    gate_up_sum = gate_up_sum.transpose(2, 1, 0, 3).reshape(chunk_rows, 2, n_fsdp * ff_shard)
    d_w_gate_up = lax.all_gather(gate_up_sum, "ctx", axis=0, tiled=True).astype(F32)
    d_w_down = lax.all_gather(down_sum[0], "ctx", axis=0, tiled=True)[:ff_shard].astype(F32)
    d_hidden, dh_all, d_gain_two = group_sum(
        "mlp", d_normed2, hidden, cotangent[0], gain_two[None], collective=2
    )
    dh_all = dh_all.reshape(rows, D)
    d_attended16 = contract_cols(dh_all, w_out).astype(BF16).reshape(2, stretch_len, q_cols)
    d_query, d_kv = attend_back(
        table, ids, query, keys_values, attended, d_attended16, lse, heads
    )
    d_kv_own = return_grads(d_kv.reshape(n_ctx, 2, stretch_len, 2 * HEAD_DIM), 5).reshape(rows, -1)

    d_w_out = contract_rows(attended16, dh_all).astype(BF16).reshape(n_ctx, chunk_rows, D)
    d_rotated = jnp.concatenate([d_query.reshape(rows, q_cols), d_kv_own[:, :HEAD_DIM]], 1)
    d_rotated = unrotate(
        d_rotated.reshape(rows, heads + 1, HEAD_DIM), cosines, sines
    ).reshape(rows, q_cols + HEAD_DIM)
    d_qkv = jnp.concatenate([d_rotated, d_kv_own[:, HEAD_DIM:]], 1)
    d_bias = jnp.sum(d_qkv, 0)
    d_qkv16 = d_qkv.astype(BF16)
    d_normed1 = by_member(contract_cols(d_qkv16, w_qkv_cols))
    d_tokens, d_gain_one = group_sum(
        "input",
        d_normed1,
        tokens_own,
        d_hidden,
        gain_one[None],
        collective=3,
    )
    d_tokens = d_tokens.reshape(tokens.shape)

    zeros = jnp.zeros_like(d_bias)
    d_bias_full = by_columns([jnp.where(fsdp_index == f, d_bias, zeros) for f in range(n_fsdp)])
    parts = jnp.concatenate(
        [v.reshape(n_fsdp, -1, HEAD_DIM) for v in (d_gain_one, d_gain_two, d_bias_full)], 1
    )
    parts = jnp.pad(parts, ((0, 0), (0, -parts.shape[1] % 8), (0, 0)))
    vector = vector_sum(parts, n_ctx, 6)
    d_w_qkv = contract_rows(normed1, d_qkv16).astype(BF16).reshape(n_fsdp, n_ctx, chunk_rows, -1)
    vector = vector.reshape(-1)
    pieces, out_sum = ring_sum(
        (d_w_qkv, d_w_out[None]),
        ((0, 0, q_cols, 1), (0, q_cols, d_w_qkv.shape[-1], -1), (1, 0, side, 1), (1, side, D, -1)),
        8,
    )
    d_w_pieces = exchange(pieces, "fsdp")
    qkv_sum = by_columns([d_w_pieces[f] for f in range(n_fsdp)])
    attention_sum = ring_gather(jnp.concatenate([qkv_sum, out_sum[0]], -1), n_ctx, 9)
    attention_sum = attention_sum.reshape(d_shard, -1).astype(F32)
    d_w_qkv, d_w_out = attention_sum[:, :-D], attention_sum[:, -D:]

    d_gain_attn = vector[:d_shard]
    d_gain_mlp = vector[d_shard : 2 * d_shard]
    d_b_qkv = vector[2 * d_shard : 2 * d_shard + b_qkv.shape[0]]

    return (
        block_output,
        d_tokens,
        d_gain_attn,
        d_w_qkv,
        d_b_qkv,
        d_w_out,
        d_gain_mlp,
        d_w_gate_up,
        d_w_down,
    )


def solution(mesh):
    placed = (
        P("ctx", None, "fsdp", None),
        P(),
        P("fsdp"),
        P("fsdp", None),
        P("fsdp"),
        P("fsdp", None),
        P("fsdp"),
        P("fsdp", None, None),
        P("fsdp", None),
        P("ctx", None, "fsdp", None),
    )
    return jax.shard_map(
        body,
        mesh=mesh,
        in_specs=placed,
        out_specs=(
            P("ctx", None, "fsdp", None),
            P("ctx", None, "fsdp", None),
            P("fsdp"),
            P("fsdp", None),
            P("fsdp"),
            P("fsdp", None),
            P("fsdp"),
            P("fsdp", None, None),
            P("fsdp", None),
        ),
        check_vma=False,
    )
```

```python
import functools

import jax
import jax.numpy as jnp
from jax import lax
from jax.experimental import pallas as pl
from jax.experimental.pallas import tpu as pltpu
from jax.sharding import PartitionSpec as P

D = 1536
HEADS = 12
KV_HEADS = 2
HEAD_DIM = 128

eps = 1e-06
rope_base = 1000000.0
F32 = jnp.float32
BF16 = jnp.bfloat16
VMEM_LIMIT = 60 * 1024 * 1024


def rope_tables(position):
    half = HEAD_DIM // 2
    inverse = rope_base ** (-(jnp.arange(half, dtype=F32) * 2.0 / HEAD_DIM))
    angle = position.astype(F32)[:, None] * inverse[None, :]
    return (jnp.cos(angle)[:, None, :], jnp.sin(angle)[:, None, :])


def rotate(vectors, cosines, sines):
    half = HEAD_DIM // 2
    first, second = (vectors[..., :half], vectors[..., half:])
    return jnp.concatenate([first * cosines - second * sines, second * cosines + first * sines], -1)


def unrotate(grads, cosines, sines):
    half = HEAD_DIM // 2
    first, second = (grads[..., :half], grads[..., half:])
    return jnp.concatenate([first * cosines + second * sines, second * cosines - first * sines], -1)


def rms_scale(values):
    return lax.rsqrt(jnp.mean(values * values, -1, keepdims=True) + eps)


def rms_backward(values, scale_rows, gain, d_normed):
    d_gain = jnp.sum(d_normed * values * scale_rows, 0)
    d_inner = d_normed * gain
    d_values = scale_rows * d_inner - values * scale_rows**3 * jnp.mean(
        d_inner * values, -1, keepdims=True
    )
    return (d_values, d_gain)


def dot(left, right, contract):
    return lax.dot_general(left, right, (contract, ((), ())), preferred_element_type=F32)


def contract_rows(left, right):
    return dot(left, right, ((0,), (0,)))


def contract_cols(left, right):
    return dot(left, right, ((1,), (1,)))


def stacked_heads(ref, which, heads):
    return jnp.concatenate(
        [ref[which, :, h * HEAD_DIM : (h + 1) * HEAD_DIM] for h in range(heads)], 0
    )


def causal(block_len, heads):
    keys = lax.broadcasted_iota(jnp.int32, (block_len, block_len), 0)
    queries = lax.broadcasted_iota(jnp.int32, (block_len, block_len), 1)
    return jnp.concatenate([keys <= queries] * heads, 1)


def attend_kernel(heads, table, ids, q_ref, kv_ref, o_ref, lse_ref):
    block_len = q_ref.shape[1]
    cols = heads * block_len
    scale = HEAD_DIM ** (-0.5)
    for which in range(2):
        last = ids[which]
        query = stacked_heads(q_ref, which, heads)

        def step(block, carry, masked=False):
            highest, total, acc = carry
            start = pl.multiple_of(table[block] * block_len, block_len)
            key = kv_ref[pl.ds(start, block_len), :HEAD_DIM]
            value = kv_ref[pl.ds(start, block_len), HEAD_DIM:]
            scores = contract_cols(key, query) * scale
            if masked:
                scores = jnp.where(causal(block_len, heads), scores, -1e30)
            new_high = jnp.maximum(highest, jnp.max(scores, 0, keepdims=True))
            probs = jnp.exp(scores - new_high)
            fade = jnp.exp(highest - new_high)
            total = total * fade + jnp.sum(probs, 0, keepdims=True)
            acc = acc * fade + contract_rows(value, probs.astype(BF16))
            return (new_high, total, acc)

        begin = (
            jnp.full((1, cols), -1e30, F32),
            jnp.zeros((1, cols), F32),
            jnp.zeros((HEAD_DIM, cols), F32),
        )
        carry = lax.fori_loop(0, last, step, begin)
        highest, total, acc = step(last, carry, True)
        lse_ref[which] = highest + jnp.log(total)
        out = (acc / total).T
        for h in range(heads):
            o_ref[which, :, h * HEAD_DIM : (h + 1) * HEAD_DIM] = out[
                h * block_len : (h + 1) * block_len
            ].astype(BF16)


def attend_back_kernel(
    heads, table, ids, q_ref, kv_ref, o_ref, do_ref, lse_ref, dq_ref, dkv_ref, sums
):
    block_len = q_ref.shape[1]
    cols = heads * block_len
    scale = HEAD_DIM ** (-0.5)
    sums[...] = jnp.zeros_like(sums)
    for which in range(2):
        last = ids[which]
        query = stacked_heads(q_ref, which, heads)
        d_out = stacked_heads(do_ref, which, heads)
        out = stacked_heads(o_ref, which, heads)
        delta = jnp.sum((d_out.astype(F32) * out.astype(F32)).T, 0, keepdims=True)
        lse = lse_ref[which]

        def step(block, d_query, masked=False):
            start = pl.multiple_of(table[block] * block_len, block_len)
            key = kv_ref[pl.ds(start, block_len), :HEAD_DIM]
            value = kv_ref[pl.ds(start, block_len), HEAD_DIM:]
            scores = contract_cols(key, query) * scale
            probs = jnp.exp(scores - lse)
            if masked:
                probs = jnp.where(causal(block_len, heads), probs, 0.0)
            d_probs = contract_cols(value, d_out)
            d_scores = (probs * (d_probs - delta)).astype(BF16)
            sums[pl.ds(start, block_len), :HEAD_DIM] += dot(d_scores, query, ((1,), (0,)))
            sums[pl.ds(start, block_len), HEAD_DIM:] += dot(
                probs.astype(BF16), d_out, ((1,), (0,))
            )
            return d_query + contract_rows(key, d_scores)

        d_query = lax.fori_loop(0, last, step, jnp.zeros((HEAD_DIM, cols), F32))
        d_query = step(last, d_query, True)
        d_query = (d_query * scale).T
        for h in range(heads):
            dq_ref[which, :, h * HEAD_DIM : (h + 1) * HEAD_DIM] = d_query[
                h * block_len : (h + 1) * block_len
            ]
    dkv_ref[:, :HEAD_DIM] = (sums[:, :HEAD_DIM] * scale).astype(BF16)
    dkv_ref[:, HEAD_DIM:] = sums[:, HEAD_DIM:].astype(BF16)


def in_vmem(count):
    return [pl.BlockSpec(memory_space=pltpu.VMEM)] * count


def in_smem(count):
    return [pl.BlockSpec(memory_space=pltpu.SMEM)] * count


def attend(table, ids, query, keys_values, heads):
    _, block_len, width = query.shape
    tall = keys_values.shape[0]
    return pl.pallas_call(
        functools.partial(attend_kernel, heads),
        out_shape=(
            jax.ShapeDtypeStruct(query.shape, BF16),
            jax.ShapeDtypeStruct((2, 1, heads * block_len), F32),
        ),
        in_specs=in_smem(2) + in_vmem(2),
        out_specs=tuple(in_vmem(2)),
        compiler_params=pltpu.CompilerParams(vmem_limit_bytes=VMEM_LIMIT),
        cost_estimate=pl.CostEstimate(
            flops=2 * tall * block_len * width * 2,
            bytes_accessed=tall * 512,
            transcendentals=tall * heads * block_len,
        ),
        name="attend",
    )(table, ids, query, keys_values)


def attend_back(table, ids, query, keys_values, out, d_out, lse, heads):
    _, block_len, width = query.shape
    tall = keys_values.shape[0]
    return pl.pallas_call(
        functools.partial(attend_back_kernel, heads),
        out_shape=(
            jax.ShapeDtypeStruct(query.shape, F32),
            jax.ShapeDtypeStruct(keys_values.shape, BF16),
        ),
        in_specs=in_smem(2) + in_vmem(5),
        out_specs=tuple(in_vmem(2)),
        scratch_shapes=[pltpu.VMEM(keys_values.shape, F32)],
        compiler_params=pltpu.CompilerParams(vmem_limit_bytes=VMEM_LIMIT),
        cost_estimate=pl.CostEstimate(
            flops=5 * tall * block_len * width * 2,
            bytes_accessed=tall * 1024,
            transcendentals=tall * heads * block_len,
        ),
        name="attend_back",
    )(table, ids, query, keys_values, out, d_out, lse)


MESH = pl.DeviceIdType.MESH


def greet(devices):
    barrier = pltpu.get_barrier_semaphore()
    for device in devices:
        pl.semaphore_signal(barrier, inc=1, device_id=device, device_id_type=MESH)
    pl.semaphore_wait(barrier, len(devices))


def remote(src, dst, send, recv, device):
    return pltpu.make_async_remote_copy(
        src_ref=src, dst_ref=dst, send_sem=send, recv_sem=recv, device_id=device, device_id_type=MESH
    )


def group_places(n):
    ctx = lax.axis_index("ctx")
    me = lax.axis_index("fsdp")
    partner = me + 1 - 2 * (me % 2)
    others = [(me + 2 * k) % n for k in range(1, n // 2)]
    senders = [(me + n - 2 * k) % n for k in range(1, n // 2)]
    return ctx, me, partner, others, senders


def sum_phases(mode, n, cuts, *refs):
    gathers = mode != "input"
    if mode == "attention":
        partial, tokens, gain, hidden_out, all_out = refs[:5]
    elif mode == "mlp":
        partial, hidden_in, cot, gain, d_out, all_out, d_gain = refs[:7]
    else:
        partial, tokens, d_hidden_in, gain, d_out, d_gain = refs[:6]
    near, summed, far, stage, near_s, near_r, far_s, far_r, own_s, own_r, out_s, out_r, fwd_s, fwd_r = refs[-14:]
    ctx, me, partner, others, senders = group_places(n)
    chips = n // 2
    rows = partial.shape[2]
    piece = rows // cuts
    chunks = [(w, i * piece) for w in range(2) for i in range(cuts)]

    def part(ref, w, lead, start):
        return ref.at[w, lead, pl.ds(start, piece)]

    first = []
    for c, (w, start) in enumerate(chunks):
        for j in range(chips):
            target = (partner + 2 * (j + 1)) % n
            copy = remote(
                part(partial, w, target, start),
                part(near, w, j, start),
                near_s.at[c, j],
                near_r.at[c, j],
                (ctx, partner),
            )
            copy.start()
            first.append(copy)
    yield

    second = []

    def post(c):
        w, start = chunks[c]
        for j in range(chips - 1):
            copy = remote(
                part(summed, w, j, start),
                part(far, w, j, start),
                far_s.at[c, j],
                far_r.at[c, j],
                (ctx, others[j]),
            )
            copy.start()
            second.append(copy)

    for c, (w, start) in enumerate(chunks):
        span = pl.ds(start, piece)
        for j in range(chips - 1):
            first[c * chips + j].wait()
            target = (me + 2 * (j + 1)) % n
            summed[w, j, span] = (
                partial[w, target, span].astype(F32) + near[w, j, span].astype(F32)
            ).astype(BF16)
        if c:
            post(c - 1)
    post(len(chunks) - 1)
    yield

    if mode != "attention":
        d_gain[...] = jnp.zeros_like(d_gain)
    third = []

    def spread(c):
        w, start = chunks[c]
        src = stage.at[w, pl.ds(start, piece)]
        for k in range(chips - 1):
            copy = remote(src, part(all_out, w, me, start), out_s.at[c, k], out_r.at[c, k], (ctx, others[k]))
            copy.start()
            third.append(copy)
        copy = remote(src, part(all_out, w, me, start), own_s.at[c], own_r.at[c], (ctx, partner))
        copy.start()
        return copy

    near_copies = []
    for c, (w, start) in enumerate(chunks):
        span = pl.ds(start, piece)
        first[c * chips + chips - 1].wait()
        total = partial[w, me, span].astype(F32) + near[w, chips - 1, span].astype(F32)
        for j in range(chips - 1):
            second[c * (chips - 1) + j].wait()
            total += far[w, j, span].astype(F32)
        if mode == "attention":
            hidden = tokens[w, span].astype(F32) + total
            hidden_out[w, span] = hidden
            rounded = (hidden * rms_scale(hidden) * gain[...]).astype(BF16)
        elif mode == "mlp":
            hidden = hidden_in[w, span]
            d_norm, gain_part = rms_backward(hidden, rms_scale(hidden), gain[...], total)
            d_gain[...] += gain_part[None]
            d_hidden = cot[w, span].astype(F32) + d_norm
            d_out[w, span] = d_hidden
            rounded = d_hidden.astype(BF16)
        else:
            values = tokens[w, span].astype(F32)
            d_norm, gain_part = rms_backward(values, rms_scale(values), gain[...], total)
            d_gain[...] += gain_part[None]
            d_out[w, span] = d_hidden_in[w, span] + d_norm
        if gathers:
            stage[w, span] = rounded
            all_out[w, me, span] = rounded
            if c:
                near_copies.append(spread(c - 1))
    if not gathers:
        return
    near_copies.append(spread(len(chunks) - 1))
    yield

    forwards = []
    for c, (w, start) in enumerate(chunks):
        for k in range(chips - 1):
            third[c * (chips - 1) + k].wait_recv()
            block = part(all_out, w, senders[k], start)
            copy = remote(block, block, fwd_s.at[c, k], fwd_r.at[c, k], (ctx, partner))
            copy.start()
            forwards.append(copy)
    yield
    for copy in third:
        copy.wait_send()
    for copy in near_copies + forwards:
        copy.wait()


def sum_kernel(mode, n, cuts, *refs):
    ctx, _, partner, others, _ = group_places(n)
    greet([(ctx, partner)] + [(ctx, o) for o in others])
    for _ in sum_phases(mode, n, cuts, *refs):
        pass


def sum_shapes(mode, partial):
    _, n, rows, width = partial.shape
    chips = n // 2
    row_shape = (2, rows, width)
    full = jax.ShapeDtypeStruct(row_shape, F32)
    gathered = jax.ShapeDtypeStruct(partial.shape, BF16)
    gain_sum = jax.ShapeDtypeStruct((1, width), F32)
    out_shape = {
        "attention": (full, gathered),
        "mlp": (full, gathered, gain_sum),
        "input": (full, gain_sum),
    }[mode]
    dma = pltpu.SemaphoreType.DMA
    chunks = 2 * SUM_CUTS
    scratch = [
        pltpu.VMEM((2, chips, rows, width), BF16),
        pltpu.VMEM((2, chips - 1, rows, width), BF16),
        pltpu.VMEM((2, chips - 1, rows, width), BF16),
        pltpu.VMEM(row_shape, BF16),
        dma((chunks, chips)),
        dma((chunks, chips)),
        dma((chunks, chips - 1)),
        dma((chunks, chips - 1)),
        dma((chunks,)),
        dma((chunks,)),
        dma((chunks, chips - 1)),
        dma((chunks, chips - 1)),
        dma((chunks, chips - 1)),
        dma((chunks, chips - 1)),
    ]
    return out_shape, scratch


SUM_CUTS = 2


def group_sum(mode, partial, *operands, collective):
    _, n, rows, width = partial.shape
    out_shape, scratch = sum_shapes(mode, partial)
    return pl.pallas_call(
        functools.partial(sum_kernel, mode, n, SUM_CUTS),
        out_shape=out_shape,
        in_specs=in_vmem(1 + len(operands)),
        out_specs=tuple(in_vmem(len(out_shape))),
        scratch_shapes=scratch,
        compiler_params=pltpu.CompilerParams(
            vmem_limit_bytes=VMEM_LIMIT, collective_id=collective, has_side_effects=True
        ),
        cost_estimate=pl.CostEstimate(
            flops=20 * rows * width, bytes_accessed=60_000_000, transcendentals=0
        ),
        name="group_sum_" + mode,
    )(partial, *operands)


def ring_index(place, n):
    late = place // (n // 2)
    return (1 - late) * 2 * place + late * (2 * n - 1 - 2 * place)


def ring_place(index, n):
    odd = index % 2
    return (1 - odd) * (index // 2) + odd * (n - 1 - index // 2)


def share_kernel(n, own, out, right_s, right_r, left_s, left_r, near_s, near_r):
    ctx = lax.axis_index("ctx")
    me = lax.axis_index("fsdp")
    which = me % 2
    partner = me + 1 - 2 * which
    place = ring_place(ctx, n)
    right = (ring_index((place + 1) % n, n), me)
    left = (ring_index((place + n - 1) % n, n), me)
    greet([right, left, (ctx, partner)])

    def block(offset):
        return out.at[ring_index((place + n + offset) % n, n), which]

    def to_right(step):
        src = own.at[which] if step == 0 else block(-step)
        return remote(src, block(-step), right_s.at[step], right_r.at[step], right)

    def to_left(step):
        src = own.at[which] if step == 0 else block(step)
        return remote(src, block(step), left_s.at[step], left_r.at[step], left)

    rights, lefts = n // 2, n - 1 - n // 2
    sent = [to_right(0), to_left(0)]
    for copy in sent:
        copy.start()
    out[ctx] = own[...]
    going = [sent[0], sent[1]]
    for step in range(1, rights + 1):
        going[0].wait_recv()
        if step < rights:
            going[0] = to_right(step)
            going[0].start()
            sent.append(going[0])
        hand = remote(block(-step), block(-step), near_s.at[step - 1], near_r.at[step - 1], (ctx, partner))
        hand.start()
        sent.append(hand)
        if step <= lefts:
            going[1].wait_recv()
            if step < lefts:
                going[1] = to_left(step)
                going[1].start()
                sent.append(going[1])
            slot = rights + step - 1
            hand = remote(block(step), block(step), near_s.at[slot], near_r.at[slot], (ctx, partner))
            hand.start()
            sent.append(hand)
    for copy in sent:
        copy.wait_send()
    for step in range(1, rights + 1):
        remote(block(-step), block(-step), near_s.at[step - 1], near_r.at[step - 1], (ctx, partner)).wait_recv()
    for step in range(1, lefts + 1):
        slot = rights + step - 1
        remote(block(step), block(step), near_s.at[slot], near_r.at[slot], (ctx, partner)).wait_recv()


def share_keys(own, n, collective):
    dma = pltpu.SemaphoreType.DMA
    return pl.pallas_call(
        functools.partial(share_kernel, n),
        out_shape=jax.ShapeDtypeStruct((n,) + own.shape, BF16),
        in_specs=in_vmem(1),
        out_specs=in_vmem(1)[0],
        scratch_shapes=[dma((n // 2,))] * 4 + [dma((n - 1,))] * 2,
        compiler_params=pltpu.CompilerParams(
            vmem_limit_bytes=VMEM_LIMIT, collective_id=collective, has_side_effects=True
        ),
        cost_estimate=pl.CostEstimate(flops=0, bytes_accessed=60_000_000, transcendentals=0),
        name="share_keys",
    )(own)


def return_kernel(n, partial, out, near, summed, far, near_s, near_r, far_s, far_r):
    ctx = lax.axis_index("ctx")
    me = lax.axis_index("fsdp")
    which = me % 2
    partner = me + 1 - 2 * which
    others = [(ctx + k) % n for k in range(1, n)]
    greet([(ctx, partner)] + [(o, me) for o in others])
    order = others + [ctx]
    first = []
    for k, target in enumerate(order):
        copy = remote(partial.at[target, 1 - which], near.at[k], near_s.at[k], near_r.at[k], (ctx, partner))
        copy.start()
        first.append(copy)
    second = []

    def post(k):
        copy = remote(summed.at[k], far.at[k], far_s.at[k], far_r.at[k], (others[k], me))
        copy.start()
        second.append(copy)

    for k in range(n - 1):
        first[k].wait()
        summed[k] = (partial[others[k], which].astype(F32) + near[k].astype(F32)).astype(BF16)
        if k:
            post(k - 1)
    post(n - 2)
    out[1 - which] = jnp.zeros(out.shape[1:], F32)
    first[n - 1].wait()
    out[which] = partial[ctx, which].astype(F32) + near[n - 1].astype(F32)
    for k in range(n - 1):
        second[k].wait()
        out[which] += far[k].astype(F32)


def return_grads(partial, collective):
    n = partial.shape[0]
    block = partial.shape[2:]
    dma = pltpu.SemaphoreType.DMA
    return pl.pallas_call(
        functools.partial(return_kernel, n),
        out_shape=jax.ShapeDtypeStruct(partial.shape[1:], F32),
        in_specs=in_vmem(1),
        out_specs=in_vmem(1)[0],
        scratch_shapes=[
            pltpu.VMEM((n,) + block, BF16),
            pltpu.VMEM((n - 1,) + block, BF16),
            pltpu.VMEM((n - 1,) + block, BF16),
            dma((n,)),
            dma((n,)),
            dma((n - 1,)),
            dma((n - 1,)),
        ],
        compiler_params=pltpu.CompilerParams(
            vmem_limit_bytes=VMEM_LIMIT, collective_id=collective, has_side_effects=True
        ),
        cost_estimate=pl.CostEstimate(flops=0, bytes_accessed=80_000_000, transcendentals=0),
        name="return_grads",
    )(partial)


def ring_sum_kernel(n, members, plan, swaps, arrays, mode, extra_ins, extra_outs, *refs):
    ins, refs = refs[:arrays], refs[arrays:]
    side_ins, refs = refs[:extra_ins], refs[extra_ins:]
    outs, refs = refs[:arrays], refs[arrays:]
    side_outs, refs = refs[:extra_outs], refs[extra_outs:]
    count = len(plan)
    arrived, stages, sends, recvs = (refs[i * count : (i + 1) * count] for i in range(4))
    refs = refs[4 * count :]
    done, swap_s, swap_r = (refs[i * len(swaps) : (i + 1) * len(swaps)] for i in range(3))
    refs = refs[3 * len(swaps) :]
    ctx = lax.axis_index("ctx")
    me = lax.axis_index("fsdp")
    place = ring_place(ctx, n)
    around = {step: (ring_index((place + n + step) % n, n), me) for step in (1, -1)}
    greet([around[1], around[-1]] + [(ctx, (me + k) % members) for k in range(1, members)])
    beside = iter(())
    if mode:
        beside = sum_phases(mode, members, SUM_CUTS, *side_ins, *side_outs, *refs)

    def copy(i, hop, src):
        step = plan[i][3]
        return remote(src, arrived[i].at[hop], sends[i].at[hop], recvs[i].at[hop], around[step])

    def chunk(i, hop):
        step = plan[i][3]
        return ring_index((place + n * n - step * (hop + 1)) % n, n)

    def window(i, group, hop):
        which, low, high, _ = plan[i]
        return ins[which][group, chunk(i, hop), :, low:high].astype(F32)

    def first(i):
        which, low, high, _ = plan[i]
        return copy(i, 0, ins[which].at[:, chunk(i, 0), :, pl.ds(low, high - low)])

    for i in range(count):
        first(i).start()
    next(beside, None)

    def add(i, hop, store):
        copy(i, hop - 1, stages[i].at[0]).wait_recv()

        def group_add(group, carry):
            store(group, (arrived[i][hop - 1, group].astype(F32) + window(i, group, hop)).astype(BF16))
            return carry

        lax.fori_loop(0, ins[plan[i][0]].shape[0], group_add, 0)

    def one_hop(hop, carry):
        slot = hop % 2
        for i in range(count):
            @pl.when(hop > 2)
            def _():
                copy(i, hop - 2, stages[i].at[slot]).wait_send()

            def store(group, value):
                stages[i][slot, group] = value

            add(i, hop, store)
            if i:
                copy(i - 1, hop, stages[i - 1].at[slot]).start()
        copy(count - 1, hop, stages[count - 1].at[slot]).start()
        return carry

    hop = 1
    if mode:
        for _ in range(min(4, n - 3)):
            one_hop(jnp.int32(hop), 0)
            hop += 1
            next(beside, None)
    lax.fori_loop(hop, n - 1, one_hop, 0)
    for i, (which, low, high, _) in enumerate(plan):
        target = done[swaps.index(which)] if which in swaps else outs[which]

        def store(group, value):
            target[group, :, low:high] = value

        add(i, n - 1, store)
    swapped = []
    for j, which in enumerate(swaps):
        for k in range(1, members):
            other = (me + k) % members
            swapped.append(
                remote(
                    done[j].at[other],
                    outs[which].at[me],
                    swap_s[j].at[k - 1],
                    swap_r[j].at[k - 1],
                    (ctx, other),
                )
            )
            swapped[-1].start()
        outs[which][me] = done[j][me]
    for _ in beside:
        pass
    for i in range(count):
        first(i).wait_send()
        for hop in (n - 3, n - 2):
            copy(i, hop, stages[i].at[hop % 2]).wait_send()
    for move in swapped:
        move.wait()


def ring_sum(arrays, plan, swaps, members, collective, mode=None, operands=()):
    n = arrays[0].shape[1]
    dma = pltpu.SemaphoreType.DMA
    blocks = [
        (arrays[which].shape[0], arrays[which].shape[2], high - low) for which, low, high, _ in plan
    ]
    sums = [(a.shape[0],) + a.shape[2:] for a in arrays]
    extra_shape, extra_scratch = sum_shapes(mode, operands[0]) if mode else ((), [])
    out_shape = tuple(jax.ShapeDtypeStruct(shape, BF16) for shape in sums) + tuple(extra_shape)
    return pl.pallas_call(
        functools.partial(
            ring_sum_kernel, n, members, plan, swaps, len(arrays), mode, len(operands), len(extra_shape)
        ),
        out_shape=out_shape,
        in_specs=in_vmem(len(arrays) + len(operands)),
        out_specs=tuple(in_vmem(len(out_shape))),
        scratch_shapes=[pltpu.VMEM((n - 1,) + b, BF16) for b in blocks]
        + [pltpu.VMEM((2,) + b, BF16) for b in blocks]
        + [dma((n - 1,)) for _ in blocks] * 2
        + [pltpu.VMEM(sums[which], BF16) for which in swaps]
        + [dma((members - 1,)) for _ in swaps] * 2
        + extra_scratch,
        compiler_params=pltpu.CompilerParams(
            vmem_limit_bytes=VMEM_LIMIT, collective_id=collective, has_side_effects=True
        ),
        cost_estimate=pl.CostEstimate(flops=0, bytes_accessed=200_000_000, transcendentals=0),
        name="ring_sum",
    )(*arrays, *operands)


def ring_gather_kernel(n, count, *refs):
    owns, outs, sends, recvs = (refs[i * count : (i + 1) * count] for i in range(4))
    ctx = lax.axis_index("ctx")
    me = lax.axis_index("fsdp")
    place = ring_place(ctx, n)
    around = {step: (ring_index((place + n + step) % n, n), me) for step in (1, -1)}
    greet([around[1], around[-1]])
    far = n // 2

    def copy(i, step, half, hop):
        middle = owns[i].shape[-1] // 2
        lanes = pl.ds(half * middle, middle)
        block = outs[i].at[ring_index((place + n - step * hop) % n, n), :, lanes]
        src = block if hop else owns[i].at[:, lanes]
        row = half if step == 1 else 2 + half
        return remote(src, block, sends[i].at[row, hop], recvs[i].at[row, hop], around[step])

    def hops(step, half):
        return far if (step == 1) == (half == 0) else far - 1

    lines = [(i, step, half) for step, half in ((1, 0), (-1, 1), (1, 1), (-1, 0)) for i in range(count)]
    for i, step, half in lines:
        copy(i, step, half, 0).start()
    for own, out in zip(owns, outs):
        out[ctx] = own[...]
    for hop in range(1, far + 1):
        for i, step, half in lines:
            if hop <= hops(step, half):
                copy(i, step, half, hop - 1).wait_recv()
                if hop < hops(step, half):
                    copy(i, step, half, hop).start()
    for i, step, half in lines:
        for hop in range(hops(step, half)):
            copy(i, step, half, hop).wait_send()


def ring_gather(owns, n, collective):
    count = len(owns)
    return pl.pallas_call(
        functools.partial(ring_gather_kernel, n, count),
        out_shape=tuple(jax.ShapeDtypeStruct((n,) + own.shape, BF16) for own in owns),
        in_specs=in_vmem(count),
        out_specs=tuple(in_vmem(count)),
        scratch_shapes=[pltpu.SemaphoreType.DMA((4, n // 2))] * (2 * count),
        compiler_params=pltpu.CompilerParams(
            vmem_limit_bytes=VMEM_LIMIT, collective_id=collective, has_side_effects=True
        ),
        cost_estimate=pl.CostEstimate(flops=0, bytes_accessed=120_000_000, transcendentals=0),
        name="ring_gather",
    )(*owns)


def weave_kernel(planes, out):
    for e in range(2):
        out[:, e, :] = planes[e].astype(F32)


def weave(planes):
    _, rows, lanes = planes.shape
    block = 32 if rows % 32 == 0 else rows
    return pl.pallas_call(
        weave_kernel,
        grid=(rows // block,),
        out_shape=jax.ShapeDtypeStruct((rows, 2, lanes), F32),
        in_specs=[pl.BlockSpec((2, block, lanes), lambda i: (0, i, 0))],
        out_specs=pl.BlockSpec((block, 2, lanes), lambda i: (i, 0, 0)),
        cost_estimate=pl.CostEstimate(
            flops=0, bytes_accessed=12 * rows * lanes, transcendentals=0
        ),
        name="weave",
    )(planes)


def exchange(pieces, axis):
    return lax.all_to_all(pieces, axis, split_axis=0, concat_axis=0, tiled=True)


def together(*values):
    return lax.optimization_barrier(values)


def body(tokens, pairing, gain_attn, w_qkv, b_qkv, w_out, gain_mlp, w_gate_up, w_down, cotangent):
    half_rows = tokens.shape[2]
    n_ctx = lax.axis_size("ctx")
    n_fsdp = lax.axis_size("fsdp")
    ctx_index = lax.axis_index("ctx")
    fsdp_index = lax.axis_index("fsdp")
    stretch_len = half_rows * n_fsdp
    rows = 2 * stretch_len
    local_count = 2 * half_rows
    q_width = HEADS * HEAD_DIM
    kv_width = KV_HEADS * HEAD_DIM
    heads = HEADS // n_fsdp
    q_cols = heads * HEAD_DIM
    d_shard = w_qkv.shape[0]
    ff_shard = w_down.shape[0]

    owner_range = jnp.arange(n_ctx, dtype=jnp.int32)
    own_first = jnp.sum(jnp.where(owner_range == ctx_index, pairing, 0))
    ids = jnp.stack([own_first, 2 * n_ctx - 1 - own_first])
    inverse_pair = jnp.sum(
        owner_range[:, None] * (pairing[:, None] == owner_range[None, :]).astype(jnp.int32), 0
    )
    table = jnp.concatenate([2 * inverse_pair, 2 * inverse_pair[::-1] + 1])
    position = (
        ids[:, None] * stretch_len + jnp.arange(stretch_len, dtype=jnp.int32)[None, :]
    ).reshape(rows)
    kv_of = [f * KV_HEADS // n_fsdp for f in range(n_fsdp)]
    my_kv = fsdp_index * KV_HEADS // n_fsdp

    small = lax.all_gather(jnp.concatenate([gain_attn, gain_mlp, b_qkv]), "fsdp", axis=0)
    small, w_qkv, w_gate_up = together(small, w_qkv, w_gate_up)
    gain_one = small[:, :d_shard].reshape(D).astype(F32)
    gain_two = small[:, d_shard : 2 * d_shard].reshape(D).astype(F32)
    bias = small[:, 2 * d_shard :].reshape(-1).astype(F32)
    x_all = lax.all_gather(tokens[0], "fsdp", axis=1, tiled=True).reshape(rows, D)
    qkv_pieces = jnp.stack(
        [
            jnp.concatenate(
                [
                    w_qkv[:, f * q_cols : (f + 1) * q_cols],
                    w_qkv[:, q_width + kv_of[f] * HEAD_DIM : q_width + (kv_of[f] + 1) * HEAD_DIM],
                    w_qkv[
                        :,
                        q_width + kv_width + kv_of[f] * HEAD_DIM : q_width
                        + kv_width
                        + (kv_of[f] + 1) * HEAD_DIM,
                    ],
                ],
                1,
            )
            for f in range(n_fsdp)
        ]
    )
    w_qkv_cols = exchange(qkv_pieces, "fsdp").reshape(D, -1)
    bias_cols = jnp.concatenate(
        [
            lax.dynamic_slice_in_dim(bias, fsdp_index * q_cols, q_cols),
            lax.dynamic_slice_in_dim(bias, q_width + my_kv * HEAD_DIM, HEAD_DIM),
            lax.dynamic_slice_in_dim(bias, q_width + kv_width + my_kv * HEAD_DIM, HEAD_DIM),
        ]
    )
    gate_up_pieces = w_gate_up.reshape(d_shard, 2, n_fsdp, ff_shard).transpose(2, 1, 0, 3)
    x_all, w_qkv_cols, gate_up_pieces = together(x_all, w_qkv_cols, gate_up_pieces)
    gate_up_cols = exchange(gate_up_pieces, "fsdp")
    cot_all = lax.all_gather(cotangent[0], "fsdp", axis=1, tiled=True).reshape(rows, D)

    x32 = x_all.astype(F32)
    normed1 = (x32 * rms_scale(x32) * gain_one).astype(BF16)
    qkv = jnp.dot(normed1, w_qkv_cols, preferred_element_type=F32) + bias_cols
    cosines, sines = rope_tables(position)
    rotated = rotate(
        qkv[:, : q_cols + HEAD_DIM].reshape(rows, heads + 1, HEAD_DIM), cosines, sines
    ).astype(BF16)
    query = rotated[:, :heads].reshape(2, stretch_len, q_cols)
    own_kv = jnp.concatenate([rotated[:, heads], qkv[:, q_cols + HEAD_DIM :].astype(BF16)], 1)
    keys_values = share_keys(own_kv.reshape(2, stretch_len, 2 * HEAD_DIM), n_ctx, 4)
    keys_values = keys_values.reshape(n_ctx * rows, 2 * HEAD_DIM)
    attended, lse = attend(table, ids, query, keys_values, heads)
    attended16 = attended.reshape(rows, q_cols)

    def scatter(partial):
        return lax.psum_scatter(
            partial.astype(BF16).reshape(2, stretch_len, D), "fsdp", scatter_dimension=1, tiled=True
        ).astype(F32).reshape(local_count, D)

    def by_member(partial):
        return partial.astype(BF16).reshape(2, n_fsdp, half_rows, D)

    tokens_own = tokens[0]
    hidden, normed2 = group_sum(
        "attention",
        by_member(jnp.dot(attended16, w_out, preferred_element_type=F32)),
        tokens_own,
        gain_two[None],
        collective=1,
    )
    normed2 = normed2.reshape(rows, D)
    w_gate_cols, w_up_cols = (gate_up_cols[:, e] for e in range(2))
    normed2_parts = normed2.reshape(rows, n_fsdp, d_shard)
    gate_val, up_val = (
        jnp.einsum("tsk,skf->tf", normed2_parts, w, preferred_element_type=F32)
        for w in (w_gate_cols, w_up_cols)
    )
    sigmoid_gate = jax.nn.sigmoid(gate_val)
    act16 = (jax.nn.silu(gate_val) * up_val).astype(BF16)
    result = hidden.reshape(local_count, D) + scatter(jnp.dot(act16, w_down, preferred_element_type=F32))
    block_output = result.astype(BF16).reshape(tokens.shape)

    d_act = contract_cols(cot_all, w_down)
    d_gate16 = (d_act * up_val * sigmoid_gate * (1.0 + gate_val * (1.0 - sigmoid_gate))).astype(BF16)
    d_up16 = (d_act * gate_val * sigmoid_gate).astype(BF16)
    d_normed2 = sum(
        jnp.einsum("tf,skf->tsk", d, w, preferred_element_type=F32)
        for d, w in ((d_gate16, w_gate_cols), (d_up16, w_up_cols))
    )
    def by_columns(pieces):
        queries = [pieces[f][..., :q_cols] for f in range(n_fsdp)]
        rest = []
        for part in range(2):
            lo = q_cols + part * HEAD_DIM
            for g in range(KV_HEADS):
                rest.append(
                    sum(
                        pieces[f][..., lo : lo + HEAD_DIM].astype(F32)
                        for f in range(n_fsdp)
                        if kv_of[f] == g
                    ).astype(pieces[0].dtype)
                )
        return jnp.concatenate(queries + rest, -1)

    chunk_rows = d_shard // n_ctx
    down_rows = -(-ff_shard // (16 * n_ctx)) * 16
    side = D // 2

    def padded(grad):
        extra = n_ctx * down_rows - grad.shape[0]
        return jnp.pad(grad, ((0, extra), (0, 0))).astype(BF16).reshape(n_ctx, down_rows, D)

    d_w_down = padded(contract_rows(act16, cot_all))
    d_w_gate, d_w_up = (
        contract_rows(normed2, piece).astype(BF16).reshape(n_fsdp, n_ctx, chunk_rows, ff_shard)
        for piece in (d_gate16, d_up16)
    )

    gate_sum, up_sum, down_sum, d_hidden, dh_all, d_gain_two = ring_sum(
        (d_w_gate, d_w_up, d_w_down[None]),
        ((0, 0, ff_shard, 1), (1, 0, ff_shard, -1), (2, 0, side, 1), (2, side, D, -1)),
        (0, 1),
        n_fsdp,
        7,
        "mlp",
        (by_member(d_normed2), hidden, cotangent[0], gain_two[None]),
    )
    planes = jnp.stack(
        [
            total.transpose(1, 0, 2).reshape(chunk_rows, n_fsdp * ff_shard)
            for total in (gate_sum, up_sum)
        ]
    )
    d_w_gate_up = weave(lax.all_gather(planes, "ctx", axis=1, tiled=True))
    dh_all = dh_all.reshape(rows, D)
    d_attended16 = contract_cols(dh_all, w_out).astype(BF16).reshape(2, stretch_len, q_cols)
    d_query, d_kv = attend_back(
        table, ids, query, keys_values, attended, d_attended16, lse, heads
    )
    d_kv_own = return_grads(d_kv.reshape(n_ctx, 2, stretch_len, 2 * HEAD_DIM), 5).reshape(rows, -1)

    d_w_out = contract_rows(attended16, dh_all).astype(BF16).reshape(n_ctx, chunk_rows, D)
    d_rotated = jnp.concatenate([d_query.reshape(rows, q_cols), d_kv_own[:, :HEAD_DIM]], 1)
    d_rotated = unrotate(
        d_rotated.reshape(rows, heads + 1, HEAD_DIM), cosines, sines
    ).reshape(rows, q_cols + HEAD_DIM)
    d_qkv = jnp.concatenate([d_rotated, d_kv_own[:, HEAD_DIM:]], 1)
    d_bias = jnp.sum(d_qkv, 0)
    d_qkv16 = d_qkv.astype(BF16)
    d_normed1 = by_member(contract_cols(d_qkv16, w_qkv_cols))
    d_tokens, d_gain_one = group_sum(
        "input",
        d_normed1,
        tokens_own,
        d_hidden,
        gain_one[None],
        collective=3,
    )
    d_tokens = d_tokens.reshape(tokens.shape)

    zeros = jnp.zeros_like(d_bias)
    d_bias_full = by_columns([jnp.where(fsdp_index == f, d_bias, zeros) for f in range(n_fsdp)])
    parts = jnp.concatenate(
        [v.reshape(n_fsdp, -1) for v in (d_gain_one, d_gain_two, d_bias_full)], 1
    ).astype(BF16)
    length = parts.shape[1]
    few = 2 * HEAD_DIM
    vector_rows = -(-length // (n_ctx * few))
    parts = jnp.pad(parts, ((0, 0), (0, n_ctx * vector_rows * few - length)))
    parts = parts.reshape(n_fsdp, n_ctx, vector_rows, few)
    parts = jnp.pad(parts, ((0, 0), (0, 0), (0, -vector_rows % 16), (0, 0)))
    d_w_qkv = contract_rows(normed1, d_qkv16).astype(BF16).reshape(n_fsdp, n_ctx, chunk_rows, -1)
    pieces, out_sum, vector = ring_sum(
        (d_w_qkv, d_w_out[None], parts),
        (
            (0, 0, q_cols, 1),
            (0, q_cols, d_w_qkv.shape[-1], -1),
            (1, 0, side, 1),
            (1, side, D, -1),
            (2, 0, few, 1),
        ),
        (0, 2),
        n_fsdp,
        8,
    )
    qkv_sum = by_columns([pieces[f] for f in range(n_fsdp)])
    vector = jnp.sum(vector.astype(F32), 0)[:vector_rows].astype(BF16)
    vector = jnp.pad(vector, ((0, chunk_rows - vector_rows), (0, 0)))
    attention_sum, d_w_down = ring_gather(
        (jnp.concatenate([qkv_sum, out_sum[0], vector], -1), down_sum[0]), n_ctx, 9
    )
    d_w_down = d_w_down.reshape(n_ctx * down_rows, D)[:ff_shard].astype(F32)
    vector = attention_sum[:, :vector_rows, -few:].astype(F32).reshape(-1)
    attention_sum = attention_sum.reshape(d_shard, -1)
    qkv_width = qkv_sum.shape[-1]
    d_w_qkv = attention_sum[:, :qkv_width].astype(F32)
    d_w_out = attention_sum[:, qkv_width : qkv_width + D].astype(F32)
    d_gain_attn = vector[:d_shard]
    d_gain_mlp = vector[d_shard : 2 * d_shard]
    d_b_qkv = vector[2 * d_shard : 2 * d_shard + b_qkv.shape[0]]

    return (
        block_output,
        d_tokens,
        d_gain_attn,
        d_w_qkv,
        d_b_qkv,
        d_w_out,
        d_gain_mlp,
        d_w_gate_up,
        d_w_down,
    )


def solution(mesh):
    placed = (
        P("ctx", None, "fsdp", None),
        P(),
        P("fsdp"),
        P("fsdp", None),
        P("fsdp"),
        P("fsdp", None),
        P("fsdp"),
        P("fsdp", None, None),
        P("fsdp", None),
        P("ctx", None, "fsdp", None),
    )
    return jax.shard_map(
        body,
        mesh=mesh,
        in_specs=placed,
        out_specs=(
            P("ctx", None, "fsdp", None),
            P("ctx", None, "fsdp", None),
            P("fsdp"),
            P("fsdp", None),
            P("fsdp"),
            P("fsdp", None),
            P("fsdp"),
            P("fsdp", None, None),
            P("fsdp", None),
        ),
        check_vma=False,
    )
```

```python
import functools

import jax
import jax.numpy as jnp
from jax import lax
from jax.experimental import pallas as pl
from jax.experimental.layout import Layout, with_layout_constraint
from jax.experimental.pallas import tpu as pltpu
from jax.sharding import PartitionSpec as P

D = 1536
HEADS = 12
KV_HEADS = 2
HEAD_DIM = 128

eps = 1e-06
rope_base = 1000000.0
F32 = jnp.float32
BF16 = jnp.bfloat16
VMEM_LIMIT = 60 * 1024 * 1024


def rope_tables(position):
    half = HEAD_DIM // 2
    inverse = rope_base ** (-(jnp.arange(half, dtype=F32) * 2.0 / HEAD_DIM))
    angle = position.astype(F32)[:, None] * inverse[None, :]
    return (jnp.cos(angle)[:, None, :], jnp.sin(angle)[:, None, :])


def rotate(vectors, cosines, sines):
    half = HEAD_DIM // 2
    first, second = (vectors[..., :half], vectors[..., half:])
    return jnp.concatenate([first * cosines - second * sines, second * cosines + first * sines], -1)


def unrotate(grads, cosines, sines):
    half = HEAD_DIM // 2
    first, second = (grads[..., :half], grads[..., half:])
    return jnp.concatenate([first * cosines + second * sines, second * cosines - first * sines], -1)


def rms_scale(values):
    return lax.rsqrt(jnp.mean(values * values, -1, keepdims=True) + eps)


def rms_backward(values, scale_rows, gain, d_normed):
    d_gain = jnp.sum(d_normed * values * scale_rows, 0)
    d_inner = d_normed * gain
    d_values = scale_rows * d_inner - values * scale_rows**3 * jnp.mean(
        d_inner * values, -1, keepdims=True
    )
    return (d_values, d_gain)


def dot(left, right, contract):
    return lax.dot_general(left, right, (contract, ((), ())), preferred_element_type=F32)


def contract_rows(left, right):
    return dot(left, right, ((0,), (0,)))


def contract_cols(left, right):
    return dot(left, right, ((1,), (1,)))


def stacked_heads(ref, which, heads):
    return jnp.concatenate(
        [ref[which, :, h * HEAD_DIM : (h + 1) * HEAD_DIM] for h in range(heads)], 0
    )


def causal(block_len, heads):
    keys = lax.broadcasted_iota(jnp.int32, (block_len, block_len), 0)
    queries = lax.broadcasted_iota(jnp.int32, (block_len, block_len), 1)
    return jnp.concatenate([keys <= queries] * heads, 1)


def attend_kernel(heads, table, ids, q_ref, kv_ref, o_ref, lse_ref):
    block_len = q_ref.shape[1]
    cols = heads * block_len
    scale = HEAD_DIM ** (-0.5)
    for which in range(2):
        last = ids[which]
        query = stacked_heads(q_ref, which, heads)

        def step(block, carry, masked=False):
            highest, total, acc = carry
            start = pl.multiple_of(table[block] * block_len, block_len)
            key = kv_ref[pl.ds(start, block_len), :HEAD_DIM]
            value = kv_ref[pl.ds(start, block_len), HEAD_DIM:]
            scores = contract_cols(key, query) * scale
            if masked:
                scores = jnp.where(causal(block_len, heads), scores, -1e30)
            new_high = jnp.maximum(highest, jnp.max(scores, 0, keepdims=True))
            probs = jnp.exp(scores - new_high)
            fade = jnp.exp(highest - new_high)
            total = total * fade + jnp.sum(probs, 0, keepdims=True)
            acc = acc * fade + contract_rows(value, probs.astype(BF16))
            return (new_high, total, acc)

        begin = (
            jnp.full((1, cols), -1e30, F32),
            jnp.zeros((1, cols), F32),
            jnp.zeros((HEAD_DIM, cols), F32),
        )
        carry = lax.fori_loop(0, last, step, begin)
        highest, total, acc = step(last, carry, True)
        lse_ref[which] = highest + jnp.log(total)
        out = (acc / total).T
        for h in range(heads):
            o_ref[which, :, h * HEAD_DIM : (h + 1) * HEAD_DIM] = out[
                h * block_len : (h + 1) * block_len
            ].astype(BF16)


def attend_back_kernel(
    heads, table, ids, q_ref, kv_ref, o_ref, do_ref, lse_ref, dq_ref, dkv_ref, sums
):
    block_len = q_ref.shape[1]
    cols = heads * block_len
    scale = HEAD_DIM ** (-0.5)
    sums[...] = jnp.zeros_like(sums)
    for which in range(2):
        last = ids[which]
        query = stacked_heads(q_ref, which, heads)
        d_out = stacked_heads(do_ref, which, heads)
        out = stacked_heads(o_ref, which, heads)
        delta = jnp.sum((d_out.astype(F32) * out.astype(F32)).T, 0, keepdims=True)
        lse = lse_ref[which]

        def step(block, d_query, masked=False):
            start = pl.multiple_of(table[block] * block_len, block_len)
            key = kv_ref[pl.ds(start, block_len), :HEAD_DIM]
            value = kv_ref[pl.ds(start, block_len), HEAD_DIM:]
            scores = contract_cols(key, query) * scale
            probs = jnp.exp(scores - lse)
            if masked:
                probs = jnp.where(causal(block_len, heads), probs, 0.0)
            d_probs = contract_cols(value, d_out)
            d_scores = (probs * (d_probs - delta)).astype(BF16)
            sums[pl.ds(start, block_len), :HEAD_DIM] += dot(d_scores, query, ((1,), (0,)))
            sums[pl.ds(start, block_len), HEAD_DIM:] += dot(
                probs.astype(BF16), d_out, ((1,), (0,))
            )
            return d_query + contract_rows(key, d_scores)

        d_query = lax.fori_loop(0, last, step, jnp.zeros((HEAD_DIM, cols), F32))
        d_query = step(last, d_query, True)
        d_query = (d_query * scale).T
        for h in range(heads):
            dq_ref[which, :, h * HEAD_DIM : (h + 1) * HEAD_DIM] = d_query[
                h * block_len : (h + 1) * block_len
            ]
    dkv_ref[:, :HEAD_DIM] = (sums[:, :HEAD_DIM] * scale).astype(BF16)
    dkv_ref[:, HEAD_DIM:] = sums[:, HEAD_DIM:].astype(BF16)


def in_vmem(count):
    return [pl.BlockSpec(memory_space=pltpu.VMEM)] * count


def in_smem(count):
    return [pl.BlockSpec(memory_space=pltpu.SMEM)] * count


def attend(table, ids, query, keys_values, heads):
    _, block_len, width = query.shape
    tall = keys_values.shape[0]
    return pl.pallas_call(
        functools.partial(attend_kernel, heads),
        out_shape=(
            jax.ShapeDtypeStruct(query.shape, BF16),
            jax.ShapeDtypeStruct((2, 1, heads * block_len), F32),
        ),
        in_specs=in_smem(2) + in_vmem(2),
        out_specs=tuple(in_vmem(2)),
        compiler_params=pltpu.CompilerParams(vmem_limit_bytes=VMEM_LIMIT),
        cost_estimate=pl.CostEstimate(
            flops=2 * tall * block_len * width * 2,
            bytes_accessed=tall * 512,
            transcendentals=tall * heads * block_len,
        ),
        name="attend",
    )(table, ids, query, keys_values)


def attend_back(table, ids, query, keys_values, out, d_out, lse, heads):
    _, block_len, width = query.shape
    tall = keys_values.shape[0]
    return pl.pallas_call(
        functools.partial(attend_back_kernel, heads),
        out_shape=(
            jax.ShapeDtypeStruct(query.shape, F32),
            jax.ShapeDtypeStruct(keys_values.shape, BF16),
        ),
        in_specs=in_smem(2) + in_vmem(5),
        out_specs=tuple(in_vmem(2)),
        scratch_shapes=[pltpu.VMEM(keys_values.shape, F32)],
        compiler_params=pltpu.CompilerParams(vmem_limit_bytes=VMEM_LIMIT),
        cost_estimate=pl.CostEstimate(
            flops=5 * tall * block_len * width * 2,
            bytes_accessed=tall * 1024,
            transcendentals=tall * heads * block_len,
        ),
        name="attend_back",
    )(table, ids, query, keys_values, out, d_out, lse)


MESH = pl.DeviceIdType.MESH


def greet(devices):
    barrier = pltpu.get_barrier_semaphore()
    for device in devices:
        pl.semaphore_signal(barrier, inc=1, device_id=device, device_id_type=MESH)
    pl.semaphore_wait(barrier, len(devices))


def remote(src, dst, send, recv, device):
    return pltpu.make_async_remote_copy(
        src_ref=src, dst_ref=dst, send_sem=send, recv_sem=recv, device_id=device, device_id_type=MESH
    )


def group_places(n):
    ctx = lax.axis_index("ctx")
    me = lax.axis_index("fsdp")
    partner = me + 1 - 2 * (me % 2)
    others = [(me + 2 * k) % n for k in range(1, n // 2)]
    senders = [(me + n - 2 * k) % n for k in range(1, n // 2)]
    return ctx, me, partner, others, senders


def sum_phases(mode, n, cuts, *refs):
    gathers = mode != "input"
    if mode == "attention":
        partial, tokens, gain, hidden_out, all_out = refs[:5]
    elif mode == "mlp":
        partial, hidden_in, cot, gain, d_out, all_out, d_gain = refs[:7]
    else:
        partial, tokens, d_hidden_in, gain, d_out, d_gain = refs[:6]
    near, summed, far, stage, near_s, near_r, far_s, far_r, own_s, own_r, out_s, out_r, fwd_s, fwd_r = refs[-14:]
    ctx, me, partner, others, senders = group_places(n)
    chips = n // 2
    rows = partial.shape[2]
    piece = rows // cuts
    chunks = [(w, i * piece) for w in range(2) for i in range(cuts)]

    def part(ref, w, lead, start):
        return ref.at[w, lead, pl.ds(start, piece)]

    first = []
    for c, (w, start) in enumerate(chunks):
        for j in range(chips):
            target = (partner + 2 * (j + 1)) % n
            copy = remote(
                part(partial, w, target, start),
                part(near, w, j, start),
                near_s.at[c, j],
                near_r.at[c, j],
                (ctx, partner),
            )
            copy.start()
            first.append(copy)
    yield

    second = []

    def post(c):
        w, start = chunks[c]
        for j in range(chips - 1):
            copy = remote(
                part(summed, w, j, start),
                part(far, w, j, start),
                far_s.at[c, j],
                far_r.at[c, j],
                (ctx, others[j]),
            )
            copy.start()
            second.append(copy)

    for c, (w, start) in enumerate(chunks):
        span = pl.ds(start, piece)
        for j in range(chips - 1):
            first[c * chips + j].wait()
            target = (me + 2 * (j + 1)) % n
            summed[w, j, span] = (
                partial[w, target, span].astype(F32) + near[w, j, span].astype(F32)
            ).astype(BF16)
        if c:
            post(c - 1)
    post(len(chunks) - 1)
    yield

    if mode != "attention":
        d_gain[...] = jnp.zeros_like(d_gain)
    third = []

    def spread(c):
        w, start = chunks[c]
        src = stage.at[w, pl.ds(start, piece)]
        for k in range(chips - 1):
            copy = remote(src, part(all_out, w, me, start), out_s.at[c, k], out_r.at[c, k], (ctx, others[k]))
            copy.start()
            third.append(copy)
        copy = remote(src, part(all_out, w, me, start), own_s.at[c], own_r.at[c], (ctx, partner))
        copy.start()
        return copy

    near_copies = []
    for c, (w, start) in enumerate(chunks):
        span = pl.ds(start, piece)
        first[c * chips + chips - 1].wait()
        total = partial[w, me, span].astype(F32) + near[w, chips - 1, span].astype(F32)
        for j in range(chips - 1):
            second[c * (chips - 1) + j].wait()
            total += far[w, j, span].astype(F32)
        if mode == "attention":
            hidden = tokens[w, span].astype(F32) + total
            hidden_out[w, span] = hidden
            rounded = (hidden * rms_scale(hidden) * gain[...]).astype(BF16)
        elif mode == "mlp":
            hidden = hidden_in[w, span]
            d_norm, gain_part = rms_backward(hidden, rms_scale(hidden), gain[...], total)
            d_gain[...] += gain_part[None]
            d_hidden = cot[w, span].astype(F32) + d_norm
            d_out[w, span] = d_hidden
            rounded = d_hidden.astype(BF16)
        else:
            values = tokens[w, span].astype(F32)
            d_norm, gain_part = rms_backward(values, rms_scale(values), gain[...], total)
            d_gain[...] += gain_part[None]
            d_out[w, span] = d_hidden_in[w, span] + d_norm
        if gathers:
            stage[w, span] = rounded
            all_out[w, me, span] = rounded
            if c:
                near_copies.append(spread(c - 1))
    if not gathers:
        return
    near_copies.append(spread(len(chunks) - 1))
    yield

    forwards = []
    for c, (w, start) in enumerate(chunks):
        for k in range(chips - 1):
            third[c * (chips - 1) + k].wait_recv()
            block = part(all_out, w, senders[k], start)
            copy = remote(block, block, fwd_s.at[c, k], fwd_r.at[c, k], (ctx, partner))
            copy.start()
            forwards.append(copy)
    yield
    for copy in third:
        copy.wait_send()
    for copy in near_copies + forwards:
        copy.wait()


def sum_kernel(mode, n, cuts, *refs):
    ctx, _, partner, others, _ = group_places(n)
    greet([(ctx, partner)] + [(ctx, o) for o in others])
    for _ in sum_phases(mode, n, cuts, *refs):
        pass


def sum_shapes(mode, partial):
    _, n, rows, width = partial.shape
    chips = n // 2
    row_shape = (2, rows, width)
    full = jax.ShapeDtypeStruct(row_shape, F32)
    gathered = jax.ShapeDtypeStruct(partial.shape, BF16)
    gain_sum = jax.ShapeDtypeStruct((1, width), F32)
    out_shape = {
        "attention": (full, gathered),
        "mlp": (full, gathered, gain_sum),
        "input": (full, gain_sum),
    }[mode]
    dma = pltpu.SemaphoreType.DMA
    chunks = 2 * SUM_CUTS
    scratch = [
        pltpu.VMEM((2, chips, rows, width), BF16),
        pltpu.VMEM((2, chips - 1, rows, width), BF16),
        pltpu.VMEM((2, chips - 1, rows, width), BF16),
        pltpu.VMEM(row_shape, BF16),
        dma((chunks, chips)),
        dma((chunks, chips)),
        dma((chunks, chips - 1)),
        dma((chunks, chips - 1)),
        dma((chunks,)),
        dma((chunks,)),
        dma((chunks, chips - 1)),
        dma((chunks, chips - 1)),
        dma((chunks, chips - 1)),
        dma((chunks, chips - 1)),
    ]
    return out_shape, scratch


SUM_CUTS = 2


def group_sum(mode, partial, *operands, collective):
    _, n, rows, width = partial.shape
    out_shape, scratch = sum_shapes(mode, partial)
    return pl.pallas_call(
        functools.partial(sum_kernel, mode, n, SUM_CUTS),
        out_shape=out_shape,
        in_specs=in_vmem(1 + len(operands)),
        out_specs=tuple(in_vmem(len(out_shape))),
        scratch_shapes=scratch,
        compiler_params=pltpu.CompilerParams(
            vmem_limit_bytes=VMEM_LIMIT, collective_id=collective, has_side_effects=True
        ),
        cost_estimate=pl.CostEstimate(
            flops=20 * rows * width, bytes_accessed=60_000_000, transcendentals=0
        ),
        name="group_sum_" + mode,
    )(partial, *operands)


def ring_index(place, n):
    late = place // (n // 2)
    return (1 - late) * 2 * place + late * (2 * n - 1 - 2 * place)


def ring_place(index, n):
    odd = index % 2
    return (1 - odd) * (index // 2) + odd * (n - 1 - index // 2)


def share_kernel(n, own, out, right_s, right_r, left_s, left_r, near_s, near_r):
    ctx = lax.axis_index("ctx")
    me = lax.axis_index("fsdp")
    which = me % 2
    partner = me + 1 - 2 * which
    place = ring_place(ctx, n)
    right = (ring_index((place + 1) % n, n), me)
    left = (ring_index((place + n - 1) % n, n), me)
    greet([right, left, (ctx, partner)])

    def block(offset):
        return out.at[ring_index((place + n + offset) % n, n), which]

    def to_right(step):
        src = own.at[which] if step == 0 else block(-step)
        return remote(src, block(-step), right_s.at[step], right_r.at[step], right)

    def to_left(step):
        src = own.at[which] if step == 0 else block(step)
        return remote(src, block(step), left_s.at[step], left_r.at[step], left)

    rights, lefts = n // 2, n - 1 - n // 2
    sent = [to_right(0), to_left(0)]
    for copy in sent:
        copy.start()
    out[ctx] = own[...]
    going = [sent[0], sent[1]]
    for step in range(1, rights + 1):
        going[0].wait_recv()
        if step < rights:
            going[0] = to_right(step)
            going[0].start()
            sent.append(going[0])
        hand = remote(block(-step), block(-step), near_s.at[step - 1], near_r.at[step - 1], (ctx, partner))
        hand.start()
        sent.append(hand)
        if step <= lefts:
            going[1].wait_recv()
            if step < lefts:
                going[1] = to_left(step)
                going[1].start()
                sent.append(going[1])
            slot = rights + step - 1
            hand = remote(block(step), block(step), near_s.at[slot], near_r.at[slot], (ctx, partner))
            hand.start()
            sent.append(hand)
    for copy in sent:
        copy.wait_send()
    for step in range(1, rights + 1):
        remote(block(-step), block(-step), near_s.at[step - 1], near_r.at[step - 1], (ctx, partner)).wait_recv()
    for step in range(1, lefts + 1):
        slot = rights + step - 1
        remote(block(step), block(step), near_s.at[slot], near_r.at[slot], (ctx, partner)).wait_recv()


def share_keys(own, n, collective):
    dma = pltpu.SemaphoreType.DMA
    return pl.pallas_call(
        functools.partial(share_kernel, n),
        out_shape=jax.ShapeDtypeStruct((n,) + own.shape, BF16),
        in_specs=in_vmem(1),
        out_specs=in_vmem(1)[0],
        scratch_shapes=[dma((n // 2,))] * 4 + [dma((n - 1,))] * 2,
        compiler_params=pltpu.CompilerParams(
            vmem_limit_bytes=VMEM_LIMIT, collective_id=collective, has_side_effects=True
        ),
        cost_estimate=pl.CostEstimate(flops=0, bytes_accessed=60_000_000, transcendentals=0),
        name="share_keys",
    )(own)


def return_kernel(n, partial, out, near, summed, far, near_s, near_r, far_s, far_r):
    ctx = lax.axis_index("ctx")
    me = lax.axis_index("fsdp")
    which = me % 2
    partner = me + 1 - 2 * which
    others = [(ctx + k) % n for k in range(1, n)]
    greet([(ctx, partner)] + [(o, me) for o in others])
    order = others + [ctx]
    first = []
    for k, target in enumerate(order):
        copy = remote(partial.at[target, 1 - which], near.at[k], near_s.at[k], near_r.at[k], (ctx, partner))
        copy.start()
        first.append(copy)
    second = []

    def post(k):
        copy = remote(summed.at[k], far.at[k], far_s.at[k], far_r.at[k], (others[k], me))
        copy.start()
        second.append(copy)

    for k in range(n - 1):
        first[k].wait()
        summed[k] = (partial[others[k], which].astype(F32) + near[k].astype(F32)).astype(BF16)
        if k:
            post(k - 1)
    post(n - 2)
    out[1 - which] = jnp.zeros(out.shape[1:], F32)
    first[n - 1].wait()
    out[which] = partial[ctx, which].astype(F32) + near[n - 1].astype(F32)
    for k in range(n - 1):
        second[k].wait()
        out[which] += far[k].astype(F32)


def return_grads(partial, collective):
    n = partial.shape[0]
    block = partial.shape[2:]
    dma = pltpu.SemaphoreType.DMA
    return pl.pallas_call(
        functools.partial(return_kernel, n),
        out_shape=jax.ShapeDtypeStruct(partial.shape[1:], F32),
        in_specs=in_vmem(1),
        out_specs=in_vmem(1)[0],
        scratch_shapes=[
            pltpu.VMEM((n,) + block, BF16),
            pltpu.VMEM((n - 1,) + block, BF16),
            pltpu.VMEM((n - 1,) + block, BF16),
            dma((n,)),
            dma((n,)),
            dma((n - 1,)),
            dma((n - 1,)),
        ],
        compiler_params=pltpu.CompilerParams(
            vmem_limit_bytes=VMEM_LIMIT, collective_id=collective, has_side_effects=True
        ),
        cost_estimate=pl.CostEstimate(flops=0, bytes_accessed=80_000_000, transcendentals=0),
        name="return_grads",
    )(partial)


def ring_sum_kernel(n, members, plan, swaps, arrays, mode, extra_ins, extra_outs, *refs):
    ins, refs = refs[:arrays], refs[arrays:]
    side_ins, refs = refs[:extra_ins], refs[extra_ins:]
    outs, refs = refs[:arrays], refs[arrays:]
    side_outs, refs = refs[:extra_outs], refs[extra_outs:]
    count = len(plan)
    arrived, stages, sends, recvs = (refs[i * count : (i + 1) * count] for i in range(4))
    refs = refs[4 * count :]
    done, swap_s, swap_r = (refs[i * len(swaps) : (i + 1) * len(swaps)] for i in range(3))
    refs = refs[3 * len(swaps) :]
    ctx = lax.axis_index("ctx")
    me = lax.axis_index("fsdp")
    place = ring_place(ctx, n)
    around = {step: (ring_index((place + n + step) % n, n), me) for step in (1, -1)}
    greet([around[1], around[-1]] + [(ctx, (me + k) % members) for k in range(1, members)])
    beside = iter(())
    if mode:
        beside = sum_phases(mode, members, SUM_CUTS, *side_ins, *side_outs, *refs)

    def copy(i, hop, src):
        step = plan[i][3]
        return remote(src, arrived[i].at[hop], sends[i].at[hop], recvs[i].at[hop], around[step])

    def chunk(i, hop):
        step = plan[i][3]
        return ring_index((place + n * n - step * (hop + 1)) % n, n)

    def window(i, group, hop):
        which, low, high, _ = plan[i]
        return ins[which][group, chunk(i, hop), :, low:high].astype(F32)

    def first(i):
        which, low, high, _ = plan[i]
        return copy(i, 0, ins[which].at[:, chunk(i, 0), :, pl.ds(low, high - low)])

    for i in range(count):
        first(i).start()
    next(beside, None)

    def add(i, hop, store):
        copy(i, hop - 1, stages[i].at[0]).wait_recv()

        def group_add(group, carry):
            store(group, (arrived[i][hop - 1, group].astype(F32) + window(i, group, hop)).astype(BF16))
            return carry

        lax.fori_loop(0, ins[plan[i][0]].shape[0], group_add, 0)

    def one_hop(hop, carry):
        slot = hop % 2
        for i in range(count):
            @pl.when(hop > 2)
            def _():
                copy(i, hop - 2, stages[i].at[slot]).wait_send()

            def store(group, value):
                stages[i][slot, group] = value

            add(i, hop, store)
            if i:
                copy(i - 1, hop, stages[i - 1].at[slot]).start()
        copy(count - 1, hop, stages[count - 1].at[slot]).start()
        return carry

    hop = 1
    if mode:
        for _ in range(min(4, n - 3)):
            one_hop(jnp.int32(hop), 0)
            hop += 1
            next(beside, None)
    lax.fori_loop(hop, n - 1, one_hop, 0)
    for i, (which, low, high, _) in enumerate(plan):
        target = done[swaps.index(which)] if which in swaps else outs[which]

        def store(group, value):
            target[group, :, low:high] = value

        add(i, n - 1, store)
    swapped = []
    for j, which in enumerate(swaps):
        for k in range(1, members):
            other = (me + k) % members
            swapped.append(
                remote(
                    done[j].at[other],
                    outs[which].at[me],
                    swap_s[j].at[k - 1],
                    swap_r[j].at[k - 1],
                    (ctx, other),
                )
            )
            swapped[-1].start()
        outs[which][me] = done[j][me]
    for _ in beside:
        pass
    for i in range(count):
        first(i).wait_send()
        for hop in (n - 3, n - 2):
            copy(i, hop, stages[i].at[hop % 2]).wait_send()
    for move in swapped:
        move.wait()


def ring_sum(arrays, plan, swaps, members, collective, mode=None, operands=()):
    n = arrays[0].shape[1]
    dma = pltpu.SemaphoreType.DMA
    blocks = [
        (arrays[which].shape[0], arrays[which].shape[2], high - low) for which, low, high, _ in plan
    ]
    sums = [(a.shape[0],) + a.shape[2:] for a in arrays]
    extra_shape, extra_scratch = sum_shapes(mode, operands[0]) if mode else ((), [])
    out_shape = tuple(jax.ShapeDtypeStruct(shape, BF16) for shape in sums) + tuple(extra_shape)
    return pl.pallas_call(
        functools.partial(
            ring_sum_kernel, n, members, plan, swaps, len(arrays), mode, len(operands), len(extra_shape)
        ),
        out_shape=out_shape,
        in_specs=in_vmem(len(arrays) + len(operands)),
        out_specs=tuple(in_vmem(len(out_shape))),
        scratch_shapes=[pltpu.VMEM((n - 1,) + b, BF16) for b in blocks]
        + [pltpu.VMEM((2,) + b, BF16) for b in blocks]
        + [dma((n - 1,)) for _ in blocks] * 2
        + [pltpu.VMEM(sums[which], BF16) for which in swaps]
        + [dma((members - 1,)) for _ in swaps] * 2
        + extra_scratch,
        compiler_params=pltpu.CompilerParams(
            vmem_limit_bytes=VMEM_LIMIT, collective_id=collective, has_side_effects=True
        ),
        cost_estimate=pl.CostEstimate(flops=0, bytes_accessed=200_000_000, transcendentals=0),
        name="ring_sum",
    )(*arrays, *operands)


def ring_gather_kernel(n, count, *refs):
    owns, outs, sends, recvs = (refs[i * count : (i + 1) * count] for i in range(4))
    ctx = lax.axis_index("ctx")
    me = lax.axis_index("fsdp")
    place = ring_place(ctx, n)
    around = {step: (ring_index((place + n + step) % n, n), me) for step in (1, -1)}
    greet([around[1], around[-1]])
    far = n // 2

    def copy(i, step, half, hop):
        middle = owns[i].shape[-1] // 2
        lanes = pl.ds(half * middle, middle)
        block = outs[i].at[ring_index((place + n - step * hop) % n, n), :, lanes]
        src = block if hop else owns[i].at[:, lanes]
        row = half if step == 1 else 2 + half
        return remote(src, block, sends[i].at[row, hop], recvs[i].at[row, hop], around[step])

    def hops(step, half):
        return far if (step == 1) == (half == 0) else far - 1

    lines = [(i, step, half) for step, half in ((1, 0), (-1, 1), (1, 1), (-1, 0)) for i in range(count)]
    for i, step, half in lines:
        copy(i, step, half, 0).start()
    for own, out in zip(owns, outs):
        out[ctx] = own[...]
    for hop in range(1, far + 1):
        for i, step, half in lines:
            if hop <= hops(step, half):
                copy(i, step, half, hop - 1).wait_recv()
                if hop < hops(step, half):
                    copy(i, step, half, hop).start()
    for i, step, half in lines:
        for hop in range(hops(step, half)):
            copy(i, step, half, hop).wait_send()


def ring_gather(owns, n, collective):
    count = len(owns)
    return pl.pallas_call(
        functools.partial(ring_gather_kernel, n, count),
        out_shape=tuple(jax.ShapeDtypeStruct((n,) + own.shape, BF16) for own in owns),
        in_specs=in_vmem(count),
        out_specs=tuple(in_vmem(count)),
        scratch_shapes=[pltpu.SemaphoreType.DMA((4, n // 2))] * (2 * count),
        compiler_params=pltpu.CompilerParams(
            vmem_limit_bytes=VMEM_LIMIT, collective_id=collective, has_side_effects=True
        ),
        cost_estimate=pl.CostEstimate(flops=0, bytes_accessed=120_000_000, transcendentals=0),
        name="ring_gather",
    )(*owns)


def weave_kernel(planes, out):
    for e in range(2):
        out[:, e, :] = planes[e].astype(F32)


def weave(planes):
    _, rows, lanes = planes.shape
    block = 32 if rows % 32 == 0 else rows
    return pl.pallas_call(
        weave_kernel,
        grid=(rows // block,),
        out_shape=jax.ShapeDtypeStruct((rows, 2, lanes), F32),
        in_specs=[pl.BlockSpec((2, block, lanes), lambda i: (0, i, 0))],
        out_specs=pl.BlockSpec((block, 2, lanes), lambda i: (i, 0, 0)),
        cost_estimate=pl.CostEstimate(
            flops=0, bytes_accessed=12 * rows * lanes, transcendentals=0
        ),
        name="weave",
    )(planes)


def project_kernel(heads, x_ref, gain, w_ref, bias, cos_ref, sin_ref, normed_ref, q_ref, kv_ref):
    values = x_ref[...].astype(F32)
    normed = (values * rms_scale(values) * gain[...]).astype(BF16)
    normed_ref[...] = normed
    qkv = jnp.dot(normed, w_ref[...], preferred_element_type=F32) + bias[...]
    cosines, sines = cos_ref[...], sin_ref[...]
    for h in range(heads + 1):
        vector = qkv[:, h * HEAD_DIM : (h + 1) * HEAD_DIM]
        turned = vector * cosines + pltpu.roll(vector, HEAD_DIM // 2, 1) * sines
        if h < heads:
            q_ref[:, h * HEAD_DIM : (h + 1) * HEAD_DIM] = turned.astype(BF16)
        else:
            kv_ref[:, :HEAD_DIM] = turned.astype(BF16)
    kv_ref[:, HEAD_DIM:] = qkv[:, (heads + 1) * HEAD_DIM :].astype(BF16)


def project(x_all, gain, weights, bias, cosines, sines, heads):
    rows = x_all.shape[0]
    block = 128
    width = weights.shape[1]

    def tall(lanes):
        return pl.BlockSpec((block, lanes), lambda i: (i, 0))

    def fixed(shape):
        return pl.BlockSpec(shape, lambda i: (0, 0))

    lanes = (D, heads * HEAD_DIM, 2 * HEAD_DIM)
    return pl.pallas_call(
        functools.partial(project_kernel, heads),
        grid=(rows // block,),
        out_shape=tuple(jax.ShapeDtypeStruct((rows, n), BF16) for n in lanes),
        in_specs=[
            tall(D),
            fixed((1, D)),
            fixed((D, width)),
            fixed((1, width)),
            tall(HEAD_DIM),
            tall(HEAD_DIM),
        ],
        out_specs=tuple(tall(n) for n in lanes),
        compiler_params=pltpu.CompilerParams(vmem_limit_bytes=VMEM_LIMIT),
        cost_estimate=pl.CostEstimate(
            flops=2 * rows * D * width, bytes_accessed=4 * rows * D + 2 * D * width, transcendentals=0
        ),
        name="project",
    )(x_all, gain, weights, bias, cosines, sines)


def exchange(pieces, axis):
    return lax.all_to_all(pieces, axis, split_axis=0, concat_axis=0, tiled=True)


def together(*values):
    return lax.optimization_barrier(values)


def body(tokens, pairing, gain_attn, w_qkv, b_qkv, w_out, gain_mlp, w_gate_up, w_down, cotangent):
    half_rows = tokens.shape[2]
    n_ctx = lax.axis_size("ctx")
    n_fsdp = lax.axis_size("fsdp")
    ctx_index = lax.axis_index("ctx")
    fsdp_index = lax.axis_index("fsdp")
    stretch_len = half_rows * n_fsdp
    rows = 2 * stretch_len
    local_count = 2 * half_rows
    q_width = HEADS * HEAD_DIM
    kv_width = KV_HEADS * HEAD_DIM
    heads = HEADS // n_fsdp
    q_cols = heads * HEAD_DIM
    d_shard = w_qkv.shape[0]
    ff_shard = w_down.shape[0]

    owner_range = jnp.arange(n_ctx, dtype=jnp.int32)
    own_first = jnp.sum(jnp.where(owner_range == ctx_index, pairing, 0))
    ids = jnp.stack([own_first, 2 * n_ctx - 1 - own_first])
    inverse_pair = jnp.sum(
        owner_range[:, None] * (pairing[:, None] == owner_range[None, :]).astype(jnp.int32), 0
    )
    table = jnp.concatenate([2 * inverse_pair, 2 * inverse_pair[::-1] + 1])
    position = (
        ids[:, None] * stretch_len + jnp.arange(stretch_len, dtype=jnp.int32)[None, :]
    ).reshape(rows)
    kv_of = [f * KV_HEADS // n_fsdp for f in range(n_fsdp)]
    my_kv = fsdp_index * KV_HEADS // n_fsdp

    small = lax.all_gather(jnp.concatenate([gain_attn, gain_mlp, b_qkv]), "fsdp", axis=0)
    small, w_qkv, w_gate_up = together(small, w_qkv, w_gate_up)
    gain_one = small[:, :d_shard].reshape(D).astype(F32)
    gain_two = small[:, d_shard : 2 * d_shard].reshape(D).astype(F32)
    bias = small[:, 2 * d_shard :].reshape(-1).astype(F32)
    x_all = lax.all_gather(tokens[0], "fsdp", axis=1, tiled=True).reshape(rows, D)
    qkv_pieces = jnp.stack(
        [
            jnp.concatenate(
                [
                    w_qkv[:, f * q_cols : (f + 1) * q_cols],
                    w_qkv[:, q_width + kv_of[f] * HEAD_DIM : q_width + (kv_of[f] + 1) * HEAD_DIM],
                    w_qkv[
                        :,
                        q_width + kv_width + kv_of[f] * HEAD_DIM : q_width
                        + kv_width
                        + (kv_of[f] + 1) * HEAD_DIM,
                    ],
                ],
                1,
            )
            for f in range(n_fsdp)
        ]
    )
    w_qkv_cols = exchange(qkv_pieces, "fsdp").reshape(D, -1)
    bias_cols = jnp.concatenate(
        [
            lax.dynamic_slice_in_dim(bias, fsdp_index * q_cols, q_cols),
            lax.dynamic_slice_in_dim(bias, q_width + my_kv * HEAD_DIM, HEAD_DIM),
            lax.dynamic_slice_in_dim(bias, q_width + kv_width + my_kv * HEAD_DIM, HEAD_DIM),
        ]
    )
    gate_up_pieces = w_gate_up.reshape(d_shard, 2, n_fsdp, ff_shard).transpose(2, 1, 3, 0)
    gate_up_pieces = with_layout_constraint(gate_up_pieces, Layout((0, 1, 2, 3)))
    x_all, w_qkv_cols, gate_up_pieces = together(x_all, w_qkv_cols, gate_up_pieces)
    gate_up_cols = exchange(gate_up_pieces, "fsdp")

    cosines, sines = rope_tables(position)
    normed1, query, own_kv = project(
        x_all,
        gain_one[None],
        w_qkv_cols,
        bias_cols[None],
        jnp.concatenate([cosines[:, 0], cosines[:, 0]], 1),
        jnp.concatenate([-sines[:, 0], sines[:, 0]], 1),
        heads,
    )
    query = query.reshape(2, stretch_len, q_cols)
    keys_values = share_keys(own_kv.reshape(2, stretch_len, 2 * HEAD_DIM), n_ctx, 4)
    keys_values = keys_values.reshape(n_ctx * rows, 2 * HEAD_DIM)
    attended, lse = attend(table, ids, query, keys_values, heads)
    attended16 = attended.reshape(rows, q_cols)

    def scatter(partial):
        return lax.psum_scatter(
            partial.astype(BF16).reshape(2, stretch_len, D), "fsdp", scatter_dimension=1, tiled=True
        ).astype(F32).reshape(local_count, D)

    def by_member(partial):
        return partial.astype(BF16).reshape(2, n_fsdp, half_rows, D)

    tokens_own = tokens[0]
    hidden, normed2 = group_sum(
        "attention",
        by_member(jnp.dot(attended16, w_out, preferred_element_type=F32)),
        tokens_own,
        gain_two[None],
        collective=1,
    )
    normed2, cot_own = together(normed2, cotangent[0])
    normed2 = normed2.reshape(rows, D)
    cot_all = lax.all_gather(cot_own, "fsdp", axis=1, tiled=True).reshape(rows, D)
    w_gate_cols, w_up_cols = (gate_up_cols[:, e] for e in range(2))
    normed2_parts = normed2.reshape(rows, n_fsdp, d_shard)
    gate_val, up_val = (
        jnp.einsum("tsk,sfk->tf", normed2_parts, w, preferred_element_type=F32)
        for w in (w_gate_cols, w_up_cols)
    )
    sigmoid_gate = jax.nn.sigmoid(gate_val)
    act16 = (jax.nn.silu(gate_val) * up_val).astype(BF16)
    result = hidden.reshape(local_count, D) + scatter(jnp.dot(act16, w_down, preferred_element_type=F32))
    block_output = result.astype(BF16).reshape(tokens.shape)

    d_act = contract_cols(cot_all, w_down)
    d_gate16 = (d_act * up_val * sigmoid_gate * (1.0 + gate_val * (1.0 - sigmoid_gate))).astype(BF16)
    d_up16 = (d_act * gate_val * sigmoid_gate).astype(BF16)
    d_normed2 = sum(
        jnp.einsum("tf,sfk->tsk", d, w, preferred_element_type=F32)
        for d, w in ((d_gate16, w_gate_cols), (d_up16, w_up_cols))
    )
    def by_columns(pieces):
        queries = [pieces[f][..., :q_cols] for f in range(n_fsdp)]
        rest = []
        for part in range(2):
            lo = q_cols + part * HEAD_DIM
            for g in range(KV_HEADS):
                rest.append(
                    sum(
                        pieces[f][..., lo : lo + HEAD_DIM].astype(F32)
                        for f in range(n_fsdp)
                        if kv_of[f] == g
                    ).astype(pieces[0].dtype)
                )
        return jnp.concatenate(queries + rest, -1)

    chunk_rows = d_shard // n_ctx
    down_rows = -(-ff_shard // (16 * n_ctx)) * 16
    side = D // 2

    def padded(grad):
        extra = n_ctx * down_rows - grad.shape[0]
        return jnp.pad(grad, ((0, extra), (0, 0))).astype(BF16).reshape(n_ctx, down_rows, D)

    d_w_down = padded(contract_rows(act16, cot_all))
    d_w_gate, d_w_up = (
        contract_rows(normed2, piece).astype(BF16).reshape(n_fsdp, n_ctx, chunk_rows, ff_shard)
        for piece in (d_gate16, d_up16)
    )

    gate_sum, up_sum, down_sum, d_hidden, dh_all, d_gain_two = ring_sum(
        (d_w_gate, d_w_up, d_w_down[None]),
        ((0, 0, ff_shard, 1), (1, 0, ff_shard, -1), (2, 0, side, 1), (2, side, D, -1)),
        (0, 1),
        n_fsdp,
        7,
        "mlp",
        (by_member(d_normed2), hidden, cotangent[0], gain_two[None]),
    )
    planes = jnp.stack(
        [
            total.transpose(1, 0, 2).reshape(chunk_rows, n_fsdp * ff_shard)
            for total in (gate_sum, up_sum)
        ]
    )
    d_w_gate_up = weave(lax.all_gather(planes, "ctx", axis=1, tiled=True))
    dh_all = dh_all.reshape(rows, D)
    d_attended16 = contract_cols(dh_all, w_out).astype(BF16).reshape(2, stretch_len, q_cols)
    d_query, d_kv = attend_back(
        table, ids, query, keys_values, attended, d_attended16, lse, heads
    )
    d_kv_own = return_grads(d_kv.reshape(n_ctx, 2, stretch_len, 2 * HEAD_DIM), 5).reshape(rows, -1)

    d_w_out = contract_rows(attended16, dh_all).astype(BF16).reshape(n_ctx, chunk_rows, D)
    d_rotated = jnp.concatenate([d_query.reshape(rows, q_cols), d_kv_own[:, :HEAD_DIM]], 1)
    d_rotated = unrotate(
        d_rotated.reshape(rows, heads + 1, HEAD_DIM), cosines, sines
    ).reshape(rows, q_cols + HEAD_DIM)
    d_qkv = jnp.concatenate([d_rotated, d_kv_own[:, HEAD_DIM:]], 1)
    d_bias = jnp.sum(d_qkv, 0)
    d_qkv16 = d_qkv.astype(BF16)
    d_normed1 = contract_cols(d_qkv16, w_qkv_cols)
    x32 = x_all.astype(F32)
    d_gain_one = jnp.sum(d_normed1 * x32 * rms_scale(x32), 0)
    zeros = jnp.zeros_like(d_bias)
    d_bias_full = by_columns([jnp.where(fsdp_index == f, d_bias, zeros) for f in range(n_fsdp)])
    parts = jnp.concatenate(
        [v.reshape(n_fsdp, -1) for v in (d_gain_one, d_gain_two, d_bias_full)], 1
    ).astype(BF16)
    length = parts.shape[1]
    few = 2 * HEAD_DIM
    vector_rows = -(-length // (n_ctx * few))
    parts = jnp.pad(parts, ((0, 0), (0, n_ctx * vector_rows * few - length)))
    parts = parts.reshape(n_fsdp, n_ctx, vector_rows, few)
    parts = jnp.pad(parts, ((0, 0), (0, 0), (0, -vector_rows % 16), (0, 0)))
    d_w_qkv = contract_rows(normed1, d_qkv16).astype(BF16).reshape(n_fsdp, n_ctx, chunk_rows, -1)
    pieces, out_sum, vector, d_tokens, _ = ring_sum(
        (d_w_qkv, d_w_out[None], parts),
        (
            (0, 0, q_cols, 1),
            (0, q_cols, d_w_qkv.shape[-1], -1),
            (1, 0, side, 1),
            (1, side, D, -1),
            (2, 0, few, 1),
        ),
        (0, 2),
        n_fsdp,
        8,
        "input",
        (by_member(d_normed1), tokens_own, d_hidden, gain_one[None]),
    )
    d_tokens = d_tokens.reshape(tokens.shape)
    qkv_sum = by_columns([pieces[f] for f in range(n_fsdp)])
    vector = jnp.sum(vector.astype(F32), 0)[:vector_rows].astype(BF16)
    vector = jnp.pad(vector, ((0, chunk_rows - vector_rows), (0, 0)))
    attention_sum, d_w_down = ring_gather(
        (jnp.concatenate([qkv_sum, out_sum[0], vector], -1), down_sum[0]), n_ctx, 9
    )
    d_w_down = d_w_down.reshape(n_ctx * down_rows, D)[:ff_shard].astype(F32)
    vector = attention_sum[:, :vector_rows, -few:].astype(F32).reshape(-1)
    attention_sum = attention_sum.reshape(d_shard, -1)
    qkv_width = qkv_sum.shape[-1]
    d_w_qkv = attention_sum[:, :qkv_width].astype(F32)
    d_w_out = attention_sum[:, qkv_width : qkv_width + D].astype(F32)
    d_gain_attn = vector[:d_shard]
    d_gain_mlp = vector[d_shard : 2 * d_shard]
    d_b_qkv = vector[2 * d_shard : 2 * d_shard + b_qkv.shape[0]]

    return (
        block_output,
        d_tokens,
        d_gain_attn,
        d_w_qkv,
        d_b_qkv,
        d_w_out,
        d_gain_mlp,
        d_w_gate_up,
        d_w_down,
    )


def solution(mesh):
    placed = (
        P("ctx", None, "fsdp", None),
        P(),
        P("fsdp"),
        P("fsdp", None),
        P("fsdp"),
        P("fsdp", None),
        P("fsdp"),
        P("fsdp", None, None),
        P("fsdp", None),
        P("ctx", None, "fsdp", None),
    )
    return jax.shard_map(
        body,
        mesh=mesh,
        in_specs=placed,
        out_specs=(
            P("ctx", None, "fsdp", None),
            P("ctx", None, "fsdp", None),
            P("fsdp"),
            P("fsdp", None),
            P("fsdp"),
            P("fsdp", None),
            P("fsdp"),
            P("fsdp", None, None),
            P("fsdp", None),
        ),
        check_vma=False,
    )
```

```python
import functools

import jax
import jax.numpy as jnp
from jax import lax
from jax.experimental import pallas as pl
from jax.experimental.layout import Layout, with_layout_constraint
from jax.experimental.pallas import tpu as pltpu
from jax.sharding import PartitionSpec as P

D = 1536
HEADS = 12
KV_HEADS = 2
HEAD_DIM = 128

eps = 1e-06
rope_base = 1000000.0
F32 = jnp.float32
BF16 = jnp.bfloat16
VMEM_LIMIT = 60 * 1024 * 1024


def rope_tables(position):
    half = HEAD_DIM // 2
    inverse = rope_base ** (-(jnp.arange(half, dtype=F32) * 2.0 / HEAD_DIM))
    angle = position.astype(F32)[:, None] * inverse[None, :]
    return (jnp.cos(angle)[:, None, :], jnp.sin(angle)[:, None, :])


def rotate(vectors, cosines, sines):
    half = HEAD_DIM // 2
    first, second = (vectors[..., :half], vectors[..., half:])
    return jnp.concatenate([first * cosines - second * sines, second * cosines + first * sines], -1)


def unrotate(grads, cosines, sines):
    half = HEAD_DIM // 2
    first, second = (grads[..., :half], grads[..., half:])
    return jnp.concatenate([first * cosines + second * sines, second * cosines - first * sines], -1)


def rms_scale(values):
    return lax.rsqrt(jnp.mean(values * values, -1, keepdims=True) + eps)


def rms_backward(values, scale_rows, gain, d_normed):
    d_gain = jnp.sum(d_normed * values * scale_rows, 0)
    d_inner = d_normed * gain
    d_values = scale_rows * d_inner - values * scale_rows**3 * jnp.mean(
        d_inner * values, -1, keepdims=True
    )
    return (d_values, d_gain)


def dot(left, right, contract):
    return lax.dot_general(left, right, (contract, ((), ())), preferred_element_type=F32)


def contract_rows(left, right):
    return dot(left, right, ((0,), (0,)))


def contract_cols(left, right):
    return dot(left, right, ((1,), (1,)))


def stacked_heads(ref, which, heads):
    return jnp.concatenate(
        [ref[which, :, h * HEAD_DIM : (h + 1) * HEAD_DIM] for h in range(heads)], 0
    )


def causal(block_len, heads):
    keys = lax.broadcasted_iota(jnp.int32, (block_len, block_len), 0)
    queries = lax.broadcasted_iota(jnp.int32, (block_len, block_len), 1)
    return jnp.concatenate([keys <= queries] * heads, 1)


def attend_kernel(heads, table, ids, q_ref, kv_ref, o_ref, lse_ref):
    block_len = q_ref.shape[1]
    cols = heads * block_len
    scale = HEAD_DIM ** (-0.5)
    for which in range(2):
        last = ids[which]
        query = stacked_heads(q_ref, which, heads)

        def step(block, carry, masked=False):
            highest, total, acc = carry
            start = pl.multiple_of(table[block] * block_len, block_len)
            key = kv_ref[pl.ds(start, block_len), :HEAD_DIM]
            value = kv_ref[pl.ds(start, block_len), HEAD_DIM:]
            scores = contract_cols(key, query) * scale
            if masked:
                scores = jnp.where(causal(block_len, heads), scores, -1e30)
            new_high = jnp.maximum(highest, jnp.max(scores, 0, keepdims=True))
            probs = jnp.exp(scores - new_high)
            fade = jnp.exp(highest - new_high)
            total = total * fade + jnp.sum(probs, 0, keepdims=True)
            acc = acc * fade + contract_rows(value, probs.astype(BF16))
            return (new_high, total, acc)

        begin = (
            jnp.full((1, cols), -1e30, F32),
            jnp.zeros((1, cols), F32),
            jnp.zeros((HEAD_DIM, cols), F32),
        )
        carry = lax.fori_loop(0, last, step, begin)
        highest, total, acc = step(last, carry, True)
        lse_ref[which] = highest + jnp.log(total)
        out = (acc / total).T
        for h in range(heads):
            o_ref[which, :, h * HEAD_DIM : (h + 1) * HEAD_DIM] = out[
                h * block_len : (h + 1) * block_len
            ].astype(BF16)


def attend_back_kernel(
    heads, table, ids, q_ref, kv_ref, o_ref, do_ref, lse_ref, dq_ref, dkv_ref, sums
):
    block_len = q_ref.shape[1]
    cols = heads * block_len
    scale = HEAD_DIM ** (-0.5)
    sums[...] = jnp.zeros_like(sums)
    for which in range(2):
        last = ids[which]
        query = stacked_heads(q_ref, which, heads)
        d_out = stacked_heads(do_ref, which, heads)
        out = stacked_heads(o_ref, which, heads)
        delta = jnp.sum((d_out.astype(F32) * out.astype(F32)).T, 0, keepdims=True)
        lse = lse_ref[which]

        def step(block, d_query, masked=False):
            start = pl.multiple_of(table[block] * block_len, block_len)
            key = kv_ref[pl.ds(start, block_len), :HEAD_DIM]
            value = kv_ref[pl.ds(start, block_len), HEAD_DIM:]
            scores = contract_cols(key, query) * scale
            probs = jnp.exp(scores - lse)
            if masked:
                probs = jnp.where(causal(block_len, heads), probs, 0.0)
            d_probs = contract_cols(value, d_out)
            d_scores = (probs * (d_probs - delta)).astype(BF16)
            sums[pl.ds(start, block_len), :HEAD_DIM] += dot(d_scores, query, ((1,), (0,)))
            sums[pl.ds(start, block_len), HEAD_DIM:] += dot(
                probs.astype(BF16), d_out, ((1,), (0,))
            )
            return d_query + contract_rows(key, d_scores)

        d_query = lax.fori_loop(0, last, step, jnp.zeros((HEAD_DIM, cols), F32))
        d_query = step(last, d_query, True)
        d_query = (d_query * scale).T
        for h in range(heads):
            dq_ref[which, :, h * HEAD_DIM : (h + 1) * HEAD_DIM] = d_query[
                h * block_len : (h + 1) * block_len
            ]
    dkv_ref[:, :HEAD_DIM] = (sums[:, :HEAD_DIM] * scale).astype(BF16)
    dkv_ref[:, HEAD_DIM:] = sums[:, HEAD_DIM:].astype(BF16)


def in_vmem(count):
    return [pl.BlockSpec(memory_space=pltpu.VMEM)] * count


def in_smem(count):
    return [pl.BlockSpec(memory_space=pltpu.SMEM)] * count


def attend(table, ids, query, keys_values, heads):
    _, block_len, width = query.shape
    tall = keys_values.shape[0]
    return pl.pallas_call(
        functools.partial(attend_kernel, heads),
        out_shape=(
            jax.ShapeDtypeStruct(query.shape, BF16),
            jax.ShapeDtypeStruct((2, 1, heads * block_len), F32),
        ),
        in_specs=in_smem(2) + in_vmem(2),
        out_specs=tuple(in_vmem(2)),
        compiler_params=pltpu.CompilerParams(vmem_limit_bytes=VMEM_LIMIT),
        cost_estimate=pl.CostEstimate(
            flops=2 * tall * block_len * width * 2,
            bytes_accessed=tall * 512,
            transcendentals=tall * heads * block_len,
        ),
        name="attend",
    )(table, ids, query, keys_values)


def attend_back(table, ids, query, keys_values, out, d_out, lse, heads):
    _, block_len, width = query.shape
    tall = keys_values.shape[0]
    return pl.pallas_call(
        functools.partial(attend_back_kernel, heads),
        out_shape=(
            jax.ShapeDtypeStruct(query.shape, F32),
            jax.ShapeDtypeStruct(keys_values.shape, BF16),
        ),
        in_specs=in_smem(2) + in_vmem(5),
        out_specs=tuple(in_vmem(2)),
        scratch_shapes=[pltpu.VMEM(keys_values.shape, F32)],
        compiler_params=pltpu.CompilerParams(vmem_limit_bytes=VMEM_LIMIT),
        cost_estimate=pl.CostEstimate(
            flops=5 * tall * block_len * width * 2,
            bytes_accessed=tall * 1024,
            transcendentals=tall * heads * block_len,
        ),
        name="attend_back",
    )(table, ids, query, keys_values, out, d_out, lse)


MESH = pl.DeviceIdType.MESH


def greet(devices):
    barrier = pltpu.get_barrier_semaphore()
    for device in devices:
        pl.semaphore_signal(barrier, inc=1, device_id=device, device_id_type=MESH)
    pl.semaphore_wait(barrier, len(devices))


def remote(src, dst, send, recv, device):
    return pltpu.make_async_remote_copy(
        src_ref=src, dst_ref=dst, send_sem=send, recv_sem=recv, device_id=device, device_id_type=MESH
    )


def group_places(n):
    ctx = lax.axis_index("ctx")
    me = lax.axis_index("fsdp")
    partner = me + 1 - 2 * (me % 2)
    others = [(me + 2 * k) % n for k in range(1, n // 2)]
    senders = [(me + n - 2 * k) % n for k in range(1, n // 2)]
    return ctx, me, partner, others, senders


def sum_phases(mode, n, cuts, *refs):
    gathers = mode != "input"
    if mode == "attention":
        partial, tokens, gain, hidden_out, all_out = refs[:5]
    elif mode == "mlp":
        partial, hidden_in, cot, gain, d_out, all_out, d_gain = refs[:7]
    else:
        partial, tokens, d_hidden_in, gain, d_out, d_gain = refs[:6]
    near, summed, far, stage, near_s, near_r, far_s, far_r, own_s, own_r, out_s, out_r, fwd_s, fwd_r = refs[-14:]
    ctx, me, partner, others, senders = group_places(n)
    chips = n // 2
    rows = partial.shape[2]
    piece = rows // cuts
    chunks = [(w, i * piece) for w in range(2) for i in range(cuts)]

    def part(ref, w, lead, start):
        return ref.at[w, lead, pl.ds(start, piece)]

    first = []
    for c, (w, start) in enumerate(chunks):
        for j in range(chips):
            target = (partner + 2 * (j + 1)) % n
            copy = remote(
                part(partial, w, target, start),
                part(near, w, j, start),
                near_s.at[c, j],
                near_r.at[c, j],
                (ctx, partner),
            )
            copy.start()
            first.append(copy)
    yield

    second = []

    def post(c):
        w, start = chunks[c]
        for j in range(chips - 1):
            copy = remote(
                part(summed, w, j, start),
                part(far, w, j, start),
                far_s.at[c, j],
                far_r.at[c, j],
                (ctx, others[j]),
            )
            copy.start()
            second.append(copy)

    for c, (w, start) in enumerate(chunks):
        span = pl.ds(start, piece)
        for j in range(chips - 1):
            first[c * chips + j].wait()
            target = (me + 2 * (j + 1)) % n
            summed[w, j, span] = (
                partial[w, target, span].astype(F32) + near[w, j, span].astype(F32)
            ).astype(BF16)
        if c:
            post(c - 1)
    post(len(chunks) - 1)
    yield

    if mode != "attention":
        d_gain[...] = jnp.zeros_like(d_gain)
    third = []

    def spread(c):
        w, start = chunks[c]
        src = stage.at[w, pl.ds(start, piece)]
        for k in range(chips - 1):
            copy = remote(src, part(all_out, w, me, start), out_s.at[c, k], out_r.at[c, k], (ctx, others[k]))
            copy.start()
            third.append(copy)
        copy = remote(src, part(all_out, w, me, start), own_s.at[c], own_r.at[c], (ctx, partner))
        copy.start()
        return copy

    near_copies = []
    for c, (w, start) in enumerate(chunks):
        span = pl.ds(start, piece)
        first[c * chips + chips - 1].wait()
        total = partial[w, me, span].astype(F32) + near[w, chips - 1, span].astype(F32)
        for j in range(chips - 1):
            second[c * (chips - 1) + j].wait()
            total += far[w, j, span].astype(F32)
        if mode == "attention":
            hidden = tokens[w, span].astype(F32) + total
            hidden_out[w, span] = hidden
            rounded = (hidden * rms_scale(hidden) * gain[...]).astype(BF16)
        elif mode == "mlp":
            hidden = hidden_in[w, span]
            d_norm, gain_part = rms_backward(hidden, rms_scale(hidden), gain[...], total)
            d_gain[...] += gain_part[None]
            d_hidden = cot[w, span].astype(F32) + d_norm
            d_out[w, span] = d_hidden
            rounded = d_hidden.astype(BF16)
        else:
            values = tokens[w, span].astype(F32)
            d_norm, gain_part = rms_backward(values, rms_scale(values), gain[...], total)
            d_gain[...] += gain_part[None]
            d_out[w, span] = d_hidden_in[w, span] + d_norm
        if gathers:
            stage[w, span] = rounded
            all_out[w, me, span] = rounded
            if c:
                near_copies.append(spread(c - 1))
    if not gathers:
        return
    near_copies.append(spread(len(chunks) - 1))
    yield

    forwards = []
    for c, (w, start) in enumerate(chunks):
        for k in range(chips - 1):
            third[c * (chips - 1) + k].wait_recv()
            block = part(all_out, w, senders[k], start)
            copy = remote(block, block, fwd_s.at[c, k], fwd_r.at[c, k], (ctx, partner))
            copy.start()
            forwards.append(copy)
    yield
    for copy in third:
        copy.wait_send()
    for copy in near_copies + forwards:
        copy.wait()


def sum_kernel(mode, n, cuts, *refs):
    ctx, _, partner, others, _ = group_places(n)
    greet([(ctx, partner)] + [(ctx, o) for o in others])
    for _ in sum_phases(mode, n, cuts, *refs):
        pass


def sum_shapes(mode, partial):
    _, n, rows, width = partial.shape
    chips = n // 2
    row_shape = (2, rows, width)
    full = jax.ShapeDtypeStruct(row_shape, F32)
    gathered = jax.ShapeDtypeStruct(partial.shape, BF16)
    gain_sum = jax.ShapeDtypeStruct((1, width), F32)
    out_shape = {
        "attention": (full, gathered),
        "mlp": (full, gathered, gain_sum),
        "input": (full, gain_sum),
    }[mode]
    dma = pltpu.SemaphoreType.DMA
    chunks = 2 * SUM_CUTS
    scratch = [
        pltpu.VMEM((2, chips, rows, width), BF16),
        pltpu.VMEM((2, chips - 1, rows, width), BF16),
        pltpu.VMEM((2, chips - 1, rows, width), BF16),
        pltpu.VMEM(row_shape, BF16),
        dma((chunks, chips)),
        dma((chunks, chips)),
        dma((chunks, chips - 1)),
        dma((chunks, chips - 1)),
        dma((chunks,)),
        dma((chunks,)),
        dma((chunks, chips - 1)),
        dma((chunks, chips - 1)),
        dma((chunks, chips - 1)),
        dma((chunks, chips - 1)),
    ]
    return out_shape, scratch


SUM_CUTS = 2


def group_sum(mode, partial, *operands, collective):
    _, n, rows, width = partial.shape
    out_shape, scratch = sum_shapes(mode, partial)
    return pl.pallas_call(
        functools.partial(sum_kernel, mode, n, SUM_CUTS),
        out_shape=out_shape,
        in_specs=in_vmem(1 + len(operands)),
        out_specs=tuple(in_vmem(len(out_shape))),
        scratch_shapes=scratch,
        compiler_params=pltpu.CompilerParams(
            vmem_limit_bytes=VMEM_LIMIT, collective_id=collective, has_side_effects=True
        ),
        cost_estimate=pl.CostEstimate(
            flops=20 * rows * width, bytes_accessed=60_000_000, transcendentals=0
        ),
        name="group_sum_" + mode,
    )(partial, *operands)


def ring_index(place, n):
    late = place // (n // 2)
    return (1 - late) * 2 * place + late * (2 * n - 1 - 2 * place)


def ring_place(index, n):
    odd = index % 2
    return (1 - odd) * (index // 2) + odd * (n - 1 - index // 2)


def share_kernel(n, own, out, right_s, right_r, left_s, left_r, near_s, near_r):
    ctx = lax.axis_index("ctx")
    me = lax.axis_index("fsdp")
    which = me % 2
    partner = me + 1 - 2 * which
    place = ring_place(ctx, n)
    right = (ring_index((place + 1) % n, n), me)
    left = (ring_index((place + n - 1) % n, n), me)
    greet([right, left, (ctx, partner)])

    def block(offset):
        return out.at[ring_index((place + n + offset) % n, n), which]

    def to_right(step):
        src = own.at[which] if step == 0 else block(-step)
        return remote(src, block(-step), right_s.at[step], right_r.at[step], right)

    def to_left(step):
        src = own.at[which] if step == 0 else block(step)
        return remote(src, block(step), left_s.at[step], left_r.at[step], left)

    rights, lefts = n // 2, n - 1 - n // 2
    sent = [to_right(0), to_left(0)]
    for copy in sent:
        copy.start()
    out[ctx] = own[...]
    going = [sent[0], sent[1]]
    for step in range(1, rights + 1):
        going[0].wait_recv()
        if step < rights:
            going[0] = to_right(step)
            going[0].start()
            sent.append(going[0])
        hand = remote(block(-step), block(-step), near_s.at[step - 1], near_r.at[step - 1], (ctx, partner))
        hand.start()
        sent.append(hand)
        if step <= lefts:
            going[1].wait_recv()
            if step < lefts:
                going[1] = to_left(step)
                going[1].start()
                sent.append(going[1])
            slot = rights + step - 1
            hand = remote(block(step), block(step), near_s.at[slot], near_r.at[slot], (ctx, partner))
            hand.start()
            sent.append(hand)
    for copy in sent:
        copy.wait_send()
    for step in range(1, rights + 1):
        remote(block(-step), block(-step), near_s.at[step - 1], near_r.at[step - 1], (ctx, partner)).wait_recv()
    for step in range(1, lefts + 1):
        slot = rights + step - 1
        remote(block(step), block(step), near_s.at[slot], near_r.at[slot], (ctx, partner)).wait_recv()


def share_keys(own, n, collective):
    dma = pltpu.SemaphoreType.DMA
    return pl.pallas_call(
        functools.partial(share_kernel, n),
        out_shape=jax.ShapeDtypeStruct((n,) + own.shape, BF16),
        in_specs=in_vmem(1),
        out_specs=in_vmem(1)[0],
        scratch_shapes=[dma((n // 2,))] * 4 + [dma((n - 1,))] * 2,
        compiler_params=pltpu.CompilerParams(
            vmem_limit_bytes=VMEM_LIMIT, collective_id=collective, has_side_effects=True
        ),
        cost_estimate=pl.CostEstimate(flops=0, bytes_accessed=60_000_000, transcendentals=0),
        name="share_keys",
    )(own)


def return_kernel(n, partial, out, near, summed, far, near_s, near_r, far_s, far_r):
    ctx = lax.axis_index("ctx")
    me = lax.axis_index("fsdp")
    which = me % 2
    partner = me + 1 - 2 * which
    others = [(ctx + k) % n for k in range(1, n)]
    greet([(ctx, partner)] + [(o, me) for o in others])
    order = others + [ctx]
    first = []
    for k, target in enumerate(order):
        copy = remote(partial.at[target, 1 - which], near.at[k], near_s.at[k], near_r.at[k], (ctx, partner))
        copy.start()
        first.append(copy)
    second = []

    def post(k):
        copy = remote(summed.at[k], far.at[k], far_s.at[k], far_r.at[k], (others[k], me))
        copy.start()
        second.append(copy)

    for k in range(n - 1):
        first[k].wait()
        summed[k] = (partial[others[k], which].astype(F32) + near[k].astype(F32)).astype(BF16)
        if k:
            post(k - 1)
    post(n - 2)
    out[1 - which] = jnp.zeros(out.shape[1:], F32)
    first[n - 1].wait()
    out[which] = partial[ctx, which].astype(F32) + near[n - 1].astype(F32)
    for k in range(n - 1):
        second[k].wait()
        out[which] += far[k].astype(F32)


def return_grads(partial, collective):
    n = partial.shape[0]
    block = partial.shape[2:]
    dma = pltpu.SemaphoreType.DMA
    return pl.pallas_call(
        functools.partial(return_kernel, n),
        out_shape=jax.ShapeDtypeStruct(partial.shape[1:], F32),
        in_specs=in_vmem(1),
        out_specs=in_vmem(1)[0],
        scratch_shapes=[
            pltpu.VMEM((n,) + block, BF16),
            pltpu.VMEM((n - 1,) + block, BF16),
            pltpu.VMEM((n - 1,) + block, BF16),
            dma((n,)),
            dma((n,)),
            dma((n - 1,)),
            dma((n - 1,)),
        ],
        compiler_params=pltpu.CompilerParams(
            vmem_limit_bytes=VMEM_LIMIT, collective_id=collective, has_side_effects=True
        ),
        cost_estimate=pl.CostEstimate(flops=0, bytes_accessed=80_000_000, transcendentals=0),
        name="return_grads",
    )(partial)


def ring_sum_kernel(n, members, plan, swaps, sizes, mode, extra_ins, extra_outs, *refs):
    arrays = len(sizes)
    ins = []
    for size in sizes:
        ins.append(refs[:size])
        refs = refs[size:]
    side_ins, refs = refs[:extra_ins], refs[extra_ins:]
    outs, refs = refs[:arrays], refs[arrays:]
    side_outs, refs = refs[:extra_outs], refs[extra_outs:]
    count = len(plan)
    arrived, stages, sends, recvs = (refs[i * count : (i + 1) * count] for i in range(4))
    refs = refs[4 * count :]
    done, swap_s, swap_r = (refs[i * len(swaps) : (i + 1) * len(swaps)] for i in range(3))
    refs = refs[3 * len(swaps) :]
    ctx = lax.axis_index("ctx")
    me = lax.axis_index("fsdp")
    place = ring_place(ctx, n)
    around = {step: (ring_index((place + n + step) % n, n), me) for step in (1, -1)}
    greet([around[1], around[-1]] + [(ctx, (me + k) % members) for k in range(1, members)])
    beside = iter(())
    if mode:
        beside = sum_phases(mode, members, SUM_CUTS, *side_ins, *side_outs, *refs)

    def copy(i, hop, src):
        step = plan[i][3]
        return remote(src, arrived[i].at[hop], sends[i].at[hop], recvs[i].at[hop], around[step])

    def chunk(i, hop):
        step = plan[i][3]
        return ring_index((place + n * n - step * (hop + 1)) % n, n)

    def term(i, hop):
        which, low, high, _ = plan[i]
        if len(ins[which]) == 1:
            return ins[which][0][chunk(i, hop), :, low:high].astype(F32)
        left, right = ins[which]
        return jnp.dot(left[chunk(i, hop)], right[:, low:high], preferred_element_type=F32)

    for i in range(count):
        stages[i][0] = term(i, 0).astype(BF16)
        if i:
            copy(i - 1, 0, stages[i - 1].at[0]).start()
    copy(count - 1, 0, stages[count - 1].at[0]).start()
    next(beside, None)

    def add(i, hop):
        mine = term(i, hop)
        copy(i, hop - 1, stages[i].at[0]).wait_recv()
        return (arrived[i][hop - 1].astype(F32) + mine).astype(BF16)

    def one_hop(hop, carry):
        slot = hop % 2
        for i in range(count):
            @pl.when(hop > 1)
            def _():
                copy(i, hop - 2, stages[i].at[slot]).wait_send()

            stages[i][slot] = add(i, hop)
            if i:
                copy(i - 1, hop, stages[i - 1].at[slot]).start()
        copy(count - 1, hop, stages[count - 1].at[slot]).start()
        return carry

    hop = 1
    if mode:
        for _ in range(min(4, n - 3)):
            one_hop(jnp.int32(hop), 0)
            hop += 1
            next(beside, None)
    lax.fori_loop(hop, n - 1, one_hop, 0)
    for i, (which, low, high, _) in enumerate(plan):
        target = done[swaps.index(which)] if which in swaps else outs[which]
        value = add(i, n - 1)
        rows = target.shape[1]
        for group in range(target.shape[0]):
            target[group, :, low:high] = value[group * rows : (group + 1) * rows]
    swapped = []
    for j, which in enumerate(swaps):
        for k in range(1, members):
            other = (me + k) % members
            swapped.append(
                remote(
                    done[j].at[other],
                    outs[which].at[me],
                    swap_s[j].at[k - 1],
                    swap_r[j].at[k - 1],
                    (ctx, other),
                )
            )
            swapped[-1].start()
        outs[which][me] = done[j][me]
    for _ in beside:
        pass
    for i in range(count):
        for hop in (n - 3, n - 2):
            copy(i, hop, stages[i].at[hop % 2]).wait_send()
    for move in swapped:
        move.wait()


def ring_sum(arrays, groups, plan, swaps, members, collective, mode=None, operands=()):
    n = arrays[0][0].shape[0]
    dma = pltpu.SemaphoreType.DMA
    talls = [array[0].shape[1] for array in arrays]
    blocks = [(talls[which], high - low) for which, low, high, _ in plan]
    sums = [
        (g, tall // g, array[-1].shape[-1]) for array, g, tall in zip(arrays, groups, talls)
    ]
    flat = [operand for array in arrays for operand in array]
    extra_shape, extra_scratch = sum_shapes(mode, operands[0]) if mode else ((), [])
    out_shape = tuple(jax.ShapeDtypeStruct(shape, BF16) for shape in sums) + tuple(extra_shape)
    return pl.pallas_call(
        functools.partial(
            ring_sum_kernel,
            n,
            members,
            plan,
            swaps,
            tuple(len(array) for array in arrays),
            mode,
            len(operands),
            len(extra_shape),
        ),
        out_shape=out_shape,
        in_specs=in_vmem(len(flat) + len(operands)),
        out_specs=tuple(in_vmem(len(out_shape))),
        scratch_shapes=[pltpu.VMEM((n - 1,) + b, BF16) for b in blocks]
        + [pltpu.VMEM((2,) + b, BF16) for b in blocks]
        + [dma((n - 1,)) for _ in blocks] * 2
        + [pltpu.VMEM(sums[which], BF16) for which in swaps]
        + [dma((members - 1,)) for _ in swaps] * 2
        + extra_scratch,
        compiler_params=pltpu.CompilerParams(
            vmem_limit_bytes=VMEM_LIMIT, collective_id=collective, has_side_effects=True
        ),
        cost_estimate=pl.CostEstimate(flops=0, bytes_accessed=200_000_000, transcendentals=0),
        name="ring_sum",
    )(*flat, *operands)


def ring_gather_kernel(n, count, *refs):
    owns, outs, sends, recvs = (refs[i * count : (i + 1) * count] for i in range(4))
    ctx = lax.axis_index("ctx")
    me = lax.axis_index("fsdp")
    place = ring_place(ctx, n)
    around = {step: (ring_index((place + n + step) % n, n), me) for step in (1, -1)}
    greet([around[1], around[-1]])
    far = n // 2

    def copy(i, step, half, hop):
        middle = owns[i].shape[-1] // 2
        lanes = pl.ds(half * middle, middle)
        block = outs[i].at[ring_index((place + n - step * hop) % n, n), :, lanes]
        src = block if hop else owns[i].at[:, lanes]
        row = half if step == 1 else 2 + half
        return remote(src, block, sends[i].at[row, hop], recvs[i].at[row, hop], around[step])

    def hops(step, half):
        return far if (step == 1) == (half == 0) else far - 1

    lines = [(i, step, half) for step, half in ((1, 0), (-1, 1), (1, 1), (-1, 0)) for i in range(count)]
    for i, step, half in lines:
        copy(i, step, half, 0).start()
    for own, out in zip(owns, outs):
        out[ctx] = own[...]
    for hop in range(1, far + 1):
        for i, step, half in lines:
            if hop <= hops(step, half):
                copy(i, step, half, hop - 1).wait_recv()
                if hop < hops(step, half):
                    copy(i, step, half, hop).start()
    for i, step, half in lines:
        for hop in range(hops(step, half)):
            copy(i, step, half, hop).wait_send()


def ring_gather(owns, n, collective):
    count = len(owns)
    return pl.pallas_call(
        functools.partial(ring_gather_kernel, n, count),
        out_shape=tuple(jax.ShapeDtypeStruct((n,) + own.shape, BF16) for own in owns),
        in_specs=in_vmem(count),
        out_specs=tuple(in_vmem(count)),
        scratch_shapes=[pltpu.SemaphoreType.DMA((4, n // 2))] * (2 * count),
        compiler_params=pltpu.CompilerParams(
            vmem_limit_bytes=VMEM_LIMIT, collective_id=collective, has_side_effects=True
        ),
        cost_estimate=pl.CostEstimate(flops=0, bytes_accessed=120_000_000, transcendentals=0),
        name="ring_gather",
    )(*owns)


def weave_kernel(planes, out):
    for e in range(2):
        out[:, e, :] = planes[e].astype(F32)


def weave(planes):
    _, rows, lanes = planes.shape
    block = 32 if rows % 32 == 0 else rows
    return pl.pallas_call(
        weave_kernel,
        grid=(rows // block,),
        out_shape=jax.ShapeDtypeStruct((rows, 2, lanes), F32),
        in_specs=[pl.BlockSpec((2, block, lanes), lambda i: (0, i, 0))],
        out_specs=pl.BlockSpec((block, 2, lanes), lambda i: (i, 0, 0)),
        cost_estimate=pl.CostEstimate(
            flops=0, bytes_accessed=12 * rows * lanes, transcendentals=0
        ),
        name="weave",
    )(planes)


def project_kernel(heads, x_ref, gain, w_ref, bias, cos_ref, sin_ref, normed_ref, q_ref, kv_ref):
    values = x_ref[...].astype(F32)
    normed = (values * rms_scale(values) * gain[...]).astype(BF16)
    normed_ref[...] = normed
    qkv = jnp.dot(normed, w_ref[...], preferred_element_type=F32) + bias[...]
    cosines, sines = cos_ref[...], sin_ref[...]
    for h in range(heads + 1):
        vector = qkv[:, h * HEAD_DIM : (h + 1) * HEAD_DIM]
        turned = vector * cosines + pltpu.roll(vector, HEAD_DIM // 2, 1) * sines
        if h < heads:
            q_ref[:, h * HEAD_DIM : (h + 1) * HEAD_DIM] = turned.astype(BF16)
        else:
            kv_ref[:, :HEAD_DIM] = turned.astype(BF16)
    kv_ref[:, HEAD_DIM:] = qkv[:, (heads + 1) * HEAD_DIM :].astype(BF16)


def project(x_all, gain, weights, bias, cosines, sines, heads):
    rows = x_all.shape[0]
    block = 128
    width = weights.shape[1]

    def tall(lanes):
        return pl.BlockSpec((block, lanes), lambda i: (i, 0))

    def fixed(shape):
        return pl.BlockSpec(shape, lambda i: (0, 0))

    lanes = (D, heads * HEAD_DIM, 2 * HEAD_DIM)
    return pl.pallas_call(
        functools.partial(project_kernel, heads),
        grid=(rows // block,),
        out_shape=tuple(jax.ShapeDtypeStruct((rows, n), BF16) for n in lanes),
        in_specs=[
            tall(D),
            fixed((1, D)),
            fixed((D, width)),
            fixed((1, width)),
            tall(HEAD_DIM),
            tall(HEAD_DIM),
        ],
        out_specs=tuple(tall(n) for n in lanes),
        compiler_params=pltpu.CompilerParams(vmem_limit_bytes=VMEM_LIMIT),
        cost_estimate=pl.CostEstimate(
            flops=2 * rows * D * width, bytes_accessed=4 * rows * D + 2 * D * width, transcendentals=0
        ),
        name="project",
    )(x_all, gain, weights, bias, cosines, sines)


def exchange(pieces, axis):
    return lax.all_to_all(pieces, axis, split_axis=0, concat_axis=0, tiled=True)


def together(*values):
    return lax.optimization_barrier(values)


def body(tokens, pairing, gain_attn, w_qkv, b_qkv, w_out, gain_mlp, w_gate_up, w_down, cotangent):
    half_rows = tokens.shape[2]
    n_ctx = lax.axis_size("ctx")
    n_fsdp = lax.axis_size("fsdp")
    ctx_index = lax.axis_index("ctx")
    fsdp_index = lax.axis_index("fsdp")
    stretch_len = half_rows * n_fsdp
    rows = 2 * stretch_len
    local_count = 2 * half_rows
    q_width = HEADS * HEAD_DIM
    kv_width = KV_HEADS * HEAD_DIM
    heads = HEADS // n_fsdp
    q_cols = heads * HEAD_DIM
    d_shard = w_qkv.shape[0]
    ff_shard = w_down.shape[0]

    owner_range = jnp.arange(n_ctx, dtype=jnp.int32)
    own_first = jnp.sum(jnp.where(owner_range == ctx_index, pairing, 0))
    ids = jnp.stack([own_first, 2 * n_ctx - 1 - own_first])
    inverse_pair = jnp.sum(
        owner_range[:, None] * (pairing[:, None] == owner_range[None, :]).astype(jnp.int32), 0
    )
    table = jnp.concatenate([2 * inverse_pair, 2 * inverse_pair[::-1] + 1])
    position = (
        ids[:, None] * stretch_len + jnp.arange(stretch_len, dtype=jnp.int32)[None, :]
    ).reshape(rows)
    kv_of = [f * KV_HEADS // n_fsdp for f in range(n_fsdp)]
    my_kv = fsdp_index * KV_HEADS // n_fsdp

    small = lax.all_gather(jnp.concatenate([gain_attn, gain_mlp, b_qkv]), "fsdp", axis=0)
    small, w_qkv, w_gate_up = together(small, w_qkv, w_gate_up)
    gain_one = small[:, :d_shard].reshape(D).astype(F32)
    gain_two = small[:, d_shard : 2 * d_shard].reshape(D).astype(F32)
    bias = small[:, 2 * d_shard :].reshape(-1).astype(F32)
    x_all = lax.all_gather(tokens[0], "fsdp", axis=1, tiled=True).reshape(rows, D)
    qkv_pieces = jnp.stack(
        [
            jnp.concatenate(
                [
                    w_qkv[:, f * q_cols : (f + 1) * q_cols],
                    w_qkv[:, q_width + kv_of[f] * HEAD_DIM : q_width + (kv_of[f] + 1) * HEAD_DIM],
                    w_qkv[
                        :,
                        q_width + kv_width + kv_of[f] * HEAD_DIM : q_width
                        + kv_width
                        + (kv_of[f] + 1) * HEAD_DIM,
                    ],
                ],
                1,
            )
            for f in range(n_fsdp)
        ]
    )
    w_qkv_cols = exchange(qkv_pieces, "fsdp").reshape(D, -1)
    bias_cols = jnp.concatenate(
        [
            lax.dynamic_slice_in_dim(bias, fsdp_index * q_cols, q_cols),
            lax.dynamic_slice_in_dim(bias, q_width + my_kv * HEAD_DIM, HEAD_DIM),
            lax.dynamic_slice_in_dim(bias, q_width + kv_width + my_kv * HEAD_DIM, HEAD_DIM),
        ]
    )
    gate_up_pieces = w_gate_up.reshape(d_shard, 2, n_fsdp, ff_shard).transpose(2, 1, 3, 0)
    gate_up_pieces = with_layout_constraint(gate_up_pieces, Layout((0, 1, 2, 3)))
    x_all, w_qkv_cols, gate_up_pieces = together(x_all, w_qkv_cols, gate_up_pieces)
    gate_up_cols = exchange(gate_up_pieces, "fsdp")

    cosines, sines = rope_tables(position)
    normed1, query, own_kv = project(
        x_all,
        gain_one[None],
        w_qkv_cols,
        bias_cols[None],
        jnp.concatenate([cosines[:, 0], cosines[:, 0]], 1),
        jnp.concatenate([-sines[:, 0], sines[:, 0]], 1),
        heads,
    )
    query = query.reshape(2, stretch_len, q_cols)
    keys_values = share_keys(own_kv.reshape(2, stretch_len, 2 * HEAD_DIM), n_ctx, 4)
    keys_values = keys_values.reshape(n_ctx * rows, 2 * HEAD_DIM)
    attended, lse = attend(table, ids, query, keys_values, heads)
    attended16 = attended.reshape(rows, q_cols)

    def scatter(partial):
        return lax.psum_scatter(
            partial.astype(BF16).reshape(2, stretch_len, D), "fsdp", scatter_dimension=1, tiled=True
        ).astype(F32).reshape(local_count, D)

    def by_member(partial):
        return partial.astype(BF16).reshape(2, n_fsdp, half_rows, D)

    tokens_own = tokens[0]
    hidden, normed2 = group_sum(
        "attention",
        by_member(jnp.dot(attended16, w_out, preferred_element_type=F32)),
        tokens_own,
        gain_two[None],
        collective=1,
    )
    normed2, cot_own = together(normed2, cotangent[0])
    normed2 = normed2.reshape(rows, D)
    cot_all = lax.all_gather(cot_own, "fsdp", axis=1, tiled=True).reshape(rows, D)
    w_gate_cols, w_up_cols = (gate_up_cols[:, e] for e in range(2))
    normed2_parts = normed2.reshape(rows, n_fsdp, d_shard)
    gate_val, up_val = (
        jnp.einsum("tsk,sfk->tf", normed2_parts, w, preferred_element_type=F32)
        for w in (w_gate_cols, w_up_cols)
    )
    sigmoid_gate = jax.nn.sigmoid(gate_val)
    act16 = (jax.nn.silu(gate_val) * up_val).astype(BF16)
    result = hidden.reshape(local_count, D) + scatter(jnp.dot(act16, w_down, preferred_element_type=F32))
    block_output = result.astype(BF16).reshape(tokens.shape)

    d_act = contract_cols(cot_all, w_down)
    d_gate16 = (d_act * up_val * sigmoid_gate * (1.0 + gate_val * (1.0 - sigmoid_gate))).astype(BF16)
    d_up16 = (d_act * gate_val * sigmoid_gate).astype(BF16)
    d_normed2 = sum(
        jnp.einsum("tf,sfk->tsk", d, w, preferred_element_type=F32)
        for d, w in ((d_gate16, w_gate_cols), (d_up16, w_up_cols))
    )
    def by_columns(pieces):
        queries = [pieces[f][..., :q_cols] for f in range(n_fsdp)]
        rest = []
        for part in range(2):
            lo = q_cols + part * HEAD_DIM
            for g in range(KV_HEADS):
                rest.append(
                    sum(
                        pieces[f][..., lo : lo + HEAD_DIM].astype(F32)
                        for f in range(n_fsdp)
                        if kv_of[f] == g
                    ).astype(pieces[0].dtype)
                )
        return jnp.concatenate(queries + rest, -1)

    chunk_rows = d_shard // n_ctx
    down_rows = -(-ff_shard // (16 * n_ctx)) * 16
    side = D // 2

    def by_chunk(values):
        split = values.T.reshape(n_fsdp, n_ctx, chunk_rows, rows)
        return split.transpose(1, 0, 2, 3).reshape(n_ctx, n_fsdp * chunk_rows, rows)

    act_chunks = jnp.pad(act16.T, ((0, n_ctx * down_rows - ff_shard), (0, 0)))
    act_chunks = act_chunks.reshape(n_ctx, down_rows, rows)
    normed2_chunks = by_chunk(normed2)
    gate_sum, up_sum, down_sum, d_hidden, dh_all, d_gain_two = ring_sum(
        ((normed2_chunks, d_gate16), (normed2_chunks, d_up16), (act_chunks, cot_all)),
        (n_fsdp, n_fsdp, 1),
        ((0, 0, ff_shard, 1), (1, 0, ff_shard, -1), (2, 0, side, 1), (2, side, D, -1)),
        (0, 1),
        n_fsdp,
        7,
        "mlp",
        (by_member(d_normed2), hidden, cotangent[0], gain_two[None]),
    )
    planes = jnp.stack(
        [
            total.transpose(1, 0, 2).reshape(chunk_rows, n_fsdp * ff_shard)
            for total in (gate_sum, up_sum)
        ]
    )
    d_w_gate_up = weave(lax.all_gather(planes, "ctx", axis=1, tiled=True))
    dh_all = dh_all.reshape(rows, D)
    d_attended16 = contract_cols(dh_all, w_out).astype(BF16).reshape(2, stretch_len, q_cols)
    d_query, d_kv = attend_back(
        table, ids, query, keys_values, attended, d_attended16, lse, heads
    )
    d_kv_own = return_grads(d_kv.reshape(n_ctx, 2, stretch_len, 2 * HEAD_DIM), 5).reshape(rows, -1)

    d_rotated = jnp.concatenate([d_query.reshape(rows, q_cols), d_kv_own[:, :HEAD_DIM]], 1)
    d_rotated = unrotate(
        d_rotated.reshape(rows, heads + 1, HEAD_DIM), cosines, sines
    ).reshape(rows, q_cols + HEAD_DIM)
    d_qkv = jnp.concatenate([d_rotated, d_kv_own[:, HEAD_DIM:]], 1)
    d_bias = jnp.sum(d_qkv, 0)
    d_qkv16 = d_qkv.astype(BF16)
    d_normed1 = contract_cols(d_qkv16, w_qkv_cols)
    x32 = x_all.astype(F32)
    d_gain_one = jnp.sum(d_normed1 * x32 * rms_scale(x32), 0)
    zeros = jnp.zeros_like(d_bias)
    d_bias_full = by_columns([jnp.where(fsdp_index == f, d_bias, zeros) for f in range(n_fsdp)])
    parts = jnp.concatenate(
        [v.reshape(n_fsdp, -1) for v in (d_gain_one, d_gain_two, d_bias_full)], 1
    ).astype(BF16)
    length = parts.shape[1]
    few = 2 * HEAD_DIM
    vector_rows = -(-length // (n_ctx * few))
    parts = jnp.pad(parts, ((0, 0), (0, n_ctx * vector_rows * few - length)))
    parts = parts.reshape(n_fsdp, n_ctx, vector_rows, few)
    parts = jnp.pad(parts, ((0, 0), (0, 0), (0, -vector_rows % 16), (0, 0)))
    parts = parts.transpose(1, 0, 2, 3).reshape(n_ctx, -1, few)
    attended_chunks = attended16.T.reshape(n_ctx, chunk_rows, rows)
    pieces, out_sum, vector, d_tokens, _ = ring_sum(
        ((by_chunk(normed1), d_qkv16), (attended_chunks, dh_all), (parts,)),
        (n_fsdp, 1, n_fsdp),
        (
            (0, 0, q_cols, 1),
            (0, q_cols, d_qkv16.shape[-1], -1),
            (1, 0, side, 1),
            (1, side, D, -1),
            (2, 0, few, 1),
        ),
        (0, 2),
        n_fsdp,
        8,
        "input",
        (by_member(d_normed1), tokens_own, d_hidden, gain_one[None]),
    )
    d_tokens = d_tokens.reshape(tokens.shape)
    qkv_sum = by_columns([pieces[f] for f in range(n_fsdp)])
    vector = jnp.sum(vector.astype(F32), 0)[:vector_rows].astype(BF16)
    vector = jnp.pad(vector, ((0, chunk_rows - vector_rows), (0, 0)))
    attention_sum, d_w_down = ring_gather(
        (jnp.concatenate([qkv_sum, out_sum[0], vector], -1), down_sum[0]), n_ctx, 9
    )
    d_w_down = d_w_down.reshape(n_ctx * down_rows, D)[:ff_shard].astype(F32)
    vector = attention_sum[:, :vector_rows, -few:].astype(F32).reshape(-1)
    attention_sum = attention_sum.reshape(d_shard, -1)
    qkv_width = qkv_sum.shape[-1]
    d_w_qkv = attention_sum[:, :qkv_width].astype(F32)
    d_w_out = attention_sum[:, qkv_width : qkv_width + D].astype(F32)
    d_gain_attn = vector[:d_shard]
    d_gain_mlp = vector[d_shard : 2 * d_shard]
    d_b_qkv = vector[2 * d_shard : 2 * d_shard + b_qkv.shape[0]]

    return (
        block_output,
        d_tokens,
        d_gain_attn,
        d_w_qkv,
        d_b_qkv,
        d_w_out,
        d_gain_mlp,
        d_w_gate_up,
        d_w_down,
    )


def solution(mesh):
    placed = (
        P("ctx", None, "fsdp", None),
        P(),
        P("fsdp"),
        P("fsdp", None),
        P("fsdp"),
        P("fsdp", None),
        P("fsdp"),
        P("fsdp", None, None),
        P("fsdp", None),
        P("ctx", None, "fsdp", None),
    )
    return jax.shard_map(
        body,
        mesh=mesh,
        in_specs=placed,
        out_specs=(
            P("ctx", None, "fsdp", None),
            P("ctx", None, "fsdp", None),
            P("fsdp"),
            P("fsdp", None),
            P("fsdp"),
            P("fsdp", None),
            P("fsdp"),
            P("fsdp", None, None),
            P("fsdp", None),
        ),
        check_vma=False,
    )
```

```python
import functools

import jax
import jax.numpy as jnp
from jax import lax
from jax.experimental import pallas as pl
from jax.experimental.layout import Layout, with_layout_constraint
from jax.experimental.pallas import tpu as pltpu
from jax.sharding import PartitionSpec as P

D = 1536
HEADS = 12
KV_HEADS = 2
HEAD_DIM = 128

eps = 1e-06
rope_base = 1000000.0
F32 = jnp.float32
BF16 = jnp.bfloat16
VMEM_LIMIT = 60 * 1024 * 1024


def rope_tables(position):
    half = HEAD_DIM // 2
    inverse = rope_base ** (-(jnp.arange(half, dtype=F32) * 2.0 / HEAD_DIM))
    angle = position.astype(F32)[:, None] * inverse[None, :]
    return (jnp.cos(angle)[:, None, :], jnp.sin(angle)[:, None, :])


def rotate(vectors, cosines, sines):
    half = HEAD_DIM // 2
    first, second = (vectors[..., :half], vectors[..., half:])
    return jnp.concatenate([first * cosines - second * sines, second * cosines + first * sines], -1)


def unrotate(grads, cosines, sines):
    half = HEAD_DIM // 2
    first, second = (grads[..., :half], grads[..., half:])
    return jnp.concatenate([first * cosines + second * sines, second * cosines - first * sines], -1)


def rms_scale(values):
    return lax.rsqrt(jnp.mean(values * values, -1, keepdims=True) + eps)


def rms_backward(values, scale_rows, gain, d_normed):
    d_gain = jnp.sum(d_normed * values * scale_rows, 0)
    d_inner = d_normed * gain
    d_values = scale_rows * d_inner - values * scale_rows**3 * jnp.mean(
        d_inner * values, -1, keepdims=True
    )
    return (d_values, d_gain)


def dot(left, right, contract):
    return lax.dot_general(left, right, (contract, ((), ())), preferred_element_type=F32)


def contract_rows(left, right):
    return dot(left, right, ((0,), (0,)))


def contract_cols(left, right):
    return dot(left, right, ((1,), (1,)))


def stacked_heads(ref, which, heads):
    return jnp.concatenate(
        [ref[which, :, h * HEAD_DIM : (h + 1) * HEAD_DIM] for h in range(heads)], 0
    )


def causal(block_len, heads):
    keys = lax.broadcasted_iota(jnp.int32, (block_len, block_len), 0)
    queries = lax.broadcasted_iota(jnp.int32, (block_len, block_len), 1)
    return jnp.concatenate([keys <= queries] * heads, 1)


def attend_kernel(heads, table, ids, q_ref, kv_ref, o_ref, lse_ref):
    block_len = q_ref.shape[1]
    cols = heads * block_len
    scale = HEAD_DIM ** (-0.5)
    for which in range(2):
        last = ids[which]
        query = stacked_heads(q_ref, which, heads)

        def step(block, carry, masked=False):
            highest, total, acc = carry
            start = pl.multiple_of(table[block] * block_len, block_len)
            key = kv_ref[pl.ds(start, block_len), :HEAD_DIM]
            value = kv_ref[pl.ds(start, block_len), HEAD_DIM:]
            scores = contract_cols(key, query) * scale
            if masked:
                scores = jnp.where(causal(block_len, heads), scores, -1e30)
            new_high = jnp.maximum(highest, jnp.max(scores, 0, keepdims=True))
            probs = jnp.exp(scores - new_high)
            fade = jnp.exp(highest - new_high)
            total = total * fade + jnp.sum(probs, 0, keepdims=True)
            acc = acc * fade + contract_rows(value, probs.astype(BF16))
            return (new_high, total, acc)

        begin = (
            jnp.full((1, cols), -1e30, F32),
            jnp.zeros((1, cols), F32),
            jnp.zeros((HEAD_DIM, cols), F32),
        )
        carry = lax.fori_loop(0, last, step, begin)
        highest, total, acc = step(last, carry, True)
        lse_ref[which] = highest + jnp.log(total)
        out = (acc / total).T
        for h in range(heads):
            o_ref[which, :, h * HEAD_DIM : (h + 1) * HEAD_DIM] = out[
                h * block_len : (h + 1) * block_len
            ].astype(BF16)


def attend_back_kernel(
    heads, table, ids, q_ref, kv_ref, o_ref, do_ref, lse_ref, dq_ref, dkv_ref, sums
):
    block_len = q_ref.shape[1]
    cols = heads * block_len
    scale = HEAD_DIM ** (-0.5)
    sums[...] = jnp.zeros_like(sums)
    for which in range(2):
        last = ids[which]
        query = stacked_heads(q_ref, which, heads)
        d_out = stacked_heads(do_ref, which, heads)
        out = stacked_heads(o_ref, which, heads)
        delta = jnp.sum((d_out.astype(F32) * out.astype(F32)).T, 0, keepdims=True)
        lse = lse_ref[which]

        def step(block, d_query, masked=False):
            start = pl.multiple_of(table[block] * block_len, block_len)
            key = kv_ref[pl.ds(start, block_len), :HEAD_DIM]
            value = kv_ref[pl.ds(start, block_len), HEAD_DIM:]
            scores = contract_cols(key, query) * scale
            probs = jnp.exp(scores - lse)
            if masked:
                probs = jnp.where(causal(block_len, heads), probs, 0.0)
            d_probs = contract_cols(value, d_out)
            d_scores = (probs * (d_probs - delta)).astype(BF16)
            sums[pl.ds(start, block_len), :HEAD_DIM] += dot(d_scores, query, ((1,), (0,)))
            sums[pl.ds(start, block_len), HEAD_DIM:] += dot(
                probs.astype(BF16), d_out, ((1,), (0,))
            )
            return d_query + contract_rows(key, d_scores)

        d_query = lax.fori_loop(0, last, step, jnp.zeros((HEAD_DIM, cols), F32))
        d_query = step(last, d_query, True)
        d_query = (d_query * scale).T
        for h in range(heads):
            dq_ref[which, :, h * HEAD_DIM : (h + 1) * HEAD_DIM] = d_query[
                h * block_len : (h + 1) * block_len
            ]
    dkv_ref[:, :HEAD_DIM] = (sums[:, :HEAD_DIM] * scale).astype(BF16)
    dkv_ref[:, HEAD_DIM:] = sums[:, HEAD_DIM:].astype(BF16)


def in_vmem(count):
    return [pl.BlockSpec(memory_space=pltpu.VMEM)] * count


def in_smem(count):
    return [pl.BlockSpec(memory_space=pltpu.SMEM)] * count


def attend(table, ids, query, keys_values, heads):
    _, block_len, width = query.shape
    tall = keys_values.shape[0]
    return pl.pallas_call(
        functools.partial(attend_kernel, heads),
        out_shape=(
            jax.ShapeDtypeStruct(query.shape, BF16),
            jax.ShapeDtypeStruct((2, 1, heads * block_len), F32),
        ),
        in_specs=in_smem(2) + in_vmem(2),
        out_specs=tuple(in_vmem(2)),
        compiler_params=pltpu.CompilerParams(vmem_limit_bytes=VMEM_LIMIT),
        cost_estimate=pl.CostEstimate(
            flops=2 * tall * block_len * width * 2,
            bytes_accessed=tall * 512,
            transcendentals=tall * heads * block_len,
        ),
        name="attend",
    )(table, ids, query, keys_values)


def attend_back(table, ids, query, keys_values, out, d_out, lse, heads):
    _, block_len, width = query.shape
    tall = keys_values.shape[0]
    return pl.pallas_call(
        functools.partial(attend_back_kernel, heads),
        out_shape=(
            jax.ShapeDtypeStruct(query.shape, F32),
            jax.ShapeDtypeStruct(keys_values.shape, BF16),
        ),
        in_specs=in_smem(2) + in_vmem(5),
        out_specs=tuple(in_vmem(2)),
        scratch_shapes=[pltpu.VMEM(keys_values.shape, F32)],
        compiler_params=pltpu.CompilerParams(vmem_limit_bytes=VMEM_LIMIT),
        cost_estimate=pl.CostEstimate(
            flops=5 * tall * block_len * width * 2,
            bytes_accessed=tall * 1024,
            transcendentals=tall * heads * block_len,
        ),
        name="attend_back",
    )(table, ids, query, keys_values, out, d_out, lse)


MESH = pl.DeviceIdType.MESH


def greet(devices):
    barrier = pltpu.get_barrier_semaphore()
    for device in devices:
        pl.semaphore_signal(barrier, inc=1, device_id=device, device_id_type=MESH)
    pl.semaphore_wait(barrier, len(devices))


def remote(src, dst, send, recv, device):
    return pltpu.make_async_remote_copy(
        src_ref=src, dst_ref=dst, send_sem=send, recv_sem=recv, device_id=device, device_id_type=MESH
    )


def group_places(n):
    ctx = lax.axis_index("ctx")
    me = lax.axis_index("fsdp")
    partner = me + 1 - 2 * (me % 2)
    others = [(me + 2 * k) % n for k in range(1, n // 2)]
    senders = [(me + n - 2 * k) % n for k in range(1, n // 2)]
    return ctx, me, partner, others, senders


def sum_phases(mode, n, cuts, *refs):
    gathers = mode != "input"
    if mode == "attention":
        partial, tokens, gain, hidden_out, all_out = refs[:5]
    elif mode == "mlp":
        partial, hidden_in, cot, gain, d_out, all_out, d_gain = refs[:7]
    else:
        partial, tokens, d_hidden_in, gain, d_out, d_gain = refs[:6]
    near, summed, far, stage, near_s, near_r, far_s, far_r, own_s, own_r, out_s, out_r, fwd_s, fwd_r = refs[-14:]
    ctx, me, partner, others, senders = group_places(n)
    chips = n // 2
    rows = partial.shape[2]
    piece = rows // cuts
    chunks = [(w, i * piece) for w in range(2) for i in range(cuts)]

    def part(ref, w, lead, start):
        return ref.at[w, lead, pl.ds(start, piece)]

    first = []
    for c, (w, start) in enumerate(chunks):
        for j in range(chips):
            target = (partner + 2 * (j + 1)) % n
            copy = remote(
                part(partial, w, target, start),
                part(near, w, j, start),
                near_s.at[c, j],
                near_r.at[c, j],
                (ctx, partner),
            )
            copy.start()
            first.append(copy)
    yield

    second = []

    def post(c):
        w, start = chunks[c]
        for j in range(chips - 1):
            copy = remote(
                part(summed, w, j, start),
                part(far, w, j, start),
                far_s.at[c, j],
                far_r.at[c, j],
                (ctx, others[j]),
            )
            copy.start()
            second.append(copy)

    for c, (w, start) in enumerate(chunks):
        span = pl.ds(start, piece)
        for j in range(chips - 1):
            first[c * chips + j].wait()
            target = (me + 2 * (j + 1)) % n
            summed[w, j, span] = (
                partial[w, target, span].astype(F32) + near[w, j, span].astype(F32)
            ).astype(BF16)
        if c:
            post(c - 1)
    post(len(chunks) - 1)
    yield

    if mode != "attention":
        d_gain[...] = jnp.zeros_like(d_gain)
    third = []

    def spread(c):
        w, start = chunks[c]
        src = stage.at[w, pl.ds(start, piece)]
        for k in range(chips - 1):
            copy = remote(src, part(all_out, w, me, start), out_s.at[c, k], out_r.at[c, k], (ctx, others[k]))
            copy.start()
            third.append(copy)
        copy = remote(src, part(all_out, w, me, start), own_s.at[c], own_r.at[c], (ctx, partner))
        copy.start()
        return copy

    near_copies = []
    for c, (w, start) in enumerate(chunks):
        span = pl.ds(start, piece)
        first[c * chips + chips - 1].wait()
        total = partial[w, me, span].astype(F32) + near[w, chips - 1, span].astype(F32)
        for j in range(chips - 1):
            second[c * (chips - 1) + j].wait()
            total += far[w, j, span].astype(F32)
        if mode == "attention":
            hidden = tokens[w, span].astype(F32) + total
            hidden_out[w, span] = hidden
            rounded = (hidden * rms_scale(hidden) * gain[...]).astype(BF16)
        elif mode == "mlp":
            hidden = hidden_in[w, span]
            d_norm, gain_part = rms_backward(hidden, rms_scale(hidden), gain[...], total)
            d_gain[...] += gain_part[None]
            d_hidden = cot[w, span].astype(F32) + d_norm
            d_out[w, span] = d_hidden
            rounded = d_hidden.astype(BF16)
        else:
            values = tokens[w, span].astype(F32)
            d_norm, gain_part = rms_backward(values, rms_scale(values), gain[...], total)
            d_gain[...] += gain_part[None]
            d_out[w, span] = d_hidden_in[w, span] + d_norm
        if gathers:
            stage[w, span] = rounded
            all_out[w, me, span] = rounded
            if c:
                near_copies.append(spread(c - 1))
    if not gathers:
        return
    near_copies.append(spread(len(chunks) - 1))
    yield

    forwards = []
    for c, (w, start) in enumerate(chunks):
        for k in range(chips - 1):
            third[c * (chips - 1) + k].wait_recv()
            block = part(all_out, w, senders[k], start)
            copy = remote(block, block, fwd_s.at[c, k], fwd_r.at[c, k], (ctx, partner))
            copy.start()
            forwards.append(copy)
    yield
    for copy in third:
        copy.wait_send()
    for copy in near_copies + forwards:
        copy.wait()


def sum_kernel(mode, n, cuts, *refs):
    ctx, _, partner, others, _ = group_places(n)
    greet([(ctx, partner)] + [(ctx, o) for o in others])
    for _ in sum_phases(mode, n, cuts, *refs):
        pass


def sum_shapes(mode, partial):
    _, n, rows, width = partial.shape
    chips = n // 2
    row_shape = (2, rows, width)
    full = jax.ShapeDtypeStruct(row_shape, F32)
    gathered = jax.ShapeDtypeStruct(partial.shape, BF16)
    gain_sum = jax.ShapeDtypeStruct((1, width), F32)
    out_shape = {
        "attention": (full, gathered),
        "mlp": (full, gathered, gain_sum),
        "input": (full, gain_sum),
    }[mode]
    dma = pltpu.SemaphoreType.DMA
    chunks = 2 * SUM_CUTS
    scratch = [
        pltpu.VMEM((2, chips, rows, width), BF16),
        pltpu.VMEM((2, chips - 1, rows, width), BF16),
        pltpu.VMEM((2, chips - 1, rows, width), BF16),
        pltpu.VMEM(row_shape, BF16),
        dma((chunks, chips)),
        dma((chunks, chips)),
        dma((chunks, chips - 1)),
        dma((chunks, chips - 1)),
        dma((chunks,)),
        dma((chunks,)),
        dma((chunks, chips - 1)),
        dma((chunks, chips - 1)),
        dma((chunks, chips - 1)),
        dma((chunks, chips - 1)),
    ]
    return out_shape, scratch


SUM_CUTS = 2


def group_sum(mode, partial, *operands, collective):
    _, n, rows, width = partial.shape
    out_shape, scratch = sum_shapes(mode, partial)
    return pl.pallas_call(
        functools.partial(sum_kernel, mode, n, SUM_CUTS),
        out_shape=out_shape,
        in_specs=in_vmem(1 + len(operands)),
        out_specs=tuple(in_vmem(len(out_shape))),
        scratch_shapes=scratch,
        compiler_params=pltpu.CompilerParams(
            vmem_limit_bytes=VMEM_LIMIT, collective_id=collective, has_side_effects=True
        ),
        cost_estimate=pl.CostEstimate(
            flops=20 * rows * width, bytes_accessed=60_000_000, transcendentals=0
        ),
        name="group_sum_" + mode,
    )(partial, *operands)


def ring_index(place, n):
    late = place // (n // 2)
    return (1 - late) * 2 * place + late * (2 * n - 1 - 2 * place)


def ring_place(index, n):
    odd = index % 2
    return (1 - odd) * (index // 2) + odd * (n - 1 - index // 2)


def share_kernel(n, own, out, right_s, right_r, left_s, left_r, near_s, near_r):
    ctx = lax.axis_index("ctx")
    me = lax.axis_index("fsdp")
    which = me % 2
    partner = me + 1 - 2 * which
    place = ring_place(ctx, n)
    right = (ring_index((place + 1) % n, n), me)
    left = (ring_index((place + n - 1) % n, n), me)
    greet([right, left, (ctx, partner)])

    def block(offset):
        return out.at[ring_index((place + n + offset) % n, n), which]

    def to_right(step):
        src = own.at[which] if step == 0 else block(-step)
        return remote(src, block(-step), right_s.at[step], right_r.at[step], right)

    def to_left(step):
        src = own.at[which] if step == 0 else block(step)
        return remote(src, block(step), left_s.at[step], left_r.at[step], left)

    rights, lefts = n // 2, n - 1 - n // 2
    sent = [to_right(0), to_left(0)]
    for copy in sent:
        copy.start()
    out[ctx] = own[...]
    going = [sent[0], sent[1]]
    for step in range(1, rights + 1):
        going[0].wait_recv()
        if step < rights:
            going[0] = to_right(step)
            going[0].start()
            sent.append(going[0])
        hand = remote(block(-step), block(-step), near_s.at[step - 1], near_r.at[step - 1], (ctx, partner))
        hand.start()
        sent.append(hand)
        if step <= lefts:
            going[1].wait_recv()
            if step < lefts:
                going[1] = to_left(step)
                going[1].start()
                sent.append(going[1])
            slot = rights + step - 1
            hand = remote(block(step), block(step), near_s.at[slot], near_r.at[slot], (ctx, partner))
            hand.start()
            sent.append(hand)
    for copy in sent:
        copy.wait_send()
    for step in range(1, rights + 1):
        remote(block(-step), block(-step), near_s.at[step - 1], near_r.at[step - 1], (ctx, partner)).wait_recv()
    for step in range(1, lefts + 1):
        slot = rights + step - 1
        remote(block(step), block(step), near_s.at[slot], near_r.at[slot], (ctx, partner)).wait_recv()


def share_keys(own, n, collective):
    dma = pltpu.SemaphoreType.DMA
    return pl.pallas_call(
        functools.partial(share_kernel, n),
        out_shape=jax.ShapeDtypeStruct((n,) + own.shape, BF16),
        in_specs=in_vmem(1),
        out_specs=in_vmem(1)[0],
        scratch_shapes=[dma((n // 2,))] * 4 + [dma((n - 1,))] * 2,
        compiler_params=pltpu.CompilerParams(
            vmem_limit_bytes=VMEM_LIMIT, collective_id=collective, has_side_effects=True
        ),
        cost_estimate=pl.CostEstimate(flops=0, bytes_accessed=60_000_000, transcendentals=0),
        name="share_keys",
    )(own)


def return_kernel(n, partial, out, near, summed, far, near_s, near_r, far_s, far_r):
    ctx = lax.axis_index("ctx")
    me = lax.axis_index("fsdp")
    which = me % 2
    partner = me + 1 - 2 * which
    others = [(ctx + k) % n for k in range(1, n)]
    greet([(ctx, partner)] + [(o, me) for o in others])
    order = others + [ctx]
    first = []
    for k, target in enumerate(order):
        copy = remote(partial.at[target, 1 - which], near.at[k], near_s.at[k], near_r.at[k], (ctx, partner))
        copy.start()
        first.append(copy)
    second = []

    def post(k):
        copy = remote(summed.at[k], far.at[k], far_s.at[k], far_r.at[k], (others[k], me))
        copy.start()
        second.append(copy)

    for k in range(n - 1):
        first[k].wait()
        summed[k] = (partial[others[k], which].astype(F32) + near[k].astype(F32)).astype(BF16)
        if k:
            post(k - 1)
    post(n - 2)
    out[1 - which] = jnp.zeros(out.shape[1:], F32)
    first[n - 1].wait()
    out[which] = partial[ctx, which].astype(F32) + near[n - 1].astype(F32)
    for k in range(n - 1):
        second[k].wait()
        out[which] += far[k].astype(F32)


def return_grads(partial, collective):
    n = partial.shape[0]
    block = partial.shape[2:]
    dma = pltpu.SemaphoreType.DMA
    return pl.pallas_call(
        functools.partial(return_kernel, n),
        out_shape=jax.ShapeDtypeStruct(partial.shape[1:], F32),
        in_specs=in_vmem(1),
        out_specs=in_vmem(1)[0],
        scratch_shapes=[
            pltpu.VMEM((n,) + block, BF16),
            pltpu.VMEM((n - 1,) + block, BF16),
            pltpu.VMEM((n - 1,) + block, BF16),
            dma((n,)),
            dma((n,)),
            dma((n - 1,)),
            dma((n - 1,)),
        ],
        compiler_params=pltpu.CompilerParams(
            vmem_limit_bytes=VMEM_LIMIT, collective_id=collective, has_side_effects=True
        ),
        cost_estimate=pl.CostEstimate(flops=0, bytes_accessed=80_000_000, transcendentals=0),
        name="return_grads",
    )(partial)


def ring_sum_kernel(n, members, plan, swaps, sizes, mode, extra_ins, extra_outs, *refs):
    arrays = len(sizes)
    ins = []
    for size in sizes:
        ins.append(refs[:size])
        refs = refs[size:]
    side_ins, refs = refs[:extra_ins], refs[extra_ins:]
    outs, refs = refs[:arrays], refs[arrays:]
    side_outs, refs = refs[:extra_outs], refs[extra_outs:]
    count = len(plan)
    arrived, stages, sends, recvs = (refs[i * count : (i + 1) * count] for i in range(4))
    refs = refs[4 * count :]
    done, swap_s, swap_r = (refs[i * len(swaps) : (i + 1) * len(swaps)] for i in range(3))
    refs = refs[3 * len(swaps) :]
    ctx = lax.axis_index("ctx")
    me = lax.axis_index("fsdp")
    place = ring_place(ctx, n)
    around = {step: (ring_index((place + n + step) % n, n), me) for step in (1, -1)}
    greet([around[1], around[-1]] + [(ctx, (me + k) % members) for k in range(1, members)])
    beside = iter(())
    if mode:
        beside = sum_phases(mode, members, SUM_CUTS, *side_ins, *side_outs, *refs)

    def copy(i, hop, src):
        step = plan[i][3]
        return remote(src, arrived[i].at[hop], sends[i].at[hop], recvs[i].at[hop], around[step])

    def chunk(i, hop):
        step = plan[i][3]
        return ring_index((place + n * n - step * (hop + 1)) % n, n)

    def term(i, hop):
        which, low, high, _ = plan[i]
        if len(ins[which]) == 1:
            return ins[which][0][chunk(i, hop), :, low:high].astype(F32)
        left, right = ins[which]
        return jnp.dot(left[chunk(i, hop)], right[:, low:high], preferred_element_type=F32)

    for i in range(count):
        stages[i][0] = term(i, 0).astype(BF16)
        if i:
            copy(i - 1, 0, stages[i - 1].at[0]).start()
    copy(count - 1, 0, stages[count - 1].at[0]).start()
    next(beside, None)

    def add(i, hop):
        mine = term(i, hop)
        copy(i, hop - 1, stages[i].at[0]).wait_recv()
        return (arrived[i][hop - 1].astype(F32) + mine).astype(BF16)

    def one_hop(hop, carry):
        slot = hop % 2
        for i in range(count):
            @pl.when(hop > 1)
            def _():
                copy(i, hop - 2, stages[i].at[slot]).wait_send()

            stages[i][slot] = add(i, hop)
            if i:
                copy(i - 1, hop, stages[i - 1].at[slot]).start()
        copy(count - 1, hop, stages[count - 1].at[slot]).start()
        return carry

    hop = 1
    if mode:
        for _ in range(min(4 if mode == "mlp" else 2, n - 3)):
            one_hop(jnp.int32(hop), 0)
            hop += 1
            next(beside, None)
    lax.fori_loop(hop, n - 1, one_hop, 0)
    for i, (which, low, high, _) in enumerate(plan):
        target = done[swaps.index(which)] if which in swaps else outs[which]
        value = add(i, n - 1)
        rows = target.shape[1]
        for group in range(target.shape[0]):
            target[group, :, low:high] = value[group * rows : (group + 1) * rows]
    swapped = []
    for j, which in enumerate(swaps):
        for k in range(1, members):
            other = (me + k) % members
            swapped.append(
                remote(
                    done[j].at[other],
                    outs[which].at[me],
                    swap_s[j].at[k - 1],
                    swap_r[j].at[k - 1],
                    (ctx, other),
                )
            )
            swapped[-1].start()
        outs[which][me] = done[j][me]
    for _ in beside:
        pass
    for i in range(count):
        for hop in (n - 3, n - 2):
            copy(i, hop, stages[i].at[hop % 2]).wait_send()
    for move in swapped:
        move.wait()


def ring_sum(arrays, groups, plan, swaps, members, collective, mode=None, operands=()):
    n = arrays[0][0].shape[0]
    dma = pltpu.SemaphoreType.DMA
    talls = [array[0].shape[1] for array in arrays]
    blocks = [(talls[which], high - low) for which, low, high, _ in plan]
    sums = [
        (g, tall // g, array[-1].shape[-1]) for array, g, tall in zip(arrays, groups, talls)
    ]
    flat = [operand for array in arrays for operand in array]
    extra_shape, extra_scratch = sum_shapes(mode, operands[0]) if mode else ((), [])
    out_shape = tuple(jax.ShapeDtypeStruct(shape, BF16) for shape in sums) + tuple(extra_shape)
    return pl.pallas_call(
        functools.partial(
            ring_sum_kernel,
            n,
            members,
            plan,
            swaps,
            tuple(len(array) for array in arrays),
            mode,
            len(operands),
            len(extra_shape),
        ),
        out_shape=out_shape,
        in_specs=in_vmem(len(flat) + len(operands)),
        out_specs=tuple(in_vmem(len(out_shape))),
        scratch_shapes=[pltpu.VMEM((n - 1,) + b, BF16) for b in blocks]
        + [pltpu.VMEM((2,) + b, BF16) for b in blocks]
        + [dma((n - 1,)) for _ in blocks] * 2
        + [pltpu.VMEM(sums[which], BF16) for which in swaps]
        + [dma((members - 1,)) for _ in swaps] * 2
        + extra_scratch,
        compiler_params=pltpu.CompilerParams(
            vmem_limit_bytes=VMEM_LIMIT, collective_id=collective, has_side_effects=True
        ),
        cost_estimate=pl.CostEstimate(flops=0, bytes_accessed=200_000_000, transcendentals=0),
        name="ring_sum",
    )(*flat, *operands)


def ring_gather_kernel(n, count, *refs):
    owns, outs, sends, recvs = (refs[i * count : (i + 1) * count] for i in range(4))
    ctx = lax.axis_index("ctx")
    me = lax.axis_index("fsdp")
    place = ring_place(ctx, n)
    around = {step: (ring_index((place + n + step) % n, n), me) for step in (1, -1)}
    greet([around[1], around[-1]])
    far = n // 2

    def copy(i, step, half, hop):
        middle = owns[i].shape[-1] // 2
        lanes = pl.ds(half * middle, middle)
        block = outs[i].at[ring_index((place + n - step * hop) % n, n), :, lanes]
        src = block if hop else owns[i].at[:, lanes]
        row = half if step == 1 else 2 + half
        return remote(src, block, sends[i].at[row, hop], recvs[i].at[row, hop], around[step])

    def hops(step, half):
        return far if (step == 1) == (half == 0) else far - 1

    lines = [(i, step, half) for step, half in ((1, 0), (-1, 1), (1, 1), (-1, 0)) for i in range(count)]
    for i, step, half in lines:
        copy(i, step, half, 0).start()
    for own, out in zip(owns, outs):
        out[ctx] = own[...]
    for hop in range(1, far + 1):
        for i, step, half in lines:
            if hop <= hops(step, half):
                copy(i, step, half, hop - 1).wait_recv()
                if hop < hops(step, half):
                    copy(i, step, half, hop).start()
    for i, step, half in lines:
        for hop in range(hops(step, half)):
            copy(i, step, half, hop).wait_send()


def ring_gather(owns, n, collective):
    count = len(owns)
    return pl.pallas_call(
        functools.partial(ring_gather_kernel, n, count),
        out_shape=tuple(jax.ShapeDtypeStruct((n,) + own.shape, BF16) for own in owns),
        in_specs=in_vmem(count),
        out_specs=tuple(in_vmem(count)),
        scratch_shapes=[pltpu.SemaphoreType.DMA((4, n // 2))] * (2 * count),
        compiler_params=pltpu.CompilerParams(
            vmem_limit_bytes=VMEM_LIMIT, collective_id=collective, has_side_effects=True
        ),
        cost_estimate=pl.CostEstimate(flops=0, bytes_accessed=120_000_000, transcendentals=0),
        name="ring_gather",
    )(*owns)


def weave_kernel(planes, out):
    for e in range(2):
        out[:, e, :] = planes[e].astype(F32)


def weave(planes):
    _, rows, lanes = planes.shape
    block = 32 if rows % 32 == 0 else rows
    return pl.pallas_call(
        weave_kernel,
        grid=(rows // block,),
        out_shape=jax.ShapeDtypeStruct((rows, 2, lanes), F32),
        in_specs=[pl.BlockSpec((2, block, lanes), lambda i: (0, i, 0))],
        out_specs=pl.BlockSpec((block, 2, lanes), lambda i: (i, 0, 0)),
        cost_estimate=pl.CostEstimate(
            flops=0, bytes_accessed=12 * rows * lanes, transcendentals=0
        ),
        name="weave",
    )(planes)


def project_kernel(heads, x_ref, gain, w_ref, bias, cos_ref, sin_ref, normed_ref, q_ref, kv_ref):
    values = x_ref[...].astype(F32)
    normed = (values * rms_scale(values) * gain[...]).astype(BF16)
    normed_ref[...] = normed
    qkv = jnp.dot(normed, w_ref[...], preferred_element_type=F32) + bias[...]
    cosines, sines = cos_ref[...], sin_ref[...]
    for h in range(heads + 1):
        vector = qkv[:, h * HEAD_DIM : (h + 1) * HEAD_DIM]
        turned = vector * cosines + pltpu.roll(vector, HEAD_DIM // 2, 1) * sines
        if h < heads:
            q_ref[:, h * HEAD_DIM : (h + 1) * HEAD_DIM] = turned.astype(BF16)
        else:
            kv_ref[:, :HEAD_DIM] = turned.astype(BF16)
    kv_ref[:, HEAD_DIM:] = qkv[:, (heads + 1) * HEAD_DIM :].astype(BF16)


def project(x_all, gain, weights, bias, cosines, sines, heads):
    rows = x_all.shape[0]
    block = 128
    width = weights.shape[1]

    def tall(lanes):
        return pl.BlockSpec((block, lanes), lambda i: (i, 0))

    def fixed(shape):
        return pl.BlockSpec(shape, lambda i: (0, 0))

    lanes = (D, heads * HEAD_DIM, 2 * HEAD_DIM)
    return pl.pallas_call(
        functools.partial(project_kernel, heads),
        grid=(rows // block,),
        out_shape=tuple(jax.ShapeDtypeStruct((rows, n), BF16) for n in lanes),
        in_specs=[
            tall(D),
            fixed((1, D)),
            fixed((D, width)),
            fixed((1, width)),
            tall(HEAD_DIM),
            tall(HEAD_DIM),
        ],
        out_specs=tuple(tall(n) for n in lanes),
        compiler_params=pltpu.CompilerParams(vmem_limit_bytes=VMEM_LIMIT),
        cost_estimate=pl.CostEstimate(
            flops=2 * rows * D * width, bytes_accessed=4 * rows * D + 2 * D * width, transcendentals=0
        ),
        name="project",
    )(x_all, gain, weights, bias, cosines, sines)


def exchange(pieces, axis):
    return lax.all_to_all(pieces, axis, split_axis=0, concat_axis=0, tiled=True)


def together(*values):
    return lax.optimization_barrier(values)


def body(tokens, pairing, gain_attn, w_qkv, b_qkv, w_out, gain_mlp, w_gate_up, w_down, cotangent):
    half_rows = tokens.shape[2]
    n_ctx = lax.axis_size("ctx")
    n_fsdp = lax.axis_size("fsdp")
    ctx_index = lax.axis_index("ctx")
    fsdp_index = lax.axis_index("fsdp")
    stretch_len = half_rows * n_fsdp
    rows = 2 * stretch_len
    local_count = 2 * half_rows
    q_width = HEADS * HEAD_DIM
    kv_width = KV_HEADS * HEAD_DIM
    heads = HEADS // n_fsdp
    q_cols = heads * HEAD_DIM
    d_shard = w_qkv.shape[0]
    ff_shard = w_down.shape[0]

    owner_range = jnp.arange(n_ctx, dtype=jnp.int32)
    own_first = jnp.sum(jnp.where(owner_range == ctx_index, pairing, 0))
    ids = jnp.stack([own_first, 2 * n_ctx - 1 - own_first])
    inverse_pair = jnp.sum(
        owner_range[:, None] * (pairing[:, None] == owner_range[None, :]).astype(jnp.int32), 0
    )
    table = jnp.concatenate([2 * inverse_pair, 2 * inverse_pair[::-1] + 1])
    position = (
        ids[:, None] * stretch_len + jnp.arange(stretch_len, dtype=jnp.int32)[None, :]
    ).reshape(rows)
    kv_of = [f * KV_HEADS // n_fsdp for f in range(n_fsdp)]
    my_kv = fsdp_index * KV_HEADS // n_fsdp

    small = lax.all_gather(jnp.concatenate([gain_attn, gain_mlp, b_qkv]), "fsdp", axis=0)
    small, w_qkv, w_gate_up = together(small, w_qkv, w_gate_up)
    gain_one = small[:, :d_shard].reshape(D).astype(F32)
    gain_two = small[:, d_shard : 2 * d_shard].reshape(D).astype(F32)
    bias = small[:, 2 * d_shard :].reshape(-1).astype(F32)
    x_all = lax.all_gather(tokens[0], "fsdp", axis=1, tiled=True).reshape(rows, D)
    qkv_pieces = jnp.stack(
        [
            jnp.concatenate(
                [
                    w_qkv[:, f * q_cols : (f + 1) * q_cols],
                    w_qkv[:, q_width + kv_of[f] * HEAD_DIM : q_width + (kv_of[f] + 1) * HEAD_DIM],
                    w_qkv[
                        :,
                        q_width + kv_width + kv_of[f] * HEAD_DIM : q_width
                        + kv_width
                        + (kv_of[f] + 1) * HEAD_DIM,
                    ],
                ],
                1,
            )
            for f in range(n_fsdp)
        ]
    )
    w_qkv_cols = exchange(qkv_pieces, "fsdp").reshape(D, -1)
    bias_cols = jnp.concatenate(
        [
            lax.dynamic_slice_in_dim(bias, fsdp_index * q_cols, q_cols),
            lax.dynamic_slice_in_dim(bias, q_width + my_kv * HEAD_DIM, HEAD_DIM),
            lax.dynamic_slice_in_dim(bias, q_width + kv_width + my_kv * HEAD_DIM, HEAD_DIM),
        ]
    )
    gate_up_pieces = w_gate_up.reshape(d_shard, 2, n_fsdp, ff_shard).transpose(2, 1, 3, 0)
    gate_up_pieces = with_layout_constraint(gate_up_pieces, Layout((0, 1, 2, 3)))
    x_all, w_qkv_cols, gate_up_pieces = together(x_all, w_qkv_cols, gate_up_pieces)
    gate_up_cols = exchange(gate_up_pieces, "fsdp")

    cosines, sines = rope_tables(position)
    normed1, query, own_kv = project(
        x_all,
        gain_one[None],
        w_qkv_cols,
        bias_cols[None],
        jnp.concatenate([cosines[:, 0], cosines[:, 0]], 1),
        jnp.concatenate([-sines[:, 0], sines[:, 0]], 1),
        heads,
    )
    query = query.reshape(2, stretch_len, q_cols)
    keys_values = share_keys(own_kv.reshape(2, stretch_len, 2 * HEAD_DIM), n_ctx, 4)
    keys_values = keys_values.reshape(n_ctx * rows, 2 * HEAD_DIM)
    attended, lse = attend(table, ids, query, keys_values, heads)
    attended16 = attended.reshape(rows, q_cols)

    def scatter(partial):
        return lax.psum_scatter(
            partial.astype(BF16).reshape(2, stretch_len, D), "fsdp", scatter_dimension=1, tiled=True
        ).astype(F32).reshape(local_count, D)

    def by_member(partial):
        return partial.astype(BF16).reshape(2, n_fsdp, half_rows, D)

    tokens_own = tokens[0]
    hidden, normed2 = group_sum(
        "attention",
        by_member(jnp.dot(attended16, w_out, preferred_element_type=F32)),
        tokens_own,
        gain_two[None],
        collective=1,
    )
    normed2, cot_own = together(normed2, cotangent[0])
    normed2 = normed2.reshape(rows, D)
    cot_all = lax.all_gather(cot_own, "fsdp", axis=1, tiled=True).reshape(rows, D)
    w_gate_cols, w_up_cols = (gate_up_cols[:, e] for e in range(2))
    normed2_parts = normed2.reshape(rows, n_fsdp, d_shard)
    gate_val, up_val = (
        jnp.einsum("tsk,sfk->tf", normed2_parts, w, preferred_element_type=F32)
        for w in (w_gate_cols, w_up_cols)
    )
    sigmoid_gate = jax.nn.sigmoid(gate_val)
    act16 = (jax.nn.silu(gate_val) * up_val).astype(BF16)
    result = hidden.reshape(local_count, D) + scatter(jnp.dot(act16, w_down, preferred_element_type=F32))
    block_output = result.astype(BF16).reshape(tokens.shape)

    d_act = contract_cols(cot_all, w_down)
    d_gate16 = (d_act * up_val * sigmoid_gate * (1.0 + gate_val * (1.0 - sigmoid_gate))).astype(BF16)
    d_up16 = (d_act * gate_val * sigmoid_gate).astype(BF16)
    d_normed2 = sum(
        jnp.einsum("tf,sfk->tsk", d, w, preferred_element_type=F32)
        for d, w in ((d_gate16, w_gate_cols), (d_up16, w_up_cols))
    )
    def by_columns(pieces):
        queries = [pieces[f][..., :q_cols] for f in range(n_fsdp)]
        rest = []
        for part in range(2):
            lo = q_cols + part * HEAD_DIM
            for g in range(KV_HEADS):
                rest.append(
                    sum(
                        pieces[f][..., lo : lo + HEAD_DIM].astype(F32)
                        for f in range(n_fsdp)
                        if kv_of[f] == g
                    ).astype(pieces[0].dtype)
                )
        return jnp.concatenate(queries + rest, -1)

    chunk_rows = d_shard // n_ctx
    down_rows = -(-ff_shard // (16 * n_ctx)) * 16
    side = D // 2

    def by_chunk(values):
        split = values.T.reshape(n_fsdp, n_ctx, chunk_rows, rows)
        return split.transpose(1, 0, 2, 3).reshape(n_ctx, n_fsdp * chunk_rows, rows)

    act_chunks = jnp.pad(act16.T, ((0, n_ctx * down_rows - ff_shard), (0, 0)))
    act_chunks = act_chunks.reshape(n_ctx, down_rows, rows)
    normed2_chunks = by_chunk(normed2)
    gate_sum, up_sum, down_sum, d_hidden, dh_all, d_gain_two = ring_sum(
        ((normed2_chunks, d_gate16), (normed2_chunks, d_up16), (act_chunks, cot_all)),
        (n_fsdp, n_fsdp, 1),
        ((0, 0, ff_shard, 1), (1, 0, ff_shard, -1), (2, 0, side, 1), (2, side, D, -1)),
        (0, 1),
        n_fsdp,
        7,
        "mlp",
        (by_member(d_normed2), hidden, cotangent[0], gain_two[None]),
    )
    planes = jnp.stack(
        [
            total.transpose(1, 0, 2).reshape(chunk_rows, n_fsdp * ff_shard)
            for total in (gate_sum, up_sum)
        ]
    )
    d_w_gate_up = weave(lax.all_gather(planes, "ctx", axis=1, tiled=True))
    dh_all = dh_all.reshape(rows, D)
    d_attended16 = contract_cols(dh_all, w_out).astype(BF16).reshape(2, stretch_len, q_cols)
    d_query, d_kv = attend_back(
        table, ids, query, keys_values, attended, d_attended16, lse, heads
    )
    d_kv_own = return_grads(d_kv.reshape(n_ctx, 2, stretch_len, 2 * HEAD_DIM), 5).reshape(rows, -1)

    d_rotated = jnp.concatenate([d_query.reshape(rows, q_cols), d_kv_own[:, :HEAD_DIM]], 1)
    d_rotated = unrotate(
        d_rotated.reshape(rows, heads + 1, HEAD_DIM), cosines, sines
    ).reshape(rows, q_cols + HEAD_DIM)
    d_qkv = jnp.concatenate([d_rotated, d_kv_own[:, HEAD_DIM:]], 1)
    d_bias = jnp.sum(d_qkv, 0)
    d_qkv16 = d_qkv.astype(BF16)
    d_normed1 = contract_cols(d_qkv16, w_qkv_cols)
    x32 = x_all.astype(F32)
    d_gain_one = jnp.sum(d_normed1 * x32 * rms_scale(x32), 0)
    zeros = jnp.zeros_like(d_bias)
    d_bias_full = by_columns([jnp.where(fsdp_index == f, d_bias, zeros) for f in range(n_fsdp)])
    parts = jnp.concatenate(
        [v.reshape(n_fsdp, -1) for v in (d_gain_one, d_gain_two, d_bias_full)], 1
    ).astype(BF16)
    length = parts.shape[1]
    few = 2 * HEAD_DIM
    vector_rows = -(-length // (n_ctx * few))
    parts = jnp.pad(parts, ((0, 0), (0, n_ctx * vector_rows * few - length)))
    parts = parts.reshape(n_fsdp, n_ctx, vector_rows, few)
    parts = jnp.pad(parts, ((0, 0), (0, 0), (0, -vector_rows % 16), (0, 0)))
    parts = parts.transpose(1, 0, 2, 3).reshape(n_ctx, -1, few)
    attended_chunks = attended16.T.reshape(n_ctx, chunk_rows, rows)
    pieces, out_sum, vector, d_tokens, _ = ring_sum(
        ((by_chunk(normed1), d_qkv16), (attended_chunks, dh_all), (parts,)),
        (n_fsdp, 1, n_fsdp),
        (
            (0, 0, q_cols, 1),
            (0, q_cols, d_qkv16.shape[-1], -1),
            (1, 0, side, 1),
            (1, side, D, -1),
            (2, 0, few, 1),
        ),
        (0, 2),
        n_fsdp,
        8,
        "input",
        (by_member(d_normed1), tokens_own, d_hidden, gain_one[None]),
    )
    d_tokens = d_tokens.reshape(tokens.shape)
    qkv_sum = by_columns([pieces[f] for f in range(n_fsdp)])
    vector = jnp.sum(vector.astype(F32), 0)[:vector_rows].astype(BF16)
    vector = jnp.pad(vector, ((0, chunk_rows - vector_rows), (0, 0)))
    attention_sum, d_w_down = ring_gather(
        (jnp.concatenate([qkv_sum, out_sum[0], vector], -1), down_sum[0]), n_ctx, 9
    )
    d_w_down = d_w_down.reshape(n_ctx * down_rows, D)[:ff_shard].astype(F32)
    vector = attention_sum[:, :vector_rows, -few:].astype(F32).reshape(-1)
    attention_sum = attention_sum.reshape(d_shard, -1)
    qkv_width = qkv_sum.shape[-1]
    d_w_qkv = attention_sum[:, :qkv_width].astype(F32)
    d_w_out = attention_sum[:, qkv_width : qkv_width + D].astype(F32)
    d_gain_attn = vector[:d_shard]
    d_gain_mlp = vector[d_shard : 2 * d_shard]
    d_b_qkv = vector[2 * d_shard : 2 * d_shard + b_qkv.shape[0]]

    return (
        block_output,
        d_tokens,
        d_gain_attn,
        d_w_qkv,
        d_b_qkv,
        d_w_out,
        d_gain_mlp,
        d_w_gate_up,
        d_w_down,
    )


def solution(mesh):
    placed = (
        P("ctx", None, "fsdp", None),
        P(),
        P("fsdp"),
        P("fsdp", None),
        P("fsdp"),
        P("fsdp", None),
        P("fsdp"),
        P("fsdp", None, None),
        P("fsdp", None),
        P("ctx", None, "fsdp", None),
    )
    return jax.shard_map(
        body,
        mesh=mesh,
        in_specs=placed,
        out_specs=(
            P("ctx", None, "fsdp", None),
            P("ctx", None, "fsdp", None),
            P("fsdp"),
            P("fsdp", None),
            P("fsdp"),
            P("fsdp", None),
            P("fsdp"),
            P("fsdp", None, None),
            P("fsdp", None),
        ),
        check_vma=False,
    )
```
